32 devices in a mesh: dp: 8 (over z, core), tensor: 4 (over y, x).
Axes of the slice: x: 2, y: 2, z: 4, core: 2. Of those that a mesh axis runs over, the one named last changes fastest.
Arguments:
- block_input: bfloat16 [4096, 2048], P('dp'), may hold values from -6 to 6
- cotangent: bfloat16 [4096, 2048], P('dp'), may hold values from -6 to 6
- lengths: int32 [8], P('dp'), may hold values from 1 to 512, as said below
- attn_gain: bfloat16 [2048], P('dp'), may hold values from 0.5 to 1.5
- attn_shift: bfloat16 [2048], P('dp'), may hold values from -3 to 3
- ffn_gain: bfloat16 [2048], P('dp'), may hold values from 0.5 to 1.5
- ffn_shift: bfloat16 [2048], P('dp'), may hold values from -3 to 3
- qkv_weight: bfloat16 [3, 2048, 2048], P(None, 'dp', 'tensor')
- qkv_bias: bfloat16 [3, 2048], P(None, ('tensor', 'dp')), may hold values from -3 to 3
- out_weight: bfloat16 [2048, 2048], P('tensor', 'dp'), may hold values from -1 to 1
- out_bias: bfloat16 [2048], P('dp'), may hold values from -3 to 3
- up_weight: bfloat16 [2048, 8192], P('dp', 'tensor'), may hold values from -0.125 to 0.125
- up_bias: bfloat16 [8192], P(('tensor', 'dp')), may hold values from -3 to 3
- down_weight: bfloat16 [8192, 2048], P('tensor', 'dp'), may hold values from -0.0625 to 0.0625
Outputs:
- block_output: bfloat16 [4096, 2048], P('dp')
- dblock_input: bfloat16 [4096, 2048], P('dp')
- dattn_gain: float32 [2048], P('dp')
- dattn_shift: float32 [2048], P('dp')
- dffn_gain: float32 [2048], P('dp')
- dffn_shift: float32 [2048], P('dp')
- dqkv_weight: float32 [3, 2048, 2048], P(None, 'dp', 'tensor')
- dqkv_bias: float32 [3, 2048], P(None, ('tensor', 'dp'))
- dout_weight: float32 [2048, 2048], P('tensor', 'dp')
- dout_bias: float32 [2048], P('dp')
- dup_weight: float32 [2048, 8192], P('dp', 'tensor')
- dup_bias: float32 [8192], P(('tensor', 'dp'))
- ddown_weight: float32 [8192, 2048], P('tensor', 'dp')
The draws below stay inside these ranges and needn't reach their ends.
Inputs may be any that keep to these rules, and one draw needn't show every extreme that they name: `lengths`: one sequence for each index of dp; some sequence uses all 512 slots.
All inputs are finite; a program needn't handle non-finite values.
Results may differ from the reference program's by a relative error of at most 0.014.
Values may be sent and summed in bfloat16 or wider, within the bound.
A program may use at most 192 MiB of HBM per device.

```python
import math
import jax
import jax.numpy as jnp
from jax import lax

D = 2048
H = 8
HD = 256
FF = 8192
ROT = 64
SEQ_LEN = 512
TOKENS = 4096
N_DP = 8


def draw_lengths(key, part):
    key_shift, key_cut, key_pick = jax.random.split(key, 3)
    shifts = jax.random.randint(key_shift, (N_DP,), 0, 4)
    span_rows = SEQ_LEN // jnp.left_shift(jnp.ones((N_DP,), jnp.int32), shifts)
    cut_rows = jax.random.randint(key_cut, (N_DP,), 0, 2 ** 30) % (span_rows // 2 + 1)
    drawn_rows = span_rows - cut_rows
    chosen = jax.random.randint(key_pick, (), 0, N_DP)
    return jnp.where(jnp.arange(N_DP) == chosen, SEQ_LEN, drawn_rows).astype(jnp.int32)


def draw_qkv_weight(key, part):
    key_base = jax.random.fold_in(key, 0)
    drawn_base = jax.random.normal(key_base, (3, D, D), jnp.float32) * D ** (-0.5)
    return drawn_base.astype(jnp.bfloat16)


def shard_levels(rng, extent, cuts, least, top_value):
    def one(axis_at, blocks):
        draws = jax.random.uniform(jax.random.fold_in(jax.random.fold_in(rng, 6), axis_at), (blocks,), jnp.float32, least / len(cuts), top_value / len(cuts))
        return jnp.repeat(jnp.exp(draws), extent[axis_at] // blocks).reshape((-1,) + (1,) * (len(extent) - axis_at - 1))

    loudness = one(*cuts[0])
    for cut in cuts[1:]:
        loudness = loudness * one(*cut)
    return loudness


def centred(key, extent, spread, bound, pieces=(), kind=jnp.bfloat16):
    drawn = jax.random.normal(key, extent, jnp.float32) * spread
    if len(pieces) > 0:
        drawn = shard_levels(key, extent, pieces, -0.22, 0.18) * drawn
    return jnp.clip(drawn, min=-bound, max=bound).astype(kind)


def setup_inputs(seed: int = 0) -> dict:
    seeds = jax.random.split(jax.random.key(seed), 15)
    return {
        "block_input": centred(seeds[0], (TOKENS, D), 1.0, 6.0, ((0, 8),)),
        "cotangent": centred(seeds[1], (TOKENS, D), 1.0, 6.0, ((0, 8),)),
        "lengths": draw_lengths(jax.random.fold_in(seeds[14], 71), 0),
        "attn_gain": jnp.clip(1.0 + 0.1 * jax.random.normal(seeds[3], (D,), jnp.float32), 0.5, 1.5).astype(jnp.bfloat16),
        "attn_shift": centred(seeds[4], (D,), 0.5, 3.0, ((0, 8),)),
        "ffn_gain": jnp.clip(1.0 + 0.1 * jax.random.normal(seeds[5], (D,), jnp.float32), 0.5, 1.5).astype(jnp.bfloat16),
        "ffn_shift": centred(seeds[6], (D,), 0.5, 3.0, ((0, 8),)),
        "qkv_weight": draw_qkv_weight(jax.random.fold_in(seeds[14], 71), 0),
        "qkv_bias": centred(seeds[8], (3, D), 0.6, 3.0, ((1, 32),)),
        "out_weight": centred(seeds[9], (D, D), (max(D // 64, 1)) ** -0.5, 1.0, ((0, 4), (1, 8))),
        "out_bias": centred(seeds[10], (D,), 0.5, 3.0, ((0, 8),)),
        "up_weight": centred(seeds[11], (D, FF), D ** -0.5, 0.125, ((0, 8), (1, 4))),
        "up_bias": centred(seeds[12], (FF,), 0.5, 3.0, ((0, 32),)),
        "down_weight": centred(seeds[13], (FF, D), FF ** -0.5, 0.0625, ((0, 4), (1, 8))),
    }


norm_eps = 1e-05
rope_base = 10000.0

def rope_tables(row_count, rot_width):
    half_rot = rot_width // 2
    freq_idx = jnp.arange(half_rot, dtype=jnp.float32)
    inv_freq = jnp.exp(-(2.0 * freq_idx / rot_width) * math.log(rope_base))
    angles = jnp.arange(row_count, dtype=jnp.float32)[:, None] * inv_freq[None, :]
    return (jnp.cos(angles), jnp.sin(angles))

def rotate(heads_arr, cosine, sine_tab, direction):
    half_rot = ROT // 2
    first_half = heads_arr[..., :half_rot]
    second_half = heads_arr[..., half_rot:ROT]
    rest_dims = heads_arr[..., ROT:]
    cos_b = cosine[:, None, :]
    sin_b = sine_tab[:, None, :] * direction
    new_first = first_half * cos_b - second_half * sin_b
    new_second = second_half * cos_b + first_half * sin_b
    return jnp.concatenate([new_first, new_second, rest_dims], axis=-1)

def gelu_exact(pre_act):
    return 0.5 * pre_act * (1.0 + lax.erf(pre_act * (1.0 / math.sqrt(2.0))))

def gelu_slope(pre_act):
    cdf_part = 0.5 * (1.0 + lax.erf(pre_act * (1.0 / math.sqrt(2.0))))
    return cdf_part + pre_act * jnp.exp(-0.5 * pre_act * pre_act) * (1.0 / math.sqrt(2.0 * math.pi))

def reference(block_input, cotangent, lengths, attn_gain, attn_shift, ffn_gain, ffn_shift, qkv_weight, qkv_bias, out_weight, out_bias, up_weight, up_bias, down_weight):
    gain_a = attn_gain.astype(jnp.float32)
    shift_a = attn_shift.astype(jnp.float32)
    gain_f = ffn_gain.astype(jnp.float32)
    shift_f = ffn_shift.astype(jnp.float32)
    qkv_wide = qkv_weight.astype(jnp.float32)
    qkv_b32 = qkv_bias.astype(jnp.float32)
    out_b32 = out_bias.astype(jnp.float32)
    up_b32 = up_bias.astype(jnp.float32)
    cosine, sine_tab = rope_tables(SEQ_LEN, ROT)
    positions = jnp.arange(SEQ_LEN, dtype=jnp.int32)
    causal = positions[None, :] <= positions[:, None]
    scale_qk = 1.0 / math.sqrt(HD)

    def one_sequence(totals, inputs):
        seq_rows, seq_grad, seq_len = inputs
        x_rows = seq_rows.astype(jnp.float32)
        row_mean = lax.optimization_barrier(jnp.mean(x_rows, axis=-1, keepdims=True))
        centered = x_rows - row_mean
        inv_std = lax.rsqrt(lax.optimization_barrier(jnp.mean(centered * centered, axis=-1, keepdims=True)) + norm_eps)
        normed = centered * inv_std
        attn_in = (normed * gain_a + shift_a).astype(jnp.bfloat16)
        ffn_in = (normed * gain_f + shift_f).astype(jnp.bfloat16)
        qkv_rows = jnp.einsum('ld,pde->ple', attn_in.astype(jnp.float32), qkv_wide) + qkv_b32[:, None, :]
        query_rows = rotate(qkv_rows[0].reshape(SEQ_LEN, H, HD), cosine, sine_tab, 1.0).astype(jnp.bfloat16)
        key_rows = rotate(qkv_rows[1].reshape(SEQ_LEN, H, HD), cosine, sine_tab, 1.0).astype(jnp.bfloat16)
        value_rows = qkv_rows[2].reshape(SEQ_LEN, H, HD).astype(jnp.bfloat16)
        key_mask = causal & (positions[None, :] < seq_len)
        raw_scores = jnp.einsum('lhe,mhe->hlm', query_rows.astype(jnp.float32), key_rows.astype(jnp.float32)) * scale_qk
        scores = jnp.where(key_mask[None], raw_scores, -jnp.inf)
        row_max = lax.optimization_barrier(jnp.max(scores, axis=-1, keepdims=True))
        exp_terms = jnp.exp(scores - row_max)
        row_total = lax.optimization_barrier(jnp.sum(exp_terms, axis=-1, keepdims=True))
        prob_bf = (exp_terms / row_total).astype(jnp.bfloat16)
        log_total = row_max + jnp.log(row_total)
        mixed_rows = jnp.einsum('hlm,mhe->lhe', prob_bf.astype(jnp.float32), value_rows.astype(jnp.float32)).astype(jnp.bfloat16)
        mixed_flat = mixed_rows.reshape(SEQ_LEN, D)
        attn_part = jnp.dot(mixed_flat, out_weight, preferred_element_type=jnp.float32)
        up_pre = jnp.dot(ffn_in, up_weight, preferred_element_type=jnp.float32) + up_b32
        hidden = gelu_exact(up_pre).astype(jnp.bfloat16)
        ffn_part = jnp.dot(hidden, down_weight, preferred_element_type=jnp.float32)
        out_rows = (x_rows + (attn_part + ffn_part) + out_b32).astype(jnp.bfloat16)
        row_valid = (positions < seq_len).astype(jnp.float32)[:, None]
        grad_rows = seq_grad.astype(jnp.float32) * row_valid
        grad_bf = grad_rows.astype(jnp.bfloat16)
        dout_b = lax.optimization_barrier(jnp.sum(grad_rows, axis=0))
        ddown_w = jnp.dot(hidden.T, grad_bf, preferred_element_type=jnp.float32)
        up_grad32 = jnp.dot(grad_bf, down_weight.T, preferred_element_type=jnp.float32) * gelu_slope(up_pre)
        up_grad = up_grad32.astype(jnp.bfloat16)
        dup_w = jnp.dot(ffn_in.T, up_grad, preferred_element_type=jnp.float32)
        dup_b = lax.optimization_barrier(jnp.sum(up_grad32, axis=0))
        ffn_back = jnp.dot(up_grad, up_weight.T, preferred_element_type=jnp.float32)
        mixed_grad = jnp.dot(grad_bf, out_weight.T, preferred_element_type=jnp.float32).astype(jnp.bfloat16).reshape(SEQ_LEN, H, HD)
        dout_w = jnp.dot(mixed_flat.T, grad_bf, preferred_element_type=jnp.float32)
        delta_rows = jnp.einsum('lhe,lhe->hl', mixed_grad.astype(jnp.float32), mixed_rows.astype(jnp.float32))
        probs32 = jnp.exp(scores - log_total)
        prob_back = probs32.astype(jnp.bfloat16)
        value_grad = jnp.einsum('hlm,lhe->mhe', prob_back.astype(jnp.float32), mixed_grad.astype(jnp.float32))
        prob_grad = jnp.einsum('lhe,mhe->hlm', mixed_grad.astype(jnp.float32), value_rows.astype(jnp.float32))
        score_grad = (probs32 * (prob_grad - delta_rows[:, :, None]) * scale_qk).astype(jnp.bfloat16)
        query_grad = jnp.einsum('hlm,mhe->lhe', score_grad.astype(jnp.float32), key_rows.astype(jnp.float32))
        key_grad = jnp.einsum('hlm,lhe->mhe', score_grad.astype(jnp.float32), query_rows.astype(jnp.float32))
        query_grad = rotate(query_grad, cosine, sine_tab, -1.0)
        key_grad = rotate(key_grad, cosine, sine_tab, -1.0)
        qkv_grad32 = jnp.stack([query_grad, key_grad, value_grad]).reshape(3, SEQ_LEN, D)
        dqkv_b = lax.optimization_barrier(jnp.sum(qkv_grad32, axis=1))
        qkv_grad = qkv_grad32.astype(jnp.bfloat16)
        dqkv_w = jnp.einsum('ld,ple->pde', attn_in.astype(jnp.float32), qkv_grad.astype(jnp.float32))
        attn_back = jnp.einsum('ple,pde->ld', qkv_grad.astype(jnp.float32), qkv_wide)
        dgain_a = lax.optimization_barrier(jnp.sum(attn_back * normed, axis=0))
        dshift_a = lax.optimization_barrier(jnp.sum(attn_back, axis=0))
        dgain_f = lax.optimization_barrier(jnp.sum(ffn_back * normed, axis=0))
        dshift_f = lax.optimization_barrier(jnp.sum(ffn_back, axis=0))
        norm_grad = attn_back * gain_a + ffn_back * gain_f
        grad_mean = lax.optimization_barrier(jnp.mean(norm_grad, axis=-1, keepdims=True))
        grad_proj = lax.optimization_barrier(jnp.mean(norm_grad * normed, axis=-1, keepdims=True))
        dx_rows = (grad_rows + inv_std * (norm_grad - grad_mean - normed * grad_proj)).astype(jnp.bfloat16)
        updates = (dgain_a, dshift_a, dgain_f, dshift_f, dqkv_w, dqkv_b, dout_w, dout_b, dup_w, dup_b, ddown_w)
        new_totals = tuple((total_now + update for total_now, update in zip(totals, updates)))
        return (new_totals, (out_rows, dx_rows))
    zeros_init = (jnp.zeros((D,), jnp.float32), jnp.zeros((D,), jnp.float32), jnp.zeros((D,), jnp.float32), jnp.zeros((D,), jnp.float32), jnp.zeros((3, D, D), jnp.float32), jnp.zeros((3, D), jnp.float32), jnp.zeros((D, D), jnp.float32), jnp.zeros((D,), jnp.float32), jnp.zeros((D, FF), jnp.float32), jnp.zeros((FF,), jnp.float32), jnp.zeros((FF, D), jnp.float32))
    seq_inputs = block_input.reshape(N_DP, SEQ_LEN, D)
    seq_cotan = cotangent.reshape(N_DP, SEQ_LEN, D)
    totals, stacked = lax.scan(one_sequence, zeros_init, (seq_inputs, seq_cotan, lengths))
    out_all = stacked[0].reshape(TOKENS, D)
    dx_all = stacked[1].reshape(TOKENS, D)
    return (out_all, dx_all, totals[0], totals[1], totals[2], totals[3], totals[4], totals[5], totals[6], totals[7], totals[8], totals[9], totals[10])
```

```python
import math

import jax
import jax.numpy as jnp
from jax import lax
from jax.sharding import PartitionSpec as P

HD = 256
ROT = 64


norm_eps = 1e-05
rope_base = 10000.0


def rope_tables(row_count, rot_width):
    half_rot = rot_width // 2
    freq_idx = jnp.arange(half_rot, dtype=jnp.float32)
    inv_freq = jnp.exp(-(2.0 * freq_idx / rot_width) * math.log(rope_base))
    angles = jnp.arange(row_count, dtype=jnp.float32)[:, None] * inv_freq[None, :]
    return (jnp.cos(angles), jnp.sin(angles))


def rotate(heads_arr, cosine, sine_tab, direction):
    half_rot = ROT // 2
    first_half = heads_arr[..., :half_rot]
    second_half = heads_arr[..., half_rot:ROT]
    rest_dims = heads_arr[..., ROT:]
    cos_b = cosine[:, None, :]
    sin_b = sine_tab[:, None, :] * direction
    new_first = first_half * cos_b - second_half * sin_b
    new_second = second_half * cos_b + first_half * sin_b
    return jnp.concatenate([new_first, new_second, rest_dims], axis=-1)


def gelu_exact(pre_act):
    return 0.5 * pre_act * (1.0 + lax.erf(pre_act * (1.0 / math.sqrt(2.0))))


def gelu_slope(pre_act):
    cdf_part = 0.5 * (1.0 + lax.erf(pre_act * (1.0 / math.sqrt(2.0))))
    return cdf_part + pre_act * jnp.exp(-0.5 * pre_act * pre_act) * (1.0 / math.sqrt(2.0 * math.pi))


def per_device(
    block_input,
    cotangent,
    lengths,
    attn_gain,
    attn_shift,
    ffn_gain,
    ffn_shift,
    qkv_weight,
    qkv_bias,
    out_weight,
    out_bias,
    up_weight,
    up_bias,
    down_weight,
):
    gathered = (
        lax.all_gather(qkv_weight, "dp", axis=1, tiled=True),
        lax.all_gather(out_weight, "dp", axis=1, tiled=True),
        lax.all_gather(up_weight, "dp", axis=0, tiled=True),
        lax.all_gather(down_weight, "dp", axis=1, tiled=True),
        lax.all_gather(qkv_bias, "dp", axis=1, tiled=True),
        lax.all_gather(up_bias, "dp", axis=0, tiled=True),
        lax.all_gather(out_bias, "dp", axis=0, tiled=True),
        lax.all_gather(attn_gain, "dp", axis=0, tiled=True),
        lax.all_gather(attn_shift, "dp", axis=0, tiled=True),
        lax.all_gather(ffn_gain, "dp", axis=0, tiled=True),
        lax.all_gather(ffn_shift, "dp", axis=0, tiled=True),
    )
    (
        qkv_full,
        out_full,
        up_full,
        down_full,
        qkv_b,
        up_b,
        outb_full,
        gain_a,
        shift_a,
        gain_f,
        shift_f,
    ) = gathered
    gain_a = gain_a.astype(jnp.float32)
    gain_f = gain_f.astype(jnp.float32)
    seq_rows = block_input.shape[0]
    local_width = qkv_full.shape[2]
    local_heads = local_width // HD
    seq_len = lengths[0]
    positions = jnp.arange(seq_rows, dtype=jnp.int32)
    scale_qk = 1.0 / math.sqrt(HD)
    block_rows = min(512, seq_rows)
    x_rows = block_input.astype(jnp.float32)
    row_mean = jnp.mean(x_rows, axis=-1, keepdims=True)
    centered = x_rows - row_mean
    inv_std = lax.rsqrt(jnp.mean(centered * centered, axis=-1, keepdims=True) + norm_eps)
    normed = centered * inv_std
    attn_in = (normed * gain_a + shift_a.astype(jnp.float32)).astype(jnp.bfloat16)
    ffn_in = (normed * gain_f + shift_f.astype(jnp.float32)).astype(jnp.bfloat16)
    qkv_rows = (
        jnp.einsum("ld,pde->ple", attn_in, qkv_full, preferred_element_type=jnp.float32)
        + qkv_b.astype(jnp.float32)[:, None, :]
    )
    cosine, sine_tab = rope_tables(seq_rows, ROT)
    query_rows = rotate(
        qkv_rows[0].reshape(seq_rows, local_heads, HD), cosine, sine_tab, 1.0
    ).astype(jnp.bfloat16)
    key_rows = rotate(qkv_rows[1].reshape(seq_rows, local_heads, HD), cosine, sine_tab, 1.0).astype(
        jnp.bfloat16
    )
    value_rows = qkv_rows[2].reshape(seq_rows, local_heads, HD).astype(jnp.bfloat16)

    def block_scores(row_lo, key_end):
        raw_scores = (
            jnp.einsum("lhe,mhe->hlm", query_rows, key_rows, preferred_element_type=jnp.float32)
            * scale_qk
        )
        key_mask = (positions[None, :key_end] <= positions[row_lo:key_end, None]) & (
            positions[None, :key_end] < seq_len
        )
        return jnp.where(key_mask[None], raw_scores, -jnp.inf)

    qblock = 0
    row_lo = qblock * block_rows
    key_end = row_lo + block_rows
    scores = block_scores(row_lo, key_end)
    row_max = jnp.max(scores, axis=-1, keepdims=True)
    exp_terms = jnp.exp(scores - row_max)
    row_total = jnp.sum(exp_terms, axis=-1, keepdims=True)
    prob_bf = (exp_terms / row_total).astype(jnp.bfloat16)
    lse_blocks = [row_max + jnp.log(row_total)]
    attn_blocks = jnp.einsum(
        "hlm,mhe->lhe", prob_bf, value_rows, preferred_element_type=jnp.float32
    ).astype(jnp.bfloat16)
    mixed_flat = attn_blocks.reshape(seq_rows, local_width)
    attn_part = jnp.dot(mixed_flat, out_full, preferred_element_type=jnp.float32)
    up_pre = jnp.dot(ffn_in, up_full, preferred_element_type=jnp.float32) + up_b.astype(jnp.float32)
    hidden = gelu_exact(up_pre).astype(jnp.bfloat16)
    ffn_part = jnp.dot(hidden, down_full, preferred_element_type=jnp.float32)
    branch_sum = lax.psum((attn_part + ffn_part).astype(jnp.bfloat16), "tensor").astype(jnp.float32)
    block_output = (x_rows + branch_sum + outb_full.astype(jnp.float32)).astype(jnp.bfloat16)
    qkv_back, out_back, up_back, down_back = (qkv_full, out_full, up_full, down_full)
    row_valid = (positions < seq_len).astype(jnp.float32)[:, None]
    grad_rows = cotangent.astype(jnp.float32) * row_valid
    grad_bf = grad_rows.astype(jnp.bfloat16)
    dout_b = jnp.sum(grad_rows, axis=0)
    ddown_w = jnp.einsum("lf,ld->fd", hidden, grad_bf, preferred_element_type=jnp.float32)
    up_grad32 = jnp.einsum(
        "ld,fd->lf", grad_bf, down_back, preferred_element_type=jnp.float32
    ) * gelu_slope(up_pre)
    up_grad = up_grad32.astype(jnp.bfloat16)
    dup_w = jnp.einsum("ld,lf->df", ffn_in, up_grad, preferred_element_type=jnp.float32)
    dup_b = jnp.sum(up_grad32, axis=0)
    ffn_back = jnp.einsum("lf,df->ld", up_grad, up_back, preferred_element_type=jnp.float32)
    mixed_grad = (
        jnp.einsum("ld,ed->le", grad_bf, out_back, preferred_element_type=jnp.float32)
        .astype(jnp.bfloat16)
        .reshape(seq_rows, local_heads, HD)
    )
    dout_w = jnp.einsum("le,ld->ed", mixed_flat, grad_bf, preferred_element_type=jnp.float32)
    delta_rows = jnp.einsum(
        "lhe,lhe->hl", mixed_grad, attn_blocks, preferred_element_type=jnp.float32
    )
    query_grad = jnp.zeros((seq_rows, local_heads, HD), jnp.float32)
    key_grad = jnp.zeros((seq_rows, local_heads, HD), jnp.float32)
    value_grad = jnp.zeros((seq_rows, local_heads, HD), jnp.float32)
    qblock = 0
    row_lo = qblock * block_rows
    key_end = row_lo + block_rows
    scores = block_scores(row_lo, key_end)
    probs32 = jnp.exp(scores - lse_blocks[qblock])
    prob_back = probs32.astype(jnp.bfloat16)
    value_grad = value_grad.at[:key_end].add(
        jnp.einsum("hlm,lhe->mhe", prob_back, mixed_grad, preferred_element_type=jnp.float32)
    )
    prob_grad = jnp.einsum(
        "lhe,mhe->hlm", mixed_grad, value_rows, preferred_element_type=jnp.float32
    )
    score_grad = (probs32 * (prob_grad - delta_rows[:, row_lo:key_end, None]) * scale_qk).astype(
        jnp.bfloat16
    )
    query_grad = query_grad.at[row_lo:key_end].set(
        jnp.einsum("hlm,mhe->lhe", score_grad, key_rows, preferred_element_type=jnp.float32)
    )
    key_grad = key_grad.at[:key_end].add(
        jnp.einsum("hlm,lhe->mhe", score_grad, query_rows, preferred_element_type=jnp.float32)
    )
    query_grad = rotate(query_grad, cosine, sine_tab, -1.0)
    key_grad = rotate(key_grad, cosine, sine_tab, -1.0)
    qkv_grad32 = jnp.stack([query_grad, key_grad, value_grad]).reshape(3, seq_rows, local_width)
    dqkv_b = jnp.sum(qkv_grad32, axis=1)
    qkv_grad = qkv_grad32.astype(jnp.bfloat16)
    dqkv_w = jnp.einsum("ld,ple->pde", attn_in, qkv_grad, preferred_element_type=jnp.float32)
    attn_back = jnp.einsum("ple,pde->ld", qkv_grad, qkv_back, preferred_element_type=jnp.float32)
    norm_part = attn_back * gain_a + ffn_back * gain_f
    norm_stats = jnp.stack(
        [
            jnp.sum(attn_back * normed, axis=0),
            jnp.sum(attn_back, axis=0),
            jnp.sum(ffn_back * normed, axis=0),
            jnp.sum(ffn_back, axis=0),
        ]
    )
    norm_grad = lax.psum(norm_part.astype(jnp.bfloat16), "tensor").astype(jnp.float32)
    stat_sum = lax.psum(norm_stats, "tensor")
    grad_mean = jnp.mean(norm_grad, axis=-1, keepdims=True)
    grad_proj = jnp.mean(norm_grad * normed, axis=-1, keepdims=True)
    dblock_input = (grad_rows + inv_std * (norm_grad - grad_mean - normed * grad_proj)).astype(
        jnp.bfloat16
    )
    dqkv_sent, dout_sent, dup_sent, ddown_sent, dqkvb_sent, dupb_sent, doutb_sent, stats_sent = (
        lax.psum_scatter(dqkv_w.astype(jnp.bfloat16), "dp", scatter_dimension=1, tiled=True).astype(jnp.float32),
        lax.psum_scatter(dout_w.astype(jnp.bfloat16), "dp", scatter_dimension=1, tiled=True).astype(jnp.float32),
        lax.psum_scatter(dup_w.astype(jnp.bfloat16), "dp", scatter_dimension=0, tiled=True).astype(jnp.float32),
        lax.psum_scatter(ddown_w.astype(jnp.bfloat16), "dp", scatter_dimension=1, tiled=True).astype(jnp.float32),
        lax.psum_scatter(dqkv_b, "dp", scatter_dimension=1, tiled=True),
        lax.psum_scatter(dup_b, "dp", scatter_dimension=0, tiled=True),
        lax.psum_scatter(dout_b, "dp", scatter_dimension=0, tiled=True),
        lax.psum_scatter(stat_sum, "dp", scatter_dimension=1, tiled=True),
    )
    return (
        block_output,
        dblock_input,
        stats_sent[0],
        stats_sent[1],
        stats_sent[2],
        stats_sent[3],
        dqkv_sent,
        dqkvb_sent,
        dout_sent,
        doutb_sent,
        dup_sent,
        dupb_sent,
        ddown_sent,
    )


def solution(mesh):
    in_specs = (
        P("dp", None),
        P("dp", None),
        P("dp"),
        P("dp"),
        P("dp"),
        P("dp"),
        P("dp"),
        P(None, "dp", "tensor"),
        P(None, ("tensor", "dp")),
        P("tensor", "dp"),
        P("dp"),
        P("dp", "tensor"),
        P(("tensor", "dp")),
        P("tensor", "dp"),
    )
    out_specs = (
        P("dp", None),
        P("dp", None),
        P("dp"),
        P("dp"),
        P("dp"),
        P("dp"),
        P(None, "dp", "tensor"),
        P(None, ("tensor", "dp")),
        P("tensor", "dp"),
        P("dp"),
        P("dp", "tensor"),
        P(("tensor", "dp")),
        P("tensor", "dp"),
    )
    return jax.shard_map(
        per_device, mesh=mesh, in_specs=in_specs, out_specs=out_specs, check_vma=False
    )
```

```python
import functools
import math
import types

import jax
import jax.numpy as jnp
from jax import lax
from jax.experimental import pallas as pl
from jax.experimental.pallas import tpu as pltpu
from jax.sharding import PartitionSpec as P

HD = 256
ROT = 64
UNIT = 256
ROWS = 128
MESH = pl.DeviceIdType.MESH

norm_eps = 1e-05
rope_base = 10000.0

F32 = jnp.float32
BF16 = jnp.bfloat16


def dot(a, b):
    return lax.dot_general(a, b, (((1,), (0,)), ((), ())), preferred_element_type=F32)


def dot_nt(a, b):
    return lax.dot_general(a, b, (((1,), (1,)), ((), ())), preferred_element_type=F32)


def dot_tn(a, b):
    return lax.dot_general(a, b, (((0,), (0,)), ((), ())), preferred_element_type=F32)


def ds(i, size):
    return pl.ds(pl.multiple_of(i * size, size), size)


def layer_kernel(
    d,
    len_ref,
    x_hbm,
    cot_hbm,
    wl,
    norm_ref,
    bias_ref,
    rope_ref,
    part_hbm,
    dw_hbm,
    small_ref,
    bg_ref,
    W,
    A,
    At,
    X,
    Acc,
    Y,
    G,
    QK,
    PB,
    DS,
    S,
    SB,
    SR,
    LR,
    stage,
    in_sem,
    own_sem,
    ag_recv,
    agR,
    agL,
    agS,
    credit,
    sb_sem,
    sr_sem,
    ls_sem,
    lr_sem,
    out_sem,
):
    n, T, D, Dsl, U = d.n, d.T, d.D, d.Dsl, d.U
    NW, NS, NSR, NLR, L, LAG = d.NW, d.NS, d.NSR, d.NLR, d.L, d.LAG
    A4 = 4 * d.heads
    me = lax.axis_index("dp")
    z = me // 2
    c = me % 2
    right, left, sib = me + 2, me - 2, z * 2 + (1 - c)
    has_r = z < n - 1
    has_l = z > 0
    seq_len = len_ref[0]

    def rcopy(src, dst, ss, rs, dev):
        return pltpu.make_async_remote_copy(
            src_ref=src,
            dst_ref=dst,
            send_sem=ss,
            recv_sem=rs,
            device_id={"dp": dev},
            device_id_type=MESH,
        )

    def signal(sem, dev):
        pl.semaphore_signal(sem, inc=1, device_id={"dp": dev}, device_id_type=MESH)

    def aidx(u):
        attn = jnp.where(u % 4 == 3, 2, 0)
        ffn = jnp.where((u - A4) % 2 == 0, 1, 2)
        return jnp.where(u < A4, attn, ffn)

    def ag_first(u):
        slot = u % NW

        @pl.when(u >= NW)
        def _():
            @pl.when(has_r)
            def _():
                pl.semaphore_wait(credit.at[0], 1)

            @pl.when(has_l)
            def _():
                pl.semaphore_wait(credit.at[1], 1)

            pl.semaphore_wait(credit.at[2], 1)

        pltpu.make_async_copy(wl.at[u], W.at[slot, me], own_sem.at[slot]).start()

        @pl.when(has_r)
        def _():
            rcopy(wl.at[u], W.at[slot, me], agR.at[slot, z], ag_recv.at[slot, me], right).start()

        @pl.when(has_l)
        def _():
            rcopy(wl.at[u], W.at[slot, me], agL.at[slot, z], ag_recv.at[slot, me], left).start()

        rcopy(wl.at[u], W.at[slot, me], agS.at[slot, z], ag_recv.at[slot, me], sib).start()

    def ag_tile(slot, sj, sem, dev):
        return rcopy(W.at[slot, sj], W.at[slot, sj], sem, ag_recv.at[slot, sj], dev)

    def ag_relay(u, k):
        slot = u % NW

        @pl.when(z - k >= 0)
        def _():
            j = z - k
            sj = j * 2 + c
            ag_tile(slot, sj, agS.at[slot, j], sib).wait_recv()

            @pl.when(has_r)
            def _():
                ag_tile(slot, sj, agR.at[slot, j], right).start()

            ag_tile(slot, sj, agS.at[slot, j], sib).start()

        @pl.when(z + k <= n - 1)
        def _():
            j = z + k
            sj = j * 2 + c
            ag_tile(slot, sj, agS.at[slot, j], sib).wait_recv()

            @pl.when(has_l)
            def _():
                ag_tile(slot, sj, agL.at[slot, j], left).start()

            ag_tile(slot, sj, agS.at[slot, j], sib).start()

    def ag_step(s):
        @pl.when(s + L < U)
        def _():
            ag_first(s + L)

        for k in range(1, n):
            u = s + L - k

            @pl.when((u >= 0) & (u < U))
            def _(u=u, k=k):
                ag_relay(u, k)

    def ag_wait(u):
        slot = u % NW
        pltpu.make_async_copy(wl.at[u], W.at[slot, me], own_sem.at[slot]).wait()
        for j in range(n):
            ag_tile(slot, j * 2 + 1 - c, agS.at[slot, j], sib).wait_recv()

    def ag_finish(u):
        slot = u % NW
        for j in range(n):

            @pl.when(has_r & (j <= z))
            def _(j=j):
                ag_tile(slot, j * 2 + c, agR.at[slot, j], right).wait_send()

            @pl.when(has_l & (j >= z))
            def _(j=j):
                ag_tile(slot, j * 2 + c, agL.at[slot, j], left).wait_send()

            ag_tile(slot, j * 2 + c, agS.at[slot, j], sib).wait_send()

        @pl.when(u + NW < U)
        def _():
            @pl.when(has_r)
            def _():
                signal(credit.at[1], right)

            @pl.when(has_l)
            def _():
                signal(credit.at[0], left)

            signal(credit.at[2], sib)

    def sb_copy(u):
        return rcopy(
            SB.at[u % 2], SR.at[u % NSR], sb_sem.at[u % 2], sr_sem.at[u % NSR], sib
        )

    def ls_copy(v, zt, to_right):
        slot = zt + 1 if to_right else zt
        return rcopy(
            S.at[v % NS, zt],
            LR.at[v % NLR, slot],
            ls_sem.at[v % NS, zt],
            lr_sem.at[v % NLR, slot],
            right if to_right else left,
        )

    def dw_half(u, core, put):
        a = aidx(u)
        g = G[u % 4]
        for j in range(n):
            put(j, dot(At[a, core, j * Dsl : (j + 1) * Dsl, :], g).astype(BF16))

    def dw_sib(u):
        @pl.when(u >= 2)
        def _():
            sb_copy(u - 2).wait_send()

        def put(j, v):
            SB[u % 2, j] = v

        dw_half(u, 1 - c, put)
        sb_copy(u).start()

    def rs_finish(v):
        for zt in range(n):

            @pl.when(zt != z)
            def _(zt=zt):
                ls_copy(v, zt, True).wait_send()

    def dw_own(u):
        @pl.when(u >= NS)
        def _():
            rs_finish(u - NS)

        def put(j, v):
            S[u % NS, j] = v

        dw_half(u, c, put)

    def add_into(v, zt, other):
        S[v % NS, zt] = (S[v % NS, zt].astype(F32) + other.astype(F32)).astype(BF16)

    def combine(v):
        sb_copy(v).wait_recv()
        for zt in range(n):
            add_into(v, zt, SR[v % NSR, zt])

    def send_right(v):
        for zt in range(1, n):

            @pl.when(zt > z)
            def _(zt=zt):
                @pl.when(has_l)
                def _():
                    ls_copy(v, zt, True).wait_recv()
                    add_into(v, zt, LR[v % NLR, zt + 1])

                ls_copy(v, zt, True).start()

    def send_left(v):
        for zt in range(0, n - 1):

            @pl.when(zt < z)
            def _(zt=zt):
                @pl.when(has_r)
                def _():
                    ls_copy(v, zt, False).wait_recv()
                    add_into(v, zt, LR[v % NLR, zt])

                ls_copy(v, zt, False).start()

    def out_copy(v):
        return pltpu.make_async_copy(stage.at[v % 2], dw_hbm.at[v], out_sem.at[v % 2])

    def final(v):
        @pl.when(v >= 2)
        def _():
            out_copy(v - 2).wait()

        slot = v % 2
        stage[slot] = S[v % NS, z].astype(F32)

        @pl.when(has_l)
        def _():
            ls_copy(v, z, True).wait_recv()
            stage[slot] += LR[v % NLR, z + 1].astype(F32)

        @pl.when(has_r)
        def _():
            ls_copy(v, z, False).wait_recv()
            stage[slot] += LR[v % NLR, z].astype(F32)

        out_copy(v).start()

    def rs_step(s):
        base = s - LAG - 1

        def guarded(v, f):
            @pl.when((v >= 0) & (v < U))
            def _():
                f(v)

        guarded(base, combine)
        guarded(base - z, send_right)
        guarded(base - (n - 1 - z), send_left)
        guarded(base - jnp.maximum(z, n - 1 - z), final)

    def layer_norm(x):
        mean = jnp.mean(x, axis=-1, keepdims=True)
        cen = x - mean
        inv = lax.rsqrt(jnp.mean(cen * cen, axis=-1, keepdims=True) + norm_eps)
        return cen * inv

    def ln_block(i):
        rows = ds(i, ROWS)
        normed = layer_norm(X[rows, :].astype(F32))
        A[0, rows, :] = (normed * norm_ref[0:1, :] + norm_ref[1:2, :]).astype(BF16)
        A[1, rows, :] = (normed * norm_ref[2:3, :] + norm_ref[3:4, :]).astype(BF16)
        pos = lax.broadcasted_iota(jnp.int32, (ROWS, D), 0) + i * ROWS
        grad = jnp.where(pos < seq_len, A[2, rows, :].astype(F32), 0.0)
        A[2, rows, :] = grad.astype(BF16)
        small_ref[4:5, :] += jnp.sum(grad, axis=0, keepdims=True)
        for a in range(3):
            for j in range(2 * n):
                At[a, j % 2, (j // 2) * Dsl : (j // 2 + 1) * Dsl, rows] = jnp.transpose(
                    A[a, rows, j * Dsl : (j + 1) * Dsl]
                )
            Acc[a, rows, :] = jnp.zeros((ROWS, D), F32)

    def y_step(u):
        ag_wait(u)
        w = W[u % NW].reshape(D, UNIT)
        Y[u % 4] = dot(A[aidx(u)], w)

    def acc_step(u):
        a = aidx(u)
        g = G[u % 4]
        for j in range(2 * n):
            cols = slice(j * Dsl, (j + 1) * Dsl)
            Acc[a, :, cols] += dot_nt(g, W[u % NW, j])

    lane = lax.broadcasted_iota(jnp.int32, (T, 128), 1)

    def rotate(y, sign):
        lo = y[:, :128]
        swapped = jnp.where(lane < 32, pltpu.roll(lo, 96, 1), pltpu.roll(lo, 32, 1))
        lo = lo * rope_ref[0] + swapped * (rope_ref[1] * sign)
        return jnp.concatenate([lo, y[:, 128:]], axis=1)

    def attn_core(s):
        u0 = s - 3
        QK[0] = rotate(Y[0] + bias_ref[u0, 0:1, :], 1.0).astype(BF16)
        QK[1] = rotate(Y[1] + bias_ref[u0 + 1, 0:1, :], 1.0).astype(BF16)
        QK[2] = (Y[2] + bias_ref[u0 + 2, 0:1, :]).astype(BF16)
        QK[3] = Y[3].astype(BF16)
        scale = 1.0 / math.sqrt(HD)

        def block(i, carry):
            rows = ds(i, ROWS)
            raw = dot_nt(QK[0, rows, :], QK[1]) * scale
            qpos = lax.broadcasted_iota(jnp.int32, (ROWS, T), 0) + i * ROWS
            kpos = lax.broadcasted_iota(jnp.int32, (ROWS, T), 1)
            scores = jnp.where((kpos <= qpos) & (kpos < seq_len), raw, -jnp.inf)
            top = jnp.max(scores, axis=-1, keepdims=True)
            e = jnp.exp(scores - top)
            p = e / jnp.sum(e, axis=-1, keepdims=True)
            pb = p.astype(BF16)
            PB[rows, :] = pb
            mixed = dot(pb, QK[2]).astype(BF16)
            G[3, rows, :] = mixed
            mg = QK[3, rows, :]
            delta = jnp.sum(mg.astype(F32) * mixed.astype(F32), axis=-1, keepdims=True)
            dp = dot_nt(mg, QK[2])
            dsb = (p * (dp - delta) * scale).astype(BF16)
            DS[rows, :] = dsb
            Y[0, rows, :] = dot(dsb, QK[1])
            return carry

        lax.fori_loop(0, T // ROWS, block, 0)
        Y[1] = dot_tn(DS[...], QK[0])
        for r in range(3):
            if r == 2:
                g = dot_tn(PB[...], QK[3])
            else:
                g = rotate(Y[r], -1.0)
            bg_ref[u0 + r] = jnp.broadcast_to(jnp.sum(g, axis=0, keepdims=True), (8, UNIT))
            G[r] = g.astype(BF16)

    def ffn_core(s):
        b = bias_ref[s - 1, 0:1, :]
        yu, yd = (s - 1) % 4, s % 4
        step = 64

        def block(i, total):
            rows = ds(i, step)
            v = Y[yu, rows, :] + b
            cdf2 = 1.0 + lax.erf(v * (1.0 / math.sqrt(2.0)))
            G[yd, rows, :] = (0.5 * v * cdf2).astype(BF16)
            slope = 0.5 * cdf2 + v * jnp.exp(-0.5 * v * v) * (1.0 / math.sqrt(2.0 * math.pi))
            g = Y[yd, rows, :] * slope
            G[yu, rows, :] = g.astype(BF16)
            return total + jnp.sum(g, axis=0, keepdims=True)

        total = lax.fori_loop(0, T // step, block, jnp.zeros((1, UNIT), F32))
        bg_ref[s - 1] = jnp.broadcast_to(total, (8, UNIT))

    barrier = pltpu.get_barrier_semaphore()

    @pl.when(has_r)
    def _():
        signal(barrier, right)

    @pl.when(has_l)
    def _():
        signal(barrier, left)

    signal(barrier, sib)
    peers = 1 + jnp.minimum(z, 1) + jnp.minimum(n - 1 - z, 1)
    pl.semaphore_wait(barrier, peers)

    x_in = pltpu.make_async_copy(x_hbm, X, in_sem.at[0])
    c_in = pltpu.make_async_copy(cot_hbm, A.at[2], in_sem.at[1])
    x_in.start()
    c_in.start()
    ag_step(-L)
    small_ref[...] = jnp.zeros_like(small_ref)
    bg_ref[...] = jnp.zeros_like(bg_ref)
    x_in.wait()
    c_in.wait()
    blocks = T // ROWS

    def fill(i, carry):
        @pl.when(i < blocks)
        def _():
            ln_block(i)

        @pl.when(i < L - 1)
        def _():
            ag_step(i + 1 - L)

        return carry

    lax.fori_loop(0, max(L - 1, blocks), fill, 0)

    def body(s, carry):
        ag_step(s)

        @pl.when(s < U)
        def _():
            y_step(s)

        @pl.when((s < A4) & (s % 4 == 3))
        def _():
            attn_core(s)

        @pl.when((s >= A4) & (s < U) & ((s - A4) % 2 == 1))
        def _():
            ffn_core(s)

        u = s - LAG

        @pl.when((u >= 0) & (u < U))
        def _():
            dw_sib(u)

        rs_step(s)

        @pl.when((u >= 0) & (u < U))
        def _():
            dw_own(u)
            acc_step(u)

        @pl.when((u >= 1) & (u < U + 1))
        def _():
            ag_finish(u - 1)

        return carry

    lax.fori_loop(0, U + LAG + n, body, 0)

    def tail(i, carry):
        rows = ds(i, ROWS)
        normed = layer_norm(X[rows, :].astype(F32))
        ab = Acc[0, rows, :]
        fb = Acc[1, rows, :]
        small_ref[0:1, :] += jnp.sum(ab * normed, axis=0, keepdims=True)
        small_ref[1:2, :] += jnp.sum(ab, axis=0, keepdims=True)
        small_ref[2:3, :] += jnp.sum(fb * normed, axis=0, keepdims=True)
        small_ref[3:4, :] += jnp.sum(fb, axis=0, keepdims=True)
        A[1, rows, :] = (ab * norm_ref[0:1, :] + fb * norm_ref[2:3, :]).astype(BF16)
        A[0, rows, :] = Acc[2, rows, :].astype(BF16)
        return carry

    lax.fori_loop(0, blocks, tail, 0)
    copies = [
        pltpu.make_async_copy(A.at[i], part_hbm.at[i], in_sem.at[i]) for i in range(2)
    ]
    for cp in copies:
        cp.start()
    for v in range(max(0, U - NS), U):
        rs_finish(v)
    for v in range(max(0, U - 2), U):
        sb_copy(v).wait_send()
        out_copy(v).wait()
    for cp in copies:
        cp.wait()


def run_layer(d, seq_len, x, cot, wl, norms, bias, rope):
    n, T, D, Dsl, U = d.n, d.T, d.D, d.Dsl, d.U
    dma = pltpu.SemaphoreType.DMA
    vm = pl.BlockSpec(memory_space=pltpu.VMEM)
    hbm = pl.BlockSpec(memory_space=pl.ANY)
    flops = 6 * U * T * D * UNIT
    return pl.pallas_call(
        functools.partial(layer_kernel, d),
        out_shape=(
            jax.ShapeDtypeStruct((2, T, D), BF16),
            jax.ShapeDtypeStruct((U, Dsl, UNIT), F32),
            jax.ShapeDtypeStruct((8, D), F32),
            jax.ShapeDtypeStruct((U, 8, UNIT), F32),
        ),
        in_specs=[pl.BlockSpec(memory_space=pltpu.SMEM), hbm, hbm, hbm, vm, vm, vm],
        out_specs=(hbm, hbm, vm, vm),
        scratch_shapes=[
            pltpu.VMEM((d.NW, 2 * n, Dsl, UNIT), BF16),
            pltpu.VMEM((3, T, D), BF16),
            pltpu.VMEM((3, 2, n * Dsl, T), BF16),
            pltpu.VMEM((T, D), BF16),
            pltpu.VMEM((3, T, D), F32),
            pltpu.VMEM((4, T, UNIT), F32),
            pltpu.VMEM((4, T, UNIT), BF16),
            pltpu.VMEM((4, T, UNIT), BF16),
            pltpu.VMEM((T, T), BF16),
            pltpu.VMEM((T, T), BF16),
            pltpu.VMEM((d.NS, n, Dsl, UNIT), BF16),
            pltpu.VMEM((2, n, Dsl, UNIT), BF16),
            pltpu.VMEM((d.NSR, n, Dsl, UNIT), BF16),
            pltpu.VMEM((d.NLR, n + 1, Dsl, UNIT), BF16),
            pltpu.VMEM((2, Dsl, UNIT), F32),
            dma((2,)),
            dma((d.NW,)),
            dma((d.NW, 2 * n)),
            dma((d.NW, n)),
            dma((d.NW, n)),
            dma((d.NW, n)),
            pltpu.SemaphoreType.REGULAR((3,)),
            dma((2,)),
            dma((d.NSR,)),
            dma((d.NS, n)),
            dma((d.NLR, n + 1)),
            dma((2,)),
        ],
        compiler_params=pltpu.CompilerParams(
            collective_id=0, has_side_effects=True, vmem_limit_bytes=67_000_000
        ),
        cost_estimate=pl.CostEstimate(
            flops=flops, bytes_accessed=4 * U * Dsl * UNIT * 8, transcendentals=T * UNIT * U
        ),
    )(seq_len, x, cot, wl, norms, bias, rope)


def rope_pair(rows):
    half = ROT // 2
    freq_idx = jnp.arange(half, dtype=F32)
    inv_freq = jnp.exp(-(2.0 * freq_idx / ROT) * math.log(rope_base))
    angles = jnp.arange(rows, dtype=F32)[:, None] * inv_freq[None, :]
    cosine, sine = jnp.cos(angles), jnp.sin(angles)
    rest = 128 - ROT
    return jnp.stack(
        [
            jnp.concatenate([cosine, cosine, jnp.ones((rows, rest), F32)], axis=1),
            jnp.concatenate([-sine, sine, jnp.zeros((rows, rest), F32)], axis=1),
        ]
    )


def per_device(
    n_dp,
    block_input,
    cotangent,
    lengths,
    attn_gain,
    attn_shift,
    ffn_gain,
    ffn_shift,
    qkv_weight,
    qkv_bias,
    out_weight,
    out_bias,
    up_weight,
    up_bias,
    down_weight,
):
    T, D = block_input.shape
    n = n_dp // 2
    Dsl = D // n_dp
    width = qkv_weight.shape[2]
    heads = width // HD
    hidden = up_weight.shape[1]
    chunks = hidden // UNIT
    U = 4 * heads + 2 * chunks
    L, LAG = n + 1, 3
    d = types.SimpleNamespace(
        n=n, T=T, D=D, Dsl=Dsl, U=U, heads=heads, chunks=chunks, L=L, LAG=LAG,
        NW=min(U, L + LAG + 6), NS=min(U, n + 3), NSR=4, NLR=n + 2,
    )

    nb, ub = qkv_bias.shape[1], up_bias.shape[0]
    packed = jnp.concatenate(
        [attn_gain, attn_shift, ffn_gain, ffn_shift, out_bias, qkv_bias.reshape(-1), up_bias]
    )
    packed = lax.all_gather(packed, "dp", axis=0).astype(F32)
    norm_rows = [packed[:, i * Dsl : (i + 1) * Dsl].reshape(D) for i in range(5)]
    outb_full = norm_rows[4]
    qkv_b = packed[:, 5 * Dsl : 5 * Dsl + 3 * nb].reshape(n_dp, 3, nb)
    qkv_b = qkv_b.transpose(1, 0, 2).reshape(3, heads, HD)
    up_b = packed[:, 5 * Dsl + 3 * nb :].reshape(chunks, UNIT)
    norms = jnp.stack(norm_rows[:4] + [jnp.zeros((D,), F32)] * 4)
    bias = jnp.concatenate(
        [
            jnp.concatenate(
                [qkv_b.transpose(1, 0, 2), jnp.zeros((heads, 1, UNIT), F32)], axis=1
            ).reshape(4 * heads, UNIT),
            jnp.stack([up_b, jnp.zeros_like(up_b)], axis=1).reshape(2 * chunks, UNIT),
        ]
    )
    bias = jnp.broadcast_to(bias[:, None, :], (U, 8, UNIT))

    qkv_u = qkv_weight.reshape(3, Dsl, heads, UNIT).transpose(2, 0, 1, 3)
    out_u = out_weight.reshape(heads, 1, UNIT, Dsl).transpose(0, 1, 3, 2)
    up_u = up_weight.reshape(Dsl, chunks, 1, UNIT).transpose(1, 2, 0, 3)
    down_u = down_weight.reshape(chunks, 1, UNIT, Dsl).transpose(0, 1, 3, 2)
    wl = jnp.concatenate(
        [
            jnp.concatenate([qkv_u, out_u], axis=1).reshape(4 * heads, Dsl, UNIT),
            jnp.concatenate([up_u, down_u], axis=1).reshape(2 * chunks, Dsl, UNIT),
        ]
    )

    part, dw, small, bg = run_layer(
        d, lengths, block_input, cotangent, wl, norms, bias, rope_pair(T)
    )

    part = lax.psum(part, "tensor").astype(F32)
    stats = lax.psum(small[:4], "tensor")
    x_rows = block_input.astype(F32)
    block_output = (x_rows + part[0] + outb_full).astype(BF16)
    mean = jnp.mean(x_rows, axis=-1, keepdims=True)
    centered = x_rows - mean
    inv_std = lax.rsqrt(jnp.mean(centered * centered, axis=-1, keepdims=True) + norm_eps)
    normed = centered * inv_std
    row_valid = (jnp.arange(T, dtype=jnp.int32) < lengths[0]).astype(F32)[:, None]
    grad_rows = cotangent.astype(F32) * row_valid
    norm_grad = part[1]
    grad_mean = jnp.mean(norm_grad, axis=-1, keepdims=True)
    grad_proj = jnp.mean(norm_grad * normed, axis=-1, keepdims=True)
    dblock_input = (grad_rows + inv_std * (norm_grad - grad_mean - normed * grad_proj)).astype(BF16)

    dqkv_b = bg[: 4 * heads, 0].reshape(heads, 4, UNIT)[:, :3].transpose(1, 0, 2)
    dup_b = bg[4 * heads :, 0].reshape(chunks, 2, UNIT)[:, 0].reshape(hidden)
    sent = jnp.concatenate(
        [
            stats.reshape(4, n_dp, Dsl).transpose(1, 0, 2).reshape(n_dp, 4 * Dsl),
            small[4].reshape(n_dp, Dsl),
            dqkv_b.reshape(3, n_dp, nb).transpose(1, 0, 2).reshape(n_dp, 3 * nb),
            dup_b.reshape(n_dp, ub),
        ],
        axis=1,
    )
    sent = lax.psum_scatter(sent, "dp", scatter_dimension=0, tiled=False)
    stats_s = sent[: 4 * Dsl].reshape(4, Dsl)
    doutb = sent[4 * Dsl : 5 * Dsl]
    dqkvb = sent[5 * Dsl : 5 * Dsl + 3 * nb].reshape(3, nb)
    dupb = sent[5 * Dsl + 3 * nb :]

    dwa = dw[: 4 * heads].reshape(heads, 4, Dsl, UNIT)
    dwf = dw[4 * heads :].reshape(chunks, 2, Dsl, UNIT)
    dqkv = dwa[:, :3].transpose(1, 2, 0, 3).reshape(3, Dsl, width)
    dout = dwa[:, 3].transpose(0, 2, 1).reshape(width, Dsl)
    dup = dwf[:, 0].transpose(1, 0, 2).reshape(Dsl, hidden)
    ddown = dwf[:, 1].transpose(0, 2, 1).reshape(hidden, Dsl)
    return (
        block_output,
        dblock_input,
        stats_s[0],
        stats_s[1],
        stats_s[2],
        stats_s[3],
        dqkv,
        dqkvb,
        dout,
        doutb,
        dup,
        dupb,
        ddown,
    )


def solution(mesh):
    in_specs = (
        P("dp", None),
        P("dp", None),
        P("dp"),
        P("dp"),
        P("dp"),
        P("dp"),
        P("dp"),
        P(None, "dp", "tensor"),
        P(None, ("tensor", "dp")),
        P("tensor", "dp"),
        P("dp"),
        P("dp", "tensor"),
        P(("tensor", "dp")),
        P("tensor", "dp"),
    )
    out_specs = (
        P("dp", None),
        P("dp", None),
        P("dp"),
        P("dp"),
        P("dp"),
        P("dp"),
        P(None, "dp", "tensor"),
        P(None, ("tensor", "dp")),
        P("tensor", "dp"),
        P("dp"),
        P("dp", "tensor"),
        P(("tensor", "dp")),
        P("tensor", "dp"),
    )
    return jax.shard_map(
        functools.partial(per_device, mesh.shape["dp"]),
        mesh=mesh,
        in_specs=in_specs,
        out_specs=out_specs,
        check_vma=False,
    )
```

```python
import functools
import math
import types

import jax
import jax.numpy as jnp
from jax import lax
from jax.experimental import pallas as pl
from jax.experimental.pallas import tpu as pltpu
from jax.sharding import PartitionSpec as P

HD = 256
ROT = 64
UNIT = 256
ROWS = 128
MESH = pl.DeviceIdType.MESH

norm_eps = 1e-05
rope_base = 10000.0

F32 = jnp.float32
BF16 = jnp.bfloat16


def dot(a, b):
    return lax.dot_general(a, b, (((1,), (0,)), ((), ())), preferred_element_type=F32)


def dot_nt(a, b):
    return lax.dot_general(a, b, (((1,), (1,)), ((), ())), preferred_element_type=F32)


def dot_tn(a, b):
    return lax.dot_general(a, b, (((0,), (0,)), ((), ())), preferred_element_type=F32)


def ds(i, size):
    return pl.ds(pl.multiple_of(i * size, size), size)


def layer_kernel(
    d,
    len_ref,
    sp_ref,
    rope_ref,
    x_hbm,
    cot_hbm,
    wqkv,
    wout,
    wup,
    wdown,
    o_hbm,
    dx_hbm,
    dqkv_hbm,
    dout_hbm,
    dup_hbm,
    ddown_hbm,
    pr_hbm,
    so_ref,
    sb_ref,
    W,
    A,
    At,
    Acc,
    Y,
    G,
    QK,
    PB,
    DS,
    S,
    DL,
    DR,
    SB,
    SR,
    LR,
    stage,
    stage_t,
    OT,
    RP,
    NB,
    BI,
    SM,
    BG,
    BGC,
    RS1,
    RB2,
    ST,
    RT,
    in_sem,
    own_sem,
    ag_recv,
    agR,
    agL,
    agS,
    credit,
    lcredit,
    ready,
    sb_sem,
    sr_sem,
    ls_sem,
    lr_sem,
    out_sem,
    sp_s,
    sp_r,
    sm_s,
    sm_r,
    st_s,
    st_r,
    pr_s,
    pr_r,
    fo_s,
    fo_r,
    loc_sem,
    raw_sem,
):
    n, tn, T, D, Dsl, U, heads = d.n, d.tn, d.T, d.D, d.Dsl, d.U, d.heads
    n_dp, NW, NS, NSR, NLR, LAG = 2 * d.n, d.NW, d.NS, d.NSR, d.NLR, d.LAG
    E, ES, E0 = d.E, d.ES, d.E0
    Tr = T // tn
    A4 = 4 * heads
    chunks = d.chunks
    me = lax.axis_index("dp")
    mt = lax.axis_index("tensor")
    z = me // 2
    c = me % 2
    right, left, sib = me + 2, me - 2, z * 2 + (1 - c)
    has_r = z < n - 1
    has_l = z > 0
    seq_len = len_ref[0]

    def rcopy_to(src, dst, ss, rs, where):
        return pltpu.make_async_remote_copy(
            src_ref=src,
            dst_ref=dst,
            send_sem=ss,
            recv_sem=rs,
            device_id=where,
            device_id_type=MESH,
        )

    def rcopy(src, dst, ss, rs, dev):
        return rcopy_to(src, dst, ss, rs, {"dp": dev})

    def signal(sem, dev, axis="dp"):
        pl.semaphore_signal(sem, inc=1, device_id={axis: dev}, device_id_type=MESH)

    def aidx(u):
        attn = jnp.where(u % 4 == 3, 2, 0)
        ffn = jnp.where((u - A4) % 2 == 0, 1, 2)
        return jnp.where(u < A4, attn, ffn)

    def each_dp(f):
        for p in range(n_dp):

            @pl.when(p != me)
            def _(p=p):
                f(p)

    def each_tensor(f):
        for p in range(tn):

            @pl.when(p != mt)
            def _(p=p):
                f(p)

    def own_tile(u, f):
        @pl.when((u < A4) & (u % 4 != 3))
        def _():
            f(wqkv.at[u % 4, :, ds(u // 4, UNIT)])

        @pl.when((u < A4) & (u % 4 == 3))
        def _():
            f(OT.at[u // 4])

        @pl.when((u >= A4) & (u % 2 == 0))
        def _():
            f(wup.at[:, ds((u - A4) // 2, UNIT)])

        @pl.when((u >= A4) & (u % 2 == 1))
        def _():
            f(OT.at[heads + (u - A4) // 2])

    def ag_tile(slot, sj, sem, dev):
        return rcopy(W.at[slot, sj], W.at[slot, sj], sem, ag_recv.at[slot, sj], dev)

    def ag_self(u):
        slot = u % NW

        @pl.when(u >= NW)
        def _():
            pl.semaphore_wait(credit.at[2], 1)

        def go(src):
            pltpu.make_async_copy(src, W.at[slot, me], own_sem.at[slot]).start()
            rcopy(src, W.at[slot, me], agS.at[slot, z], ag_recv.at[slot, me], sib).start()

        own_tile(u, go)

    def relay(u, j, has_next, sems, dev):
        slot = u % NW
        sj = j * 2 + c
        ag_tile(slot, sj, agS.at[slot, j], sib).wait_recv()

        @pl.when(has_next)
        def _():
            ag_tile(slot, sj, sems.at[slot, j], dev).start()

        ag_tile(slot, sj, agS.at[slot, j], sib).start()

    def ag_line(u, has_next, credit_sem, sems, dev, sign):
        slot = u % NW

        @pl.when(has_next)
        def _():
            @pl.when(u >= NW)
            def _():
                pl.semaphore_wait(credit_sem, 1)

            def go(src):
                rcopy(src, W.at[slot, me], sems.at[slot, z], ag_recv.at[slot, me], dev).start()

            own_tile(u, go)

        for k in range(1, n):
            j = z + sign * k

            @pl.when((j >= 0) & (j < n))
            def _(j=j):
                relay(u, j, has_next, sems, dev)

    def guarded(v, f):
        @pl.when((v >= 0) & (v < U))
        def _():
            f(v)

    def ag_step(s):
        guarded(s + ES, ag_self)
        guarded(
            s + E + d.gap * (n - 1 - z),
            lambda u: ag_line(u, has_r, credit.at[0], agR, right, -1),
        )
        guarded(s + E + d.gap * z, lambda u: ag_line(u, has_l, credit.at[1], agL, left, 1))

    def ag_wait(u):
        slot = u % NW
        pltpu.make_async_copy(OT.at[0], W.at[slot, me], own_sem.at[slot]).wait()
        for j in range(n):
            ag_tile(slot, j * 2 + 1 - c, agS.at[slot, j], sib).wait_recv()

    def ag_finish(u):
        slot = u % NW
        for j in range(n):

            @pl.when(has_r & (j <= z))
            def _(j=j):
                ag_tile(slot, j * 2 + c, agR.at[slot, j], right).wait_send()

            @pl.when(has_l & (j >= z))
            def _(j=j):
                ag_tile(slot, j * 2 + c, agL.at[slot, j], left).wait_send()

            ag_tile(slot, j * 2 + c, agS.at[slot, j], sib).wait_send()

        @pl.when(u + NW < U)
        def _():
            @pl.when(has_r)
            def _():
                signal(credit.at[1], right)

            @pl.when(has_l)
            def _():
                signal(credit.at[0], left)

            signal(credit.at[2], sib)

    def part_ref(v, zt):
        if zt == 0:
            return DL.at[v]
        if zt == n - 1:
            return DR.at[v]
        return S.at[v % NS, zt - 1]

    def sb_copy(u):
        return rcopy(SB.at[u % 2], SR.at[u % NSR], sb_sem.at[u % 2], sr_sem.at[u % NSR], sib)

    def ls_copy(v, zt, to_right):
        slot = zt if to_right else zt - 1
        return rcopy(
            S.at[v % NS, zt - 1],
            LR.at[v % NLR, slot],
            ls_sem.at[v % NS, zt - 1],
            lr_sem.at[v % NLR, slot],
            right if to_right else left,
        )

    def dw_half(u, core, put):
        a = aidx(u)
        g = G[u % 4]
        for j in range(n):
            put(j, dot(At[a, core, j * Dsl : (j + 1) * Dsl, :], g).astype(BF16))

    def dw_sib(u):
        @pl.when(u >= 2)
        def _():
            sb_copy(u - 2).wait_send()

        def put(j, v):
            SB[u % 2, j] = v

        dw_half(u, 1 - c, put)
        sb_copy(u).start()

    def rs_finish(v):
        for zt in range(1, n - 1):

            @pl.when(zt != z)
            def _(zt=zt):
                ls_copy(v, zt, True).wait_send()

    def dw_own(u):
        @pl.when(u >= NS)
        def _():
            rs_finish(u - NS)

        def put(j, v):
            part_ref(u, j)[...] = v

        dw_half(u, c, put)

    def add_into(ref, other):
        ref[...] = (ref[...].astype(F32) + other[...].astype(F32)).astype(BF16)

    def combine(v):
        sb_copy(v).wait_recv()
        for zt in range(n):
            add_into(part_ref(v, zt), SR.at[v % NSR, zt])

    def send_right(v):
        @pl.when((z + 1 <= n - 2) & (v >= NLR))
        def _():
            pl.semaphore_wait(lcredit.at[0], 1)

        for zt in range(1, n - 1):

            @pl.when(zt > z)
            def _(zt=zt):
                @pl.when(has_l)
                def _():
                    ls_copy(v, zt, True).wait_recv()
                    add_into(S.at[v % NS, zt - 1], LR.at[v % NLR, zt])

                ls_copy(v, zt, True).start()

    def send_left(v):
        @pl.when((z - 1 >= 1) & (v >= NLR))
        def _():
            pl.semaphore_wait(lcredit.at[1], 1)

        for zt in range(1, n - 1):

            @pl.when(zt < z)
            def _(zt=zt):
                @pl.when(has_r)
                def _():
                    ls_copy(v, zt, False).wait_recv()
                    add_into(S.at[v % NS, zt - 1], LR.at[v % NLR, zt - 1])

                ls_copy(v, zt, False).start()

    def out_wait(v):
        pltpu.make_async_copy(
            stage.at[v % 2], dup_hbm.at[:, 0:UNIT], out_sem.at[v % 2]
        ).wait()

    def out_start(v):
        slot = v % 2
        sem = out_sem.at[slot]

        @pl.when((v < A4) & (v % 4 != 3))
        def _():
            pltpu.make_async_copy(
                stage.at[slot], dqkv_hbm.at[v % 4, :, ds(v // 4, UNIT)], sem
            ).start()

        @pl.when((v >= A4) & (v % 2 == 0))
        def _():
            pltpu.make_async_copy(
                stage.at[slot], dup_hbm.at[:, ds((v - A4) // 2, UNIT)], sem
            ).start()

        @pl.when(((v < A4) & (v % 4 == 3)) | ((v >= A4) & (v % 2 == 1)))
        def _():
            stage_t[slot] = jnp.transpose(stage[slot])

            @pl.when(v < A4)
            def _():
                pltpu.make_async_copy(
                    stage_t.at[slot], dout_hbm.at[ds(v // 4, UNIT), :], sem
                ).start()

            @pl.when(v >= A4)
            def _():
                pltpu.make_async_copy(
                    stage_t.at[slot], ddown_hbm.at[ds((v - A4) // 2, UNIT), :], sem
                ).start()

    def final(v):
        @pl.when((z >= 1) & (z <= n - 2))
        def _():
            @pl.when(v >= 2)
            def _():
                out_wait(v - 2)

            slot = v % 2
            ls_copy(v, z, True).wait_recv()
            ls_copy(v, z, False).wait_recv()
            stage[slot] = (
                S[v % NS, z - 1].astype(F32)
                + LR[v % NLR, z].astype(F32)
                + LR[v % NLR, z - 1].astype(F32)
            )
            out_start(v)

            @pl.when(v + NLR < U)
            def _():
                signal(lcredit.at[0], left)
                signal(lcredit.at[1], right)

    def rs_step(s):
        base = s - LAG - 1
        guarded(base, combine)
        guarded(base - z, send_right)
        guarded(base - (n - 1 - z), send_left)
        guarded(base - jnp.maximum(z, n - 1 - z), final)

    def p2_slot(i):
        return W.at[i // n_dp, i % n_dp], ag_recv.at[i // n_dp, i % n_dp]

    def p2_copy(u, to_right):
        dst, rs = p2_slot(u if to_right else U + u)
        src = DR.at[u] if to_right else DL.at[u]
        sems = agR if to_right else agL
        return rcopy(src, dst, sems.at[u // n, u % n], rs, right if to_right else left)

    def p2_side(u, to_right):
        has_prev, has_next = (has_l, has_r) if to_right else (has_r, has_l)
        mine = DR.at[u] if to_right else DL.at[u]
        got, _ = p2_slot(u if to_right else U + u)
        cp = p2_copy(u, to_right)

        @pl.when(has_prev)
        def _():
            cp.wait_recv()

        @pl.when(has_next)
        def _():
            @pl.when(has_prev)
            def _():
                add_into(mine, got)

            cp.start()

        @pl.when(jnp.logical_not(has_next))
        def _():
            @pl.when(u >= 2)
            def _():
                out_wait(u - 2)

            stage[u % 2] = mine[...].astype(F32) + got[...].astype(F32)
            out_start(u)

    def p2_step(i):
        guarded(i - z, lambda u: p2_side(u, True))
        guarded(i - (n - 1 - z), lambda u: p2_side(u, False))

    def layer_norm(x):
        mean = jnp.mean(x, axis=-1, keepdims=True)
        cen = x - mean
        inv = lax.rsqrt(jnp.mean(cen * cen, axis=-1, keepdims=True) + norm_eps)
        return cen * inv, inv

    def ln_block(i):
        rows = ds(i, ROWS)
        normed, _ = layer_norm(A[0, rows, :].astype(F32))
        A[0, rows, :] = (normed * NB[0:1, :] + NB[1:2, :]).astype(BF16)
        A[1, rows, :] = (normed * NB[2:3, :] + NB[3:4, :]).astype(BF16)
        pos = lax.broadcasted_iota(jnp.int32, (ROWS, D), 0) + i * ROWS
        grad = jnp.where(pos < seq_len, A[2, rows, :].astype(F32), 0.0)
        A[2, rows, :] = grad.astype(BF16)
        SM[4:5, :] += jnp.sum(grad, axis=0, keepdims=True)
        for a in range(3):
            for j in range(2 * n):
                At[a, j % 2, (j // 2) * Dsl : (j // 2 + 1) * Dsl, rows] = jnp.transpose(
                    A[a, rows, j * Dsl : (j + 1) * Dsl]
                )
            Acc[a, rows, :] = jnp.zeros((ROWS, D), F32)

    def y_step(u):
        ag_wait(u)
        w = W[u % NW].reshape(D, UNIT)
        Y[u % 4] = dot(A[aidx(u)], w)

    def acc_step(u):
        a = aidx(u)
        g = G[u % 4]
        for j in range(2 * n):
            cols = slice(j * Dsl, (j + 1) * Dsl)
            Acc[a, :, cols] += dot_nt(g, W[u % NW, j])

    lane = lax.broadcasted_iota(jnp.int32, (T, 128), 1)

    def rotate(y, sign):
        lo = y[:, :128]
        swapped = jnp.where(lane < 32, pltpu.roll(lo, 96, 1), pltpu.roll(lo, 32, 1))
        lo = lo * rope_ref[0] + swapped * (rope_ref[1] * sign)
        return jnp.concatenate([lo, y[:, 128:]], axis=1)

    def attn_core(s):
        u0 = s - 3
        QK[0] = rotate(Y[0] + BI[u0, 0:1, :], 1.0).astype(BF16)
        QK[1] = rotate(Y[1] + BI[u0 + 1, 0:1, :], 1.0).astype(BF16)
        QK[2] = (Y[2] + BI[u0 + 2, 0:1, :]).astype(BF16)
        QK[3] = Y[3].astype(BF16)
        scale = 1.0 / math.sqrt(HD)

        def block(i, carry):
            rows = ds(i, ROWS)
            raw = dot_nt(QK[0, rows, :], QK[1]) * scale
            qpos = lax.broadcasted_iota(jnp.int32, (ROWS, T), 0) + i * ROWS
            kpos = lax.broadcasted_iota(jnp.int32, (ROWS, T), 1)
            scores = jnp.where((kpos <= qpos) & (kpos < seq_len), raw, -jnp.inf)
            top = jnp.max(scores, axis=-1, keepdims=True)
            e = jnp.exp(scores - top)
            p = e / jnp.sum(e, axis=-1, keepdims=True)
            pb = p.astype(BF16)
            PB[rows, :] = pb
            mixed = dot(pb, QK[2]).astype(BF16)
            G[3, rows, :] = mixed
            mg = QK[3, rows, :]
            delta = jnp.sum(mg.astype(F32) * mixed.astype(F32), axis=-1, keepdims=True)
            dp = dot_nt(mg, QK[2])
            dsb = (p * (dp - delta) * scale).astype(BF16)
            DS[rows, :] = dsb
            Y[0, rows, :] = dot(dsb, QK[1])
            return carry

        lax.fori_loop(0, T // ROWS, block, 0)
        Y[1] = dot_tn(DS[...], QK[0])
        for r in range(3):
            if r == 2:
                g = dot_tn(PB[...], QK[3])
            else:
                g = rotate(Y[r], -1.0)
            BG[u0 + r] = jnp.broadcast_to(jnp.sum(g, axis=0, keepdims=True), (8, UNIT))
            G[r] = g.astype(BF16)

    def ffn_core(s):
        b = BI[s - 1, 0:1, :]
        yu, yd = (s - 1) % 4, s % 4
        step = 64

        def block(i, total):
            rows = ds(i, step)
            v = Y[yu, rows, :] + b
            cdf2 = 1.0 + lax.erf(v * (1.0 / math.sqrt(2.0)))
            G[yd, rows, :] = (0.5 * v * cdf2).astype(BF16)
            slope = 0.5 * cdf2 + v * jnp.exp(-0.5 * v * v) * (1.0 / math.sqrt(2.0 * math.pi))
            g = Y[yd, rows, :] * slope
            G[yu, rows, :] = g.astype(BF16)
            return total + jnp.sum(g, axis=0, keepdims=True)

        total = lax.fori_loop(0, T // step, block, jnp.zeros((1, UNIT), F32))
        BG[s - 1] = jnp.broadcast_to(total, (8, UNIT))

    barrier = pltpu.get_barrier_semaphore()
    each_dp(lambda p: signal(barrier, p))
    each_tensor(lambda p: signal(barrier, p, "tensor"))
    x_in = pltpu.make_async_copy(x_hbm, A.at[0], in_sem.at[0])
    c_in = pltpu.make_async_copy(cot_hbm, A.at[2], in_sem.at[1])
    x_in.start()
    c_in.start()
    spots = [
        buf.at[i, r * UNIT : (r + 1) * UNIT, 0:Dsl]
        for buf in (QK, G)
        for i in range(4)
        for r in range(T // UNIT)
    ]
    raws = [
        pltpu.make_async_copy(
            wout.at[i * UNIT : (i + 1) * UNIT, :]
            if i < heads
            else wdown.at[(i - heads) * UNIT : (i - heads + 1) * UNIT, :],
            spots[i],
            raw_sem.at[i],
        )
        for i in range(heads + chunks)
    ]
    for cp in raws:
        cp.start()
    pl.semaphore_wait(barrier, n_dp - 1 + tn - 1)

    def sp_copy(p, where):
        return rcopy(sp_ref, RP.at[where], sp_s.at[p], sp_r.at[where], p)

    each_dp(lambda p: sp_copy(p, me).start())
    RP[me] = sp_ref[...]

    def early(s, carry):
        ag_step(s)
        return carry

    lax.fori_loop(-E0, 3 - E0, early, 0)
    for i, cp in enumerate(raws):
        cp.wait()
        OT[i] = jnp.transpose(spots[i][...])
    SM[...] = jnp.zeros_like(SM)
    BG[...] = jnp.zeros_like(BG)
    BI[...] = jnp.zeros_like(BI)
    each_dp(lambda p: sp_copy(p, p).wait_recv())
    for p in range(n_dp):
        NB[:, p * Dsl : (p + 1) * Dsl] = RP[p, 0:8, 0:Dsl]
    for i in range(3 * heads + chunks):
        row = RP[0, 8 + i : 9 + i, :]
        for p in range(1, n_dp):
            row = row + RP[p, 8 + i : 9 + i, :]
        u = 4 * (i // 3) + i % 3 if i < 3 * heads else A4 + 2 * (i - 3 * heads)
        BI[u] = jnp.broadcast_to(row, (8, UNIT))
    x_in.wait()
    c_in.wait()
    blocks = T // ROWS

    def fill(i, carry):
        @pl.when(i < blocks)
        def _():
            ln_block(i)

        @pl.when(i < E0 - 3)
        def _():
            ag_step(i + 3 - E0)

        return carry

    lax.fori_loop(0, max(E0 - 3, blocks), fill, 0)

    def body(s, carry):
        ag_step(s)
        guarded(s, y_step)

        @pl.when(s == A4)
        def _():
            x_in.start()

        @pl.when((s < A4) & (s % 4 == 3))
        def _():
            attn_core(s)

        @pl.when((s >= A4) & (s < U) & (s % 2 == 1))
        def _():
            ffn_core(s)

        u = s - LAG
        guarded(u, dw_sib)
        rs_step(s)

        def rest(u):
            dw_own(u)
            acc_step(u)

        guarded(u, rest)
        guarded(u - 1, ag_finish)
        return carry

    lax.fori_loop(0, U + LAG, body, 0)
    ag_finish(U - 1)
    x_in.wait()

    @pl.when(has_r)
    def _():
        signal(ready.at[1], right)

    @pl.when(has_l)
    def _():
        signal(ready.at[0], left)

    def pr_copy(k, i, where):
        return rcopy_to(
            A.at[k, ds(i, Tr), :],
            pr_hbm.at[k, ds(where, Tr), :],
            pr_s.at[k, i],
            pr_r.at[k, where],
            {"tensor": i},
        )

    def part_send(i):
        @pl.when((i >= 0) & (i != mt))
        def _():
            pr_copy(0, i, mt).start()
            pr_copy(1, i, mt).start()

    def partial(i, carry):
        rows = ds(i, Tr)
        normed, _ = layer_norm(A[0, rows, :].astype(F32))
        ab = Acc[0, rows, :]
        fb = Acc[1, rows, :]
        SM[0:1, :] += jnp.sum(ab * normed, axis=0, keepdims=True)
        SM[1:2, :] += jnp.sum(ab, axis=0, keepdims=True)
        SM[2:3, :] += jnp.sum(fb * normed, axis=0, keepdims=True)
        SM[3:4, :] += jnp.sum(fb, axis=0, keepdims=True)
        ng = ab * NB[0:1, :] + fb * NB[2:3, :]
        Acc[0, rows, :] = ng
        @pl.when(i != mt)
        def _():
            A[1, rows, :] = ng.astype(BF16)
            A[0, rows, :] = Acc[2, rows, :].astype(BF16)

        part_send(i - 1)
        return carry

    lax.fori_loop(0, tn, partial, 0)
    for u in range(U):
        BGC[u : u + 1, :] = BG[u, 0:1, :]
    part_send(tn - 1)

    def sm_copy(p, where):
        return rcopy(
            SM.at[:, ds(p, Dsl)], RS1.at[where], sm_s.at[0, p], sm_r.at[0, where], p
        )

    def bg_copy(p, where):
        return rcopy(BGC, RB2.at[where], sm_s.at[1, p], sm_r.at[1, where], p)

    def small_send(p):
        sm_copy(p, me).start()
        bg_copy(p, me).start()

    each_dp(small_send)
    RS1[me] = SM[:, ds(me, Dsl)]
    RB2[me] = BGC[...]

    @pl.when(has_r)
    def _():
        pl.semaphore_wait(ready.at[0], 1)

    @pl.when(has_l)
    def _():
        pl.semaphore_wait(ready.at[1], 1)

    def drain(i, carry):
        @pl.when(i < n)
        def _():
            rs_step(i + U + LAG)

        p2_step(i)
        return carry

    steps = U + n - 1
    middle = min(d.I1, steps)
    lax.fori_loop(0, middle, drain, 0)

    def small_wait(p):
        sm_copy(p, p).wait_recv()
        bg_copy(p, p).wait_recv()

    each_dp(small_wait)
    total = RS1[0]
    bias_total = RB2[0]
    for p in range(1, n_dp):
        total = total + RS1[p]
        bias_total = bias_total + RB2[p]
    sb_ref[...] = bias_total
    ST[...] = total

    def pr_load(k, p):
        rows = ds(p, Tr)
        return pltpu.make_async_copy(
            pr_hbm.at[k, rows, :], A.at[k, rows, :], loc_sem.at[k, p]
        )

    def part_take(p):
        for k in range(2):
            pr_copy(k, p, mt).wait_send()
            pr_copy(k, p, p).wait_recv()
            pr_load(k, p).start()

    each_tensor(part_take)
    own = ds(mt, Tr)

    def part_add(p):
        for k in range(2):
            pr_load(k, p).wait()
            Acc[2 - 2 * k, own, :] += A[k, ds(p, Tr), :].astype(F32)

    each_tensor(part_add)

    def st_copy(p, where):
        return rcopy_to(ST, RT.at[where], st_s.at[p], st_r.at[where], {"tensor": p})

    each_tensor(lambda p: st_copy(p, mt).start())
    xr = A[0, own, :].astype(F32)
    normed, inv = layer_norm(xr)
    ng = Acc[0, own, :]
    gm = jnp.mean(ng, axis=-1, keepdims=True)
    gp = jnp.mean(ng * normed, axis=-1, keepdims=True)
    A[0, own, :] = (xr + Acc[2, own, :] + NB[4:5, :]).astype(BF16)
    A[1, own, :] = (A[2, own, :].astype(F32) + inv * (ng - gm - normed * gp)).astype(BF16)
    outs = (o_hbm, dx_hbm)

    def fo_copy(k, p, where):
        return rcopy_to(
            A.at[k, own, :],
            outs[k].at[ds(where, Tr), :],
            fo_s.at[k, p],
            fo_r.at[k, where],
            {"tensor": p},
        )

    def fo_send(p):
        fo_copy(0, p, mt).start()
        fo_copy(1, p, mt).start()

    each_tensor(fo_send)
    home = [
        pltpu.make_async_copy(A.at[k, own, :], outs[k].at[own, :], in_sem.at[k])
        for k in range(2)
    ]
    for cp in home:
        cp.start()
    lax.fori_loop(middle, steps, drain, 0)

    each_tensor(lambda p: st_copy(p, p).wait_recv())
    RT[mt] = ST[...]
    whole = RT[0]
    for p in range(1, tn):
        whole = whole + RT[p]
    row = lax.broadcasted_iota(jnp.int32, (8, Dsl), 0)
    so_ref[...] = jnp.where(row < 4, whole, ST[...])

    def ends(p):
        for k in range(2):
            fo_copy(k, p, mt).wait_send()
            fo_copy(k, p, p).wait_recv()
        st_copy(p, mt).wait_send()

    each_tensor(ends)

    def dp_ends(p):
        sp_copy(p, me).wait_send()
        sm_copy(p, me).wait_send()
        bg_copy(p, me).wait_send()

    each_dp(dp_ends)
    for cp in home:
        cp.wait()

    def p2_ends(u, carry):
        @pl.when(has_r)
        def _():
            p2_copy(u, True).wait_send()

        @pl.when(has_l)
        def _():
            p2_copy(u, False).wait_send()

        return carry

    lax.fori_loop(0, U, p2_ends, 0)
    for v in range(max(0, U - NS), U):
        rs_finish(v)
    for v in range(max(0, U - 2), U):
        sb_copy(v).wait_send()
        out_wait(v)


def run_layer(d, seq_len, sp, rope, x, cot, wqkv, wout, wup, wdown):
    n, tn, T, D, Dsl, U = d.n, d.tn, d.T, d.D, d.Dsl, d.U
    n_dp = 2 * n
    width, hidden = d.heads * UNIT, d.chunks * UNIT
    rp, up = sp.shape[0], (U + 7) // 8 * 8
    dma = pltpu.SemaphoreType.DMA
    reg = pltpu.SemaphoreType.REGULAR
    vm = pl.BlockSpec(memory_space=pltpu.VMEM)
    hbm = pl.BlockSpec(memory_space=pl.ANY)
    tile = (Dsl, UNIT)
    return pl.pallas_call(
        functools.partial(layer_kernel, d),
        out_shape=(
            jax.ShapeDtypeStruct((T, D), BF16),
            jax.ShapeDtypeStruct((T, D), BF16),
            jax.ShapeDtypeStruct((3, Dsl, width), F32),
            jax.ShapeDtypeStruct((width, Dsl), F32),
            jax.ShapeDtypeStruct((Dsl, hidden), F32),
            jax.ShapeDtypeStruct((hidden, Dsl), F32),
            jax.ShapeDtypeStruct((2, T, D), BF16),
            jax.ShapeDtypeStruct((8, Dsl), F32),
            jax.ShapeDtypeStruct((up, UNIT), F32),
        ),
        in_specs=[pl.BlockSpec(memory_space=pltpu.SMEM), vm, vm] + [hbm] * 6,
        out_specs=(hbm,) * 7 + (vm, vm),
        scratch_shapes=[
            pltpu.VMEM((d.NW, n_dp) + tile, BF16),
            pltpu.VMEM((3, T, D), BF16),
            pltpu.VMEM((3, 2, n * Dsl, T), BF16),
            pltpu.VMEM((3, T, D), F32),
            pltpu.VMEM((4, T, UNIT), F32),
            pltpu.VMEM((4, T, UNIT), BF16),
            pltpu.VMEM((4, T, UNIT), BF16),
            pltpu.VMEM((T, T), BF16),
            pltpu.VMEM((T, T), BF16),
            pltpu.VMEM((d.NS, n - 2) + tile, BF16),
            pltpu.VMEM((U,) + tile, BF16),
            pltpu.VMEM((U,) + tile, BF16),
            pltpu.VMEM((2, n) + tile, BF16),
            pltpu.VMEM((d.NSR, n) + tile, BF16),
            pltpu.VMEM((d.NLR, n - 1) + tile, BF16),
            pltpu.VMEM((2,) + tile, F32),
            pltpu.VMEM((2, UNIT, Dsl), F32),
            pltpu.VMEM((d.heads + d.chunks,) + tile, BF16),
            pltpu.VMEM((n_dp, rp, UNIT), F32),
            pltpu.VMEM((8, D), F32),
            pltpu.VMEM((U, 8, UNIT), F32),
            pltpu.VMEM((8, D), F32),
            pltpu.VMEM((U, 8, UNIT), F32),
            pltpu.VMEM((up, UNIT), F32),
            pltpu.VMEM((n_dp, 8, Dsl), F32),
            pltpu.VMEM((n_dp, up, UNIT), F32),
            pltpu.VMEM((8, Dsl), F32),
            pltpu.VMEM((tn, 8, Dsl), F32),
            dma((2,)),
            dma((d.NW,)),
            dma((d.NW, n_dp)),
            dma((d.NW, n)),
            dma((d.NW, n)),
            dma((d.NW, n)),
            reg((3,)),
            reg((2,)),
            reg((2,)),
            dma((2,)),
            dma((d.NSR,)),
            dma((d.NS, n - 2)),
            dma((d.NLR, n - 1)),
            dma((2,)),
            dma((n_dp,)),
            dma((n_dp,)),
            dma((2, n_dp)),
            dma((2, n_dp)),
            dma((tn,)),
            dma((tn,)),
            dma((2, tn)),
            dma((2, tn)),
            dma((2, tn)),
            dma((2, tn)),
            dma((2, tn)),
            dma((d.heads + d.chunks,)),
        ],
        compiler_params=pltpu.CompilerParams(
            collective_id=0, has_side_effects=True, vmem_limit_bytes=67_000_000
        ),
        cost_estimate=pl.CostEstimate(
            flops=6 * U * T * D * UNIT,
            bytes_accessed=6 * U * Dsl * UNIT + 8 * T * D,
            transcendentals=T * UNIT * U,
        ),
    )(seq_len, sp, rope, x, cot, wqkv, wout, wup, wdown)


def rope_pair(rows):
    half = ROT // 2
    freq_idx = jnp.arange(half, dtype=F32)
    inv_freq = jnp.exp(-(2.0 * freq_idx / ROT) * math.log(rope_base))
    angles = jnp.arange(rows, dtype=F32)[:, None] * inv_freq[None, :]
    cosine, sine = jnp.cos(angles), jnp.sin(angles)
    rest = 128 - ROT
    return jnp.stack(
        [
            jnp.concatenate([cosine, cosine, jnp.ones((rows, rest), F32)], axis=1),
            jnp.concatenate([-sine, sine, jnp.zeros((rows, rest), F32)], axis=1),
        ]
    )


def per_device(
    n_dp,
    tn,
    block_input,
    cotangent,
    lengths,
    attn_gain,
    attn_shift,
    ffn_gain,
    ffn_shift,
    qkv_weight,
    qkv_bias,
    out_weight,
    out_bias,
    up_weight,
    up_bias,
    down_weight,
):
    T, D = block_input.shape
    n = n_dp // 2
    Dsl = D // n_dp
    width = qkv_weight.shape[2]
    heads = width // HD
    hidden = up_weight.shape[1]
    chunks = hidden // UNIT
    U = 4 * heads + 2 * chunks
    gap = 2 if n <= 4 else 1
    e0 = 1
    d = types.SimpleNamespace(
        n=n,
        tn=tn,
        T=T,
        D=D,
        Dsl=Dsl,
        U=U,
        heads=heads,
        chunks=chunks,
        LAG=3,
        E=e0,
        gap=gap,
        ES=e0 + gap * (n - 2),
        E0=e0 + gap * (n - 1),
        NW=min(U, e0 + gap * (n - 1) + 6),
        NS=min(U, n + 3),
        NSR=4,
        NLR=n + 2,
        I1=14,
    )
    me = lax.axis_index("dp")

    nb, ub = qkv_bias.shape[1], up_bias.shape[0]
    norm_rows = jnp.stack([attn_gain, attn_shift, ffn_gain, ffn_shift, out_bias])
    norm_rows = jnp.pad(norm_rows.astype(F32), ((0, 3), (0, UNIT - Dsl)))
    qkv_rows = jnp.where(
        jnp.arange(width) // nb == me, jnp.tile(qkv_bias.astype(F32), (1, n_dp)), 0.0
    )
    qkv_rows = qkv_rows.reshape(3, heads, UNIT).transpose(1, 0, 2).reshape(3 * heads, UNIT)
    up_rows = jnp.where(jnp.arange(hidden) // ub == me, jnp.tile(up_bias.astype(F32), n_dp), 0.0)
    bias_rows = jnp.concatenate([qkv_rows, up_rows.reshape(chunks, UNIT)])
    spare = -bias_rows.shape[0] % 8
    sp = jnp.concatenate([norm_rows, jnp.pad(bias_rows, ((0, spare), (0, 0)))])

    out, dx, dqkv, dout, dup, ddown, _, so, sb = run_layer(
        d,
        lengths,
        sp,
        rope_pair(T),
        block_input,
        cotangent,
        qkv_weight,
        out_weight,
        up_weight,
        down_weight,
    )
    dqkv_b = sb[: 4 * heads].reshape(heads, 4, UNIT)[:, :3].transpose(1, 0, 2).reshape(3, width)
    dup_b = sb[4 * heads : U].reshape(chunks, 2, UNIT)[:, 0].reshape(hidden)
    return (
        out,
        dx,
        so[0],
        so[1],
        so[2],
        so[3],
        dqkv,
        lax.dynamic_slice_in_dim(dqkv_b, me * nb, nb, axis=1),
        dout,
        so[4],
        dup,
        lax.dynamic_slice_in_dim(dup_b, me * ub, ub, axis=0),
        ddown,
    )


def solution(mesh):
    in_specs = (
        P("dp", None),
        P("dp", None),
        P("dp"),
        P("dp"),
        P("dp"),
        P("dp"),
        P("dp"),
        P(None, "dp", "tensor"),
        P(None, ("tensor", "dp")),
        P("tensor", "dp"),
        P("dp"),
        P("dp", "tensor"),
        P(("tensor", "dp")),
        P("tensor", "dp"),
    )
    out_specs = (
        P("dp", None),
        P("dp", None),
        P("dp"),
        P("dp"),
        P("dp"),
        P("dp"),
        P(None, "dp", "tensor"),
        P(None, ("tensor", "dp")),
        P("tensor", "dp"),
        P("dp"),
        P("dp", "tensor"),
        P(("tensor", "dp")),
        P("tensor", "dp"),
    )
    return jax.shard_map(
        functools.partial(per_device, mesh.shape["dp"], mesh.shape["tensor"]),
        mesh=mesh,
        in_specs=in_specs,
        out_specs=out_specs,
        check_vma=False,
    )
```

```python
import functools
import math
import types

import jax
import jax.numpy as jnp
from jax import lax
from jax.experimental import pallas as pl
from jax.experimental.pallas import tpu as pltpu
from jax.sharding import PartitionSpec as P

HD = 256
ROT = 64
UNIT = 256
ROWS = 128
SLAB = 64
MESH = pl.DeviceIdType.MESH

norm_eps = 1e-05
rope_base = 10000.0

F32 = jnp.float32
BF16 = jnp.bfloat16


def dot(a, b):
    return lax.dot_general(a, b, (((1,), (0,)), ((), ())), preferred_element_type=F32)


def dot_nt(a, b):
    return lax.dot_general(a, b, (((1,), (1,)), ((), ())), preferred_element_type=F32)


def dot_tn(a, b):
    return lax.dot_general(a, b, (((0,), (0,)), ((), ())), preferred_element_type=F32)


def ds(i, size):
    return pl.ds(pl.multiple_of(i * size, size), size)


def layer_kernel(
    d,
    len_ref,
    sp_ref,
    rope_ref,
    x_hbm,
    cot_hbm,
    wqkv,
    wout,
    wup,
    wdown,
    o_hbm,
    dx_hbm,
    dqkv_hbm,
    dout_hbm,
    dup_hbm,
    ddown_hbm,
    pr_hbm,
    so_ref,
    sb_ref,
    W,
    A,
    Acc,
    Y,
    G,
    QK,
    PB,
    DS,
    S,
    SB,
    SR,
    LR,
    stage,
    stage_t,
    RP,
    NB,
    BI,
    SM,
    BG,
    BGC,
    RS1,
    RB2,
    ST,
    RT,
    in_sem,
    own_sem,
    ag_recv,
    agR,
    agL,
    agS,
    lcredit,
    ready,
    sb_sem,
    sr_sem,
    ls_sem,
    lr_sem,
    out_sem,
    sp_s,
    sp_r,
    sm_s,
    sm_r,
    st_s,
    st_r,
    s1_s,
    s1_r,
    s2_s,
    s2_r,
    f1_s,
    f1_r,
    f2_s,
    f2_r,
    loc_sem,
    raw_sem,
    p2_s,
    p2_r,
):
    n, tn, T, D, Dsl, U, heads = d.n, d.tn, d.T, d.D, d.Dsl, d.U, d.heads
    n_dp, NS, NSR, NLR = 2 * d.n, d.NS, d.NSR, d.NLR
    Tr = T // tn
    F0 = d.F0
    F1 = F0 + 4 * heads
    chunks = d.chunks
    me = lax.axis_index("dp")
    mt = lax.axis_index("tensor")
    z = me // 2
    c = me % 2
    right, left, sib = me + 2, me - 2, z * 2 + (1 - c)
    has_r = z < n - 1
    has_l = z > 0
    seq_len = len_ref[0]

    def rcopy_to(src, dst, ss, rs, where):
        return pltpu.make_async_remote_copy(
            src_ref=src,
            dst_ref=dst,
            send_sem=ss,
            recv_sem=rs,
            device_id=where,
            device_id_type=MESH,
        )

    def rcopy(src, dst, ss, rs, dev):
        return rcopy_to(src, dst, ss, rs, {"dp": dev})

    def signal(sem, dev, axis="dp"):
        pl.semaphore_signal(sem, inc=1, device_id={axis: dev}, device_id_type=MESH)

    def is_attn(u):
        return (u >= F0) & (u < F1)

    def chunk_of(u):
        return jnp.where(u < F0, u // 2, (u - 4 * heads) // 2)

    def head_of(u):
        return (u - F0) // 4

    def aidx(u):
        attn = jnp.where(u % 4 == 3, 2, 0)
        ffn = jnp.where(u % 2 == 0, 1, 2)
        return jnp.where(is_attn(u), attn, ffn)

    def by_kind(u, qkv, o, up, down):
        ffn = jnp.logical_not(is_attn(u))

        @pl.when(is_attn(u) & (u % 4 != 3))
        def _():
            qkv()

        @pl.when(is_attn(u) & (u % 4 == 3))
        def _():
            o()

        @pl.when(ffn & (u % 2 == 0))
        def _():
            up()

        @pl.when(ffn & (u % 2 == 1))
        def _():
            down()

    def each_dp(f):
        for p in range(n_dp):

            @pl.when(p != me)
            def _(p=p):
                f(p)

    def each_tensor(f):
        for p in range(tn):

            @pl.when(p != mt)
            def _(p=p):
                f(p)

    def own_tile(u, f):
        by_kind(
            u,
            lambda: f(wqkv.at[u % 4, :, ds(head_of(u), UNIT)]),
            lambda: f(W.at[u, me]),
            lambda: f(wup.at[:, ds(chunk_of(u), UNIT)]),
            lambda: f(W.at[u, me]),
        )

    def ag_tile(u, sj, sem, dev):
        return rcopy(W.at[u, sj], W.at[u, sj], sem, ag_recv.at[u, sj], dev)

    def own_load(src, u):
        return pltpu.make_async_copy(src, W.at[u, me], own_sem.at[u])

    def ag_self(u):
        def go(src):
            rcopy(src, W.at[u, me], agS.at[u, z], ag_recv.at[u, me], sib).start()

        own_tile(u, go)

    def ag_own(u, has_next, sems, dev):
        @pl.when(has_next)
        def _():
            def go(src):
                rcopy(src, W.at[u, me], sems.at[u, z], ag_recv.at[u, me], dev).start()

            own_tile(u, go)

    def relay(u, j, has_next, sems, dev):
        sj = j * 2 + c
        ag_tile(u, sj, agS.at[u, j], sib).wait_recv()

        @pl.when(has_next)
        def _():
            ag_tile(u, sj, sems.at[u, j], dev).start()

        ag_tile(u, sj, agS.at[u, j], sib).start()

    def ag_line(u, has_next, sems, dev, sign):
        for k in range(1, n):
            j = z + sign * k

            @pl.when((j >= 0) & (j < n))
            def _(j=j):
                relay(u, j, has_next, sems, dev)

    def guarded(v, f):
        @pl.when((v >= 0) & (v < U))
        def _():
            f(v)

    def ahead(h):
        return d.ahead[0] if h == 0 else d.ahead[1] + d.ahead[2] * (h - 1)

    def ahead_of(h):
        total = jnp.int32(0)
        for k in range(n):
            total = jnp.where(h == k, ahead(k), total)
        return total

    to_r, to_l = n - 1 - z, z

    def ag_step(s):
        def late(v, f):
            @pl.when((v >= d.burst) & (v < U))
            def _():
                f(v)

        late(s + d.own, ag_self)

        @pl.when(has_l)
        def _():
            late(s + ahead_of(to_r) + 1, lambda u: ag_own(u, has_r, agR, right))

        @pl.when(has_r)
        def _():
            late(s + ahead_of(to_l) + 1, lambda u: ag_own(u, has_l, agL, left))

        guarded(s + ahead_of(to_r), lambda u: ag_line(u, has_r, agR, right, -1))
        guarded(s + ahead_of(to_l), lambda u: ag_line(u, has_l, agL, left, 1))

    def ag_wait(u):
        nothing = lambda: None
        landed = lambda: own_load(wup.at[:, 0:UNIT], u).wait()
        by_kind(u, landed, nothing, landed, nothing)
        for j in range(n):
            ag_tile(u, j * 2 + 1 - c, agS.at[u, j], sib).wait_recv()

    def ag_finish(u):
        for j in range(n):

            @pl.when(has_r & (j <= z))
            def _(j=j):
                ag_tile(u, j * 2 + c, agR.at[u, j], right).wait_send()

            @pl.when(has_l & (j >= z))
            def _(j=j):
                ag_tile(u, j * 2 + c, agL.at[u, j], left).wait_send()

            ag_tile(u, j * 2 + c, agS.at[u, j], sib).wait_send()

    def dead(v, j):
        return W.at[v, j * 2 + 1 - c]

    def part_ref(v, zt):
        if zt == 0 or zt == n - 1:
            return dead(v, zt)
        return S.at[v % NS, zt - 1]

    def sb_copy(u):
        return rcopy(SB.at[u % 2], SR.at[u % NSR], sb_sem.at[u % 2], sr_sem.at[u % NSR], sib)

    def ls_copy(v, zt, to_right):
        slot = zt if to_right else (zt - 1) % n
        if isinstance(zt, int):
            src = part_ref(v, zt)
        else:
            src = S.at[v % NS, zt - 1]
        return rcopy(
            src,
            LR.at[v % NLR, slot],
            ls_sem.at[v % NS, zt],
            lr_sem.at[v % NLR, slot],
            right if to_right else left,
        )

    def dw_half(u, core, put):
        a = aidx(u)
        g = G[u % 4]
        for j in range(n):
            put(j, dot_tn(A[a, :, ds(j * 2 + core, Dsl)], g).astype(BF16))

    def dw_sib(u):
        @pl.when(u >= 2)
        def _():
            sb_copy(u - 2).wait_send()

        def put(j, v):
            SB[u % 2, j] = v

        dw_half(u, 1 - c, put)
        sb_copy(u).start()

    def rs_finish(v):
        for zt in range(n):
            sent = zt != z
            if zt == n - 1:
                sent = sent & (z == 0)
            if zt == 0:
                sent = sent & (z == n - 1)

            @pl.when(sent)
            def _(zt=zt):
                ls_copy(v, zt, True).wait_send()

    def dw_own(u):
        @pl.when(u >= NS)
        def _():
            rs_finish(u - NS)

        def put(j, v):
            part_ref(u, j)[...] = v

        dw_half(u, c, put)

    def add_into(ref, other):
        ref[...] = (ref[...].astype(F32) + other[...].astype(F32)).astype(BF16)

    def combine(v):
        sb_copy(v).wait_recv()
        for zt in range(n):
            add_into(part_ref(v, zt), SR.at[v % NSR, zt])

    def send_right(v):
        @pl.when((z + 1 <= n - 2) & (v >= NLR))
        def _():
            pl.semaphore_wait(lcredit.at[0], 1)

        for zt in range(1, n):
            inner = zt < n - 1

            def take(zt=zt):
                ls_copy(v, zt, True).wait_recv()
                add_into(part_ref(v, zt), LR.at[v % NLR, zt])

            def go(zt=zt):
                ls_copy(v, zt, True).start()

            if inner:

                @pl.when(zt > z)
                def _(take=take, go=go):
                    pl.when(has_l)(take)
                    go()

            else:
                pl.when(z == 0)(go)
                pl.when(z == 1)(take)

    def send_left(v):
        @pl.when((z - 1 >= 1) & (v >= NLR))
        def _():
            pl.semaphore_wait(lcredit.at[1], 1)

        for zt in range(n - 2, -1, -1):
            inner = zt > 0

            def take(zt=zt):
                ls_copy(v, zt, False).wait_recv()
                add_into(part_ref(v, zt), LR.at[v % NLR, (zt - 1) % n])

            def go(zt=zt):
                ls_copy(v, zt, False).start()

            if inner:

                @pl.when(zt < z)
                def _(take=take, go=go):
                    pl.when(has_r)(take)
                    go()

            else:
                pl.when(z == n - 1)(go)
                pl.when(z == n - 2)(take)

    def out_wait(v):
        pltpu.make_async_copy(
            stage.at[v % 2], dup_hbm.at[:, 0:UNIT], out_sem.at[v % 2]
        ).wait()

    def out_start(v):
        slot = v % 2

        def put(src, dst):
            pltpu.make_async_copy(src.at[slot], dst, out_sem.at[slot]).start()

        @pl.when(is_attn(v) & (v % 4 == 3) | jnp.logical_not(is_attn(v)) & (v % 2 == 1))
        def _():
            stage_t[slot] = jnp.transpose(stage[slot])

        by_kind(
            v,
            lambda: put(stage, dqkv_hbm.at[v % 4, :, ds(head_of(v), UNIT)]),
            lambda: put(stage_t, dout_hbm.at[ds(head_of(v), UNIT), :]),
            lambda: put(stage, dup_hbm.at[:, ds(chunk_of(v), UNIT)]),
            lambda: put(stage_t, ddown_hbm.at[ds(chunk_of(v), UNIT), :]),
        )

    def final(v):
        @pl.when((z >= 1) & (z <= n - 2))
        def _():
            @pl.when(v >= 2)
            def _():
                out_wait(v - 2)

            slot = v % 2
            ls_copy(v, z, True).wait_recv()
            ls_copy(v, z, False).wait_recv()
            stage[slot] = (
                S[v % NS, z - 1].astype(F32)
                + LR[v % NLR, z].astype(F32)
                + LR[v % NLR, z - 1].astype(F32)
            )
            out_start(v)

            @pl.when(v + NLR < U)
            def _():
                signal(lcredit.at[0], left)
                signal(lcredit.at[1], right)

    def behind(h):
        return jnp.where(h == 0, 0, d.lag + (h - 1) * d.lag2)

    def rs_step(q):
        guarded(q - 1 - behind(z), send_right)
        guarded(q - 1 - behind(n - 1 - z), send_left)
        guarded(q - 1 - behind(jnp.maximum(z, n - 1 - z)), final)

    def p2_copy(u, to_right):
        side = 0 if to_right else 1
        return rcopy(
            dead(u, n - 1 if to_right else 0),
            dead(u, 1 if to_right else n - 2),
            p2_s.at[side, u],
            p2_r.at[side, u],
            right if to_right else left,
        )

    def p2_side(u, to_right):
        has_prev, has_next = (z >= 2, has_r) if to_right else (z <= n - 3, has_l)
        mine = dead(u, n - 1 if to_right else 0)
        got = dead(u, 1 if to_right else n - 2)
        cp = p2_copy(u, to_right)

        @pl.when(has_prev)
        def _():
            cp.wait_recv()

        @pl.when(has_next)
        def _():
            @pl.when(has_prev)
            def _():
                add_into(mine, got)

            cp.start()

        @pl.when(jnp.logical_not(has_next))
        def _():
            @pl.when(u >= 2)
            def _():
                out_wait(u - 2)

            stage[u % 2] = mine[...].astype(F32) + got[...].astype(F32)
            out_start(u)

    def p2_first(u):
        @pl.when(z == 1)
        def _():
            p2_side(u, True)

        @pl.when(z == n - 2)
        def _():
            p2_side(u, False)

    def p2_step(i):
        @pl.when(z >= 2)
        def _():
            guarded(i - d.hop * (z - 2), lambda u: p2_side(u, True))

        @pl.when(z <= n - 3)
        def _():
            guarded(i - d.hop * (n - 3 - z), lambda u: p2_side(u, False))

    def layer_norm(x):
        mean = jnp.mean(x, axis=-1, keepdims=True)
        cen = x - mean
        inv = lax.rsqrt(jnp.mean(cen * cen, axis=-1, keepdims=True) + norm_eps)
        return cen * inv, inv

    def slabs(first, count, f):
        def one(j, carry):
            f(pl.ds(pl.multiple_of(first + j * SLAB, SLAB), SLAB), first + j * SLAB)
            return carry

        lax.fori_loop(0, count // SLAB, one, 0)

    def ln_block(i):
        def normalize(rows, at):
            normed, _ = layer_norm(A[0, rows, :].astype(F32))
            A[0, rows, :] = (normed * NB[0:1, :] + NB[1:2, :]).astype(BF16)
            A[1, rows, :] = (normed * NB[2:3, :] + NB[3:4, :]).astype(BF16)
            pos = lax.broadcasted_iota(jnp.int32, (SLAB, D), 0) + at
            grad = jnp.where(pos < seq_len, A[2, rows, :].astype(F32), 0.0)
            A[2, rows, :] = grad.astype(BF16)
            SM[4:5, :] += jnp.sum(grad, axis=0, keepdims=True)

        slabs(i * ROWS, ROWS, normalize)
        for a in range(3):
            Acc[a, ds(i, ROWS), :] = jnp.zeros((ROWS, D), F32)

    def y_step(u):
        ag_wait(u)
        w = W[u].reshape(D, UNIT)
        Y[u % 4] = dot(A[aidx(u)], w)

    def acc_step(u):
        a = aidx(u)
        g = G[u % 4]
        for j in range(2 * n):
            cols = slice(j * Dsl, (j + 1) * Dsl)
            Acc[a, :, cols] += dot_nt(g, W[u, j])

    lane = lax.broadcasted_iota(jnp.int32, (T, 128), 1)

    def rotate(y, sign):
        lo = y[:, :128]
        swapped = jnp.where(lane < 32, pltpu.roll(lo, 96, 1), pltpu.roll(lo, 32, 1))
        lo = lo * rope_ref[0] + swapped * (rope_ref[1] * sign)
        return jnp.concatenate([lo, y[:, 128:]], axis=1)

    def attn_core(s):
        u0 = s - 3
        QK[0] = rotate(Y[0] + BI[u0, 0:1, :], 1.0).astype(BF16)
        QK[1] = rotate(Y[1] + BI[u0 + 1, 0:1, :], 1.0).astype(BF16)
        QK[2] = (Y[2] + BI[u0 + 2, 0:1, :]).astype(BF16)
        QK[3] = Y[3].astype(BF16)
        scale = 1.0 / math.sqrt(HD)

        def block(i, carry):
            rows = ds(i, ROWS)
            raw = dot_nt(QK[0, rows, :], QK[1]) * scale
            qpos = lax.broadcasted_iota(jnp.int32, (ROWS, T), 0) + i * ROWS
            kpos = lax.broadcasted_iota(jnp.int32, (ROWS, T), 1)
            scores = jnp.where((kpos <= qpos) & (kpos < seq_len), raw, -jnp.inf)
            top = jnp.max(scores, axis=-1, keepdims=True)
            e = jnp.exp(scores - top)
            p = e / jnp.sum(e, axis=-1, keepdims=True)
            pb = p.astype(BF16)
            PB[rows, :] = pb
            mixed = dot(pb, QK[2]).astype(BF16)
            G[3, rows, :] = mixed
            mg = QK[3, rows, :]
            delta = jnp.sum(mg.astype(F32) * mixed.astype(F32), axis=-1, keepdims=True)
            dp = dot_nt(mg, QK[2])
            dsb = (p * (dp - delta) * scale).astype(BF16)
            DS[rows, :] = dsb
            Y[0, rows, :] = dot(dsb, QK[1])
            return carry

        lax.fori_loop(0, T // ROWS, block, 0)
        Y[1] = dot_tn(DS[...], QK[0])
        for r in range(3):
            if r == 2:
                g = dot_tn(PB[...], QK[3])
            else:
                g = rotate(Y[r], -1.0)
            BG[u0 + r] = jnp.broadcast_to(jnp.sum(g, axis=0, keepdims=True), (8, UNIT))
            G[r] = g.astype(BF16)

    def ffn_core(s):
        b = BI[s - 1, 0:1, :]
        yu, yd = (s - 1) % 4, s % 4
        step = 64

        def block(i, total):
            rows = ds(i, step)
            v = Y[yu, rows, :] + b
            cdf2 = 1.0 + lax.erf(v * (1.0 / math.sqrt(2.0)))
            G[yd, rows, :] = (0.5 * v * cdf2).astype(BF16)
            slope = 0.5 * cdf2 + v * jnp.exp(-0.5 * v * v) * (1.0 / math.sqrt(2.0 * math.pi))
            g = Y[yd, rows, :] * slope
            G[yu, rows, :] = g.astype(BF16)
            return total + jnp.sum(g, axis=0, keepdims=True)

        total = lax.fori_loop(0, T // step, block, jnp.zeros((1, UNIT), F32))
        BG[s - 1] = jnp.broadcast_to(total, (8, UNIT))

    barrier = pltpu.get_barrier_semaphore()
    each_dp(lambda p: signal(barrier, p))
    each_tensor(lambda p: signal(barrier, p, "tensor"))
    x_in = pltpu.make_async_copy(x_hbm, A.at[0], in_sem.at[0])
    c_in = pltpu.make_async_copy(cot_hbm, A.at[2], in_sem.at[1])
    x_in.start()
    c_in.start()
    spots = [
        buf.at[i, r * UNIT : (r + 1) * UNIT, 0:Dsl]
        for buf in (QK, G)
        for i in range(4)
        for r in range(T // UNIT)
    ]
    raws = [
        pltpu.make_async_copy(
            wout.at[i * UNIT : (i + 1) * UNIT, :]
            if i < heads
            else wdown.at[(i - heads) * UNIT : (i - heads + 1) * UNIT, :],
            spots[i],
            raw_sem.at[i],
        )
        for i in range(heads + chunks)
    ]
    for cp in raws:
        cp.start()

    def load_own(u, carry):
        nothing = lambda: None
        by_kind(
            u,
            lambda: own_load(wqkv.at[u % 4, :, ds(head_of(u), UNIT)], u).start(),
            nothing,
            lambda: own_load(wup.at[:, ds(chunk_of(u), UNIT)], u).start(),
            nothing,
        )
        return carry

    lax.fori_loop(0, U, load_own, 0)
    pl.semaphore_wait(barrier, n_dp - 1 + tn - 1)

    def sp_copy(p, where):
        return rcopy(sp_ref, RP.at[where], sp_s.at[p], sp_r.at[where], p)

    each_dp(lambda p: sp_copy(p, me).start())
    RP[me] = sp_ref[...]

    def burst(u, carry):
        ag_own(u, has_r, agR, right)
        ag_own(u, has_l, agL, left)
        ag_self(u)
        return carry

    lax.fori_loop(0, d.burst, burst, 0)
    for i, cp in enumerate(raws):
        cp.wait()
        u = 4 * i + 3 if i < heads else F1 + 2 * (i - heads) + 1
        W[u, me] = jnp.transpose(spots[i][...])

    def end_chip(u, carry):
        @pl.when(z == 0)
        def _():
            ag_own(u, has_r, agR, right)

        @pl.when(z == n - 1)
        def _():
            ag_own(u, has_l, agL, left)

        return carry

    lax.fori_loop(d.burst, U, end_chip, 0)
    SM[...] = jnp.zeros_like(SM)
    BG[...] = jnp.zeros_like(BG)
    BI[...] = jnp.zeros_like(BI)
    each_dp(lambda p: sp_copy(p, p).wait_recv())
    for p in range(n_dp):
        NB[:, p * Dsl : (p + 1) * Dsl] = RP[p, 0:8, 0:Dsl]
    for i in range(3 * heads + chunks):
        row = RP[0, 8 + i : 9 + i, :]
        for p in range(1, n_dp):
            row = row + RP[p, 8 + i : 9 + i, :]
        if i < 3 * heads:
            u = F0 + 4 * (i // 3) + i % 3
        else:
            u = 2 * (i - 3 * heads)
            u = u if u < F0 else u + 4 * heads
        BI[u] = jnp.broadcast_to(row, (8, UNIT))
    x_in.wait()
    c_in.wait()
    blocks = T // ROWS

    fills = max(ahead(h) for h in range(n - 1))

    def fill(i, carry):
        @pl.when(i < fills)
        def _():
            ag_step(i - fills)

        @pl.when(i < blocks)
        def _():
            ln_block(i)

        return carry

    lax.fori_loop(0, max(fills, blocks), fill, 0)

    def made(s):
        return jnp.maximum(jnp.where(s < F1, s - 2, jnp.where(s == F1, s - 1, s)), 0)

    sent_early = max(0, U - d.held - 1 - d.lag)

    def early(q):
        return jnp.clip(jnp.minimum(2 * (q - d.Q0 + 1), q - d.lag), 0, sent_early)

    def first_one(u, carry):
        p2_first(u)
        return carry

    def make(q, carry):
        dw_sib(q)
        guarded(q - 1, combine)

        @pl.when(q < U - d.held)
        def _():
            rs_step(q)

        acc_step(q)
        dw_own(q)
        lax.fori_loop(early(q - 1), early(q), first_one, 0)
        return carry

    def body(s, carry):
        ag_step(s)
        guarded(s, y_step)

        @pl.when(s == F1 + 2)
        def _():
            x_in.start()

        @pl.when(is_attn(s) & (s % 4 == 3))
        def _():
            attn_core(s)

        @pl.when(jnp.logical_not(is_attn(s)) & (s < U) & (s % 2 == 1))
        def _():
            ffn_core(s)

        lax.fori_loop(made(s - 1), made(s), make, 0)
        return carry

    lax.fori_loop(0, U + 1, body, 0)
    x_in.wait()

    @pl.when(has_r)
    def _():
        signal(ready.at[1], right)

    @pl.when(has_l)
    def _():
        signal(ready.at[0], left)

    lo = d.lo
    hi = tn // lo
    size = ((lo, hi), (hi, lo))
    coord = ((mt % lo, mt // lo), (mt // lo, mt % lo))
    acc_of = (2, 0)
    own = ds(mt, Tr)

    def block_of(k, a, b):
        return b * lo + a if k == 0 else a * lo + b

    def packed(mine, theirs):
        return mine - jnp.where(mine > theirs, 1, 0)

    def s1_copy(k, a, b, sender):
        s2 = size[k][1]
        return rcopy_to(
            A.at[k, ds(block_of(k, a, b), Tr), :],
            pr_hbm.at[k, packed(sender, a) * s2 + b],
            s1_s.at[k, a * s2 + b],
            s1_r.at[k, sender * s2 + b],
            {"tensor": block_of(k, a, coord[k][1])},
        )

    def s1_wait(k, q, b):
        s2 = size[k][1]
        c1 = coord[k][0]
        return rcopy_to(
            A.at[k, own, :],
            pr_hbm.at[k, packed(q, c1) * s2 + b],
            s1_s.at[k, q * s2 + b],
            s1_r.at[k, q * s2 + b],
            {"tensor": block_of(k, q, coord[k][1])},
        )

    def s2_copy(k, b, sender):
        c1 = coord[k][0]
        return rcopy_to(
            A.at[k, ds(block_of(k, c1, b), Tr), :],
            pr_hbm.at[k, d.P1 + packed(sender, b)],
            s2_s.at[k, b],
            s2_r.at[k, sender],
            {"tensor": block_of(k, c1, b)},
        )

    def s2_wait(k, q):
        c1, c2 = coord[k]
        return rcopy_to(
            A.at[k, own, :],
            pr_hbm.at[k, d.P1 + packed(q, c2)],
            s2_s.at[k, q],
            s2_r.at[k, q],
            {"tensor": block_of(k, c1, q)},
        )

    def others(k, which, f):
        for q in range(size[k][which]):

            @pl.when(q != coord[k][which])
            def _(q=q):
                f(q)

    def s1_send(i):
        @pl.when(i >= 0)
        def _():
            for k in range(2):
                a = i % lo if k == 0 else i // lo
                b = i // lo if k == 0 else i % lo

                @pl.when(a != coord[k][0])
                def _(k=k, a=a, b=b):
                    s1_copy(k, a, b, coord[k][0]).start()

    def partial(i, carry):
        @pl.when(i == mt)
        def _():
            A[2, ds((mt + 1) % tn, Tr), :] = A[0, ds(i, Tr), :]

        def rows_of(rows, at):
            normed, _ = layer_norm(A[0, rows, :].astype(F32))
            ab = Acc[0, rows, :]
            fb = Acc[1, rows, :]
            SM[0:1, :] += jnp.sum(ab * normed, axis=0, keepdims=True)
            SM[1:2, :] += jnp.sum(ab, axis=0, keepdims=True)
            SM[2:3, :] += jnp.sum(fb * normed, axis=0, keepdims=True)
            SM[3:4, :] += jnp.sum(fb, axis=0, keepdims=True)
            ng = ab * NB[0:1, :] + fb * NB[2:3, :]
            Acc[0, rows, :] = ng
            A[1, rows, :] = ng.astype(BF16)
            A[0, rows, :] = Acc[2, rows, :].astype(BF16)

        slabs(i * Tr, Tr, rows_of)
        s1_send(i - 1)
        return carry

    lax.fori_loop(0, tn, partial, 0)
    for u in range(U):
        BGC[u : u + 1, :] = BG[u, 0:1, :]
    s1_send(tn - 1)

    def sm_copy(p, where):
        return rcopy(
            SM.at[:, ds(p, Dsl)], RS1.at[where], sm_s.at[0, p], sm_r.at[0, where], p
        )

    def bg_copy(p, where):
        return rcopy(BGC, RB2.at[where], sm_s.at[1, p], sm_r.at[1, where], p)

    def small_send(p):
        sm_copy(p, me).start()
        bg_copy(p, me).start()

    each_dp(small_send)
    RS1[me] = SM[:, ds(me, Dsl)]
    RB2[me] = BGC[...]

    @pl.when(has_r)
    def _():
        pl.semaphore_wait(ready.at[0], 1)

    @pl.when(has_l)
    def _():
        pl.semaphore_wait(ready.at[1], 1)

    rest = d.held + d.lag + (n - 3) * d.lag2 + 1
    steps = U + d.hop * (n - 3)

    def p2_count(i):
        fed = jnp.minimum(d.pace * (i + 1), sent_early + i)
        return jnp.clip(jnp.where(i < rest, fed, steps), 0, steps)

    def p2_one(i, carry):
        p2_step(i)
        return carry

    def drain(i, carry):
        rs_step(i + U - d.held)
        guarded(i + sent_early, p2_first)
        lax.fori_loop(p2_count(i - 1), p2_count(i), p2_one, 0)
        return carry

    marks = [min(m, rest) for m in d.marks]
    combine(U - 1)
    lax.fori_loop(0, marks[0], drain, 0)

    def load(k, slot, b):
        return pltpu.make_async_copy(
            pr_hbm.at[k, slot], A.at[k, ds(b, Tr), :], loc_sem.at[k, slot]
        )

    def gather_in(k, do):
        s1, s2 = size[k]
        for b in range(s2):
            do(b, block_of(k, coord[k][0], b))

    for k in range(2):
        s1, s2 = size[k]

        def take(q, k=k, s2=s2):
            for b in range(s2):
                s1_wait(k, q, b).wait_recv()

        others(k, 0, take)
        for q in range(s1 - 1):
            for b in range(s2):
                load(k, q * s2 + b, block_of(k, coord[k][0], b)).start()
            for b in range(s2):
                row_b = block_of(k, coord[k][0], b)
                load(k, q * s2 + b, row_b).wait()
                rows = ds(row_b, Tr)
                Acc[acc_of[k], rows, :] += A[k, rows, :].astype(F32)

        def pass_on(b, k=k):
            rows = ds(block_of(k, coord[k][0], b), Tr)
            A[k, rows, :] = Acc[acc_of[k], rows, :].astype(BF16)
            s2_copy(k, b, coord[k][1]).start()

        others(k, 1, pass_on)

    lax.fori_loop(marks[0], marks[1], drain, 0)

    def small_wait(p):
        sm_copy(p, p).wait_recv()
        bg_copy(p, p).wait_recv()

    each_dp(small_wait)
    total = RS1[0]
    bias_total = RB2[0]
    for p in range(1, n_dp):
        total = total + RS1[p]
        bias_total = bias_total + RB2[p]
    sb_ref[...] = bias_total
    ST[...] = total

    for k in range(2):
        others(k, 1, lambda q, k=k: s2_wait(k, q).wait_recv())
        for q in range(size[k][1] - 1):
            cp = load(k, d.P1 + q, mt)
            cp.start()
            cp.wait()
            Acc[acc_of[k], own, :] += A[k, own, :].astype(F32)

    def st_copy(p, where):
        return rcopy_to(ST, RT.at[where], st_s.at[p], st_r.at[where], {"tensor": p})

    each_tensor(lambda p: st_copy(p, mt).start())
    def finish(rows, at):
        off = pl.multiple_of((mt + 1) % tn * Tr + at - mt * Tr, SLAB)
        xr = A[2, pl.ds(off, SLAB), :].astype(F32)
        normed, inv = layer_norm(xr)
        ng = Acc[0, rows, :]
        gm = jnp.mean(ng, axis=-1, keepdims=True)
        gp = jnp.mean(ng * normed, axis=-1, keepdims=True)
        A[0, rows, :] = (xr + Acc[2, rows, :] + NB[4:5, :]).astype(BF16)
        A[1, rows, :] = (A[2, rows, :].astype(F32) + inv * (ng - gm - normed * gp)).astype(BF16)

    slabs(mt * Tr, Tr, finish)
    outs = (o_hbm, dx_hbm)

    def f1_copy(k, b, sender):
        c1 = coord[k][0]
        return rcopy_to(
            A.at[k, own, :],
            outs[k].at[ds(block_of(k, c1, sender), Tr), :],
            f1_s.at[k, b],
            f1_r.at[k, sender],
            {"tensor": block_of(k, c1, b)},
        )

    def f2_copy(k, a, b, sender, src):
        s2 = size[k][1]
        return rcopy_to(
            src,
            outs[k].at[ds(block_of(k, sender, b), Tr), :],
            f2_s.at[k, a * s2 + b],
            f2_r.at[k, sender * s2 + b],
            {"tensor": block_of(k, a, coord[k][1])},
        )

    home = [
        pltpu.make_async_copy(A.at[k, own, :], outs[k].at[own, :], in_sem.at[k])
        for k in range(2)
    ]
    for k in range(2):
        c1, c2 = coord[k]
        others(k, 1, lambda b, k=k, c2=c2: f1_copy(k, b, c2).start())
    for k in range(2):
        c1, c2 = coord[k]

        def mine_on(a, k=k, c1=c1, c2=c2):
            f2_copy(k, a, c2, c1, A.at[k, own, :]).start()

        others(k, 0, mine_on)
        home[k].start()
    lax.fori_loop(marks[1], marks[2], drain, 0)
    for k in range(2):
        c1, c2 = coord[k]

        def forward(b, k=k, c1=c1):
            f1_copy(k, b, b).wait_recv()
            rows = ds(block_of(k, c1, b), Tr)
            others(k, 0, lambda a: f2_copy(k, a, b, c1, outs[k].at[rows, :]).start())

        others(k, 1, forward)
    lax.fori_loop(marks[2], rest, drain, 0)
    lax.fori_loop(p2_count(rest - 1), steps, p2_one, 0)

    each_tensor(lambda p: st_copy(p, p).wait_recv())
    RT[mt] = ST[...]
    whole = RT[0]
    for p in range(1, tn):
        whole = whole + RT[p]
    row = lax.broadcasted_iota(jnp.int32, (8, Dsl), 0)
    so_ref[...] = jnp.where(row < 4, whole, ST[...])

    for k in range(2):
        c1, c2 = coord[k]
        s1, s2 = size[k]

        def end0(q, k=k, c1=c1, s2=s2):
            for b in range(s2):
                s1_copy(k, q, b, c1).wait_send()
                f2_copy(k, q, b, c1, A.at[k, own, :]).wait_send()
                f2_copy(k, q, b, q, A.at[k, own, :]).wait_recv()

        def end1(b, k=k, c2=c2):
            s2_copy(k, b, c2).wait_send()
            f1_copy(k, b, c2).wait_send()

        others(k, 0, end0)
        others(k, 1, end1)

    each_tensor(lambda p: st_copy(p, mt).wait_send())

    def dp_ends(p):
        sp_copy(p, me).wait_send()
        sm_copy(p, me).wait_send()
        bg_copy(p, me).wait_send()

    each_dp(dp_ends)
    for cp in home:
        cp.wait()

    def line_ends(u, carry):
        ag_finish(u)

        @pl.when(has_r & has_l)
        def _():
            p2_copy(u, True).wait_send()
            p2_copy(u, False).wait_send()

        return carry

    lax.fori_loop(0, U, line_ends, 0)
    for v in range(max(0, U - NS), U):
        rs_finish(v)
    for v in range(max(0, U - 2), U):
        sb_copy(v).wait_send()
        out_wait(v)


def run_layer(d, seq_len, sp, rope, x, cot, wqkv, wout, wup, wdown):
    n, tn, T, D, Dsl, U = d.n, d.tn, d.T, d.D, d.Dsl, d.U
    n_dp = 2 * n
    width, hidden = d.heads * UNIT, d.chunks * UNIT
    rp, up = sp.shape[0], (U + 7) // 8 * 8
    dma = pltpu.SemaphoreType.DMA
    reg = pltpu.SemaphoreType.REGULAR
    vm = pl.BlockSpec(memory_space=pltpu.VMEM)
    hbm = pl.BlockSpec(memory_space=pl.ANY)
    tile = (Dsl, UNIT)
    return pl.pallas_call(
        functools.partial(layer_kernel, d),
        out_shape=(
            jax.ShapeDtypeStruct((T, D), BF16),
            jax.ShapeDtypeStruct((T, D), BF16),
            jax.ShapeDtypeStruct((3, Dsl, width), F32),
            jax.ShapeDtypeStruct((width, Dsl), F32),
            jax.ShapeDtypeStruct((Dsl, hidden), F32),
            jax.ShapeDtypeStruct((hidden, Dsl), F32),
            jax.ShapeDtypeStruct((2, d.P1 + d.P2, T // tn, D), BF16),
            jax.ShapeDtypeStruct((8, Dsl), F32),
            jax.ShapeDtypeStruct((up, UNIT), F32),
        ),
        in_specs=[pl.BlockSpec(memory_space=pltpu.SMEM), vm, vm] + [hbm] * 6,
        out_specs=(hbm,) * 7 + (vm, vm),
        scratch_shapes=[
            pltpu.VMEM((U, n_dp) + tile, BF16),
            pltpu.VMEM((3, T, D), BF16),
            pltpu.VMEM((3, T, D), F32),
            pltpu.VMEM((4, T, UNIT), F32),
            pltpu.VMEM((4, T, UNIT), BF16),
            pltpu.VMEM((4, T, UNIT), BF16),
            pltpu.VMEM((T, T), BF16),
            pltpu.VMEM((T, T), BF16),
            pltpu.VMEM((d.NS, n - 2) + tile, BF16),
            pltpu.VMEM((2, n) + tile, BF16),
            pltpu.VMEM((d.NSR, n) + tile, BF16),
            pltpu.VMEM((d.NLR, n) + tile, BF16),
            pltpu.VMEM((2,) + tile, F32),
            pltpu.VMEM((2, UNIT, Dsl), F32),
            pltpu.VMEM((n_dp, rp, UNIT), F32),
            pltpu.VMEM((8, D), F32),
            pltpu.VMEM((U, 8, UNIT), F32),
            pltpu.VMEM((8, D), F32),
            pltpu.VMEM((U, 8, UNIT), F32),
            pltpu.VMEM((up, UNIT), F32),
            pltpu.VMEM((n_dp, 8, Dsl), F32),
            pltpu.VMEM((n_dp, up, UNIT), F32),
            pltpu.VMEM((8, Dsl), F32),
            pltpu.VMEM((tn, 8, Dsl), F32),
            dma((2,)),
            dma((U,)),
            dma((U, n_dp)),
            dma((U, n)),
            dma((U, n)),
            dma((U, n)),
            reg((2,)),
            reg((2,)),
            dma((2,)),
            dma((d.NSR,)),
            dma((d.NS, n)),
            dma((d.NLR, n)),
            dma((2,)),
            dma((n_dp,)),
            dma((n_dp,)),
            dma((2, n_dp)),
            dma((2, n_dp)),
            dma((tn,)),
            dma((tn,)),
            dma((2, tn)),
            dma((2, tn)),
            dma((2, tn)),
            dma((2, tn)),
            dma((2, tn)),
            dma((2, tn)),
            dma((2, tn)),
            dma((2, tn)),
            dma((2, d.P1 + d.P2)),
            dma((d.heads + d.chunks,)),
            dma((2, U)),
            dma((2, U)),
        ],
        compiler_params=pltpu.CompilerParams(
            collective_id=0, has_side_effects=True, vmem_limit_bytes=67_000_000
        ),
        cost_estimate=pl.CostEstimate(
            flops=6 * U * T * D * UNIT,
            bytes_accessed=6 * U * Dsl * UNIT + 8 * T * D,
            transcendentals=T * UNIT * U,
        ),
    )(seq_len, sp, rope, x, cot, wqkv, wout, wup, wdown)


def rope_pair(rows):
    half = ROT // 2
    freq_idx = jnp.arange(half, dtype=F32)
    inv_freq = jnp.exp(-(2.0 * freq_idx / ROT) * math.log(rope_base))
    angles = jnp.arange(rows, dtype=F32)[:, None] * inv_freq[None, :]
    cosine, sine = jnp.cos(angles), jnp.sin(angles)
    rest = 128 - ROT
    return jnp.stack(
        [
            jnp.concatenate([cosine, cosine, jnp.ones((rows, rest), F32)], axis=1),
            jnp.concatenate([-sine, sine, jnp.zeros((rows, rest), F32)], axis=1),
        ]
    )


def per_device(
    n_dp,
    tn,
    block_input,
    cotangent,
    lengths,
    attn_gain,
    attn_shift,
    ffn_gain,
    ffn_shift,
    qkv_weight,
    qkv_bias,
    out_weight,
    out_bias,
    up_weight,
    up_bias,
    down_weight,
):
    T, D = block_input.shape
    n = n_dp // 2
    Dsl = D // n_dp
    width = qkv_weight.shape[2]
    heads = width // HD
    hidden = up_weight.shape[1]
    chunks = hidden // UNIT
    U = 4 * heads + 2 * chunks
    F0, lag, lag2 = 0, 5, 2
    hi = 2 if tn % 2 == 0 else 1
    lo = tn // hi
    d = types.SimpleNamespace(
        n=n,
        tn=tn,
        T=T,
        D=D,
        Dsl=Dsl,
        U=U,
        heads=heads,
        chunks=chunks,
        F0=F0,
        held=3,
        ahead=(1, 4, 2),
        own=5,
        burst=3,
        hop=2,
        lag=lag,
        lag2=lag2,
        pace=3,
        Q0=U - 8,
        NS=min(U, lag + (n - 3) * lag2 + 4),
        NSR=4,
        NLR=min(U, lag + (n - 3) * lag2 + 2),
        lo=lo,
        P1=max((lo - 1) * hi, (hi - 1) * lo),
        P2=max(lo, hi) - 1,
        marks=(3, 4, 5),
    )
    me = lax.axis_index("dp")

    nb, ub = qkv_bias.shape[1], up_bias.shape[0]
    norm_rows = jnp.stack([attn_gain, attn_shift, ffn_gain, ffn_shift, out_bias])
    norm_rows = jnp.pad(norm_rows.astype(F32), ((0, 3), (0, UNIT - Dsl)))
    qkv_rows = jnp.where(
        jnp.arange(width) // nb == me, jnp.tile(qkv_bias.astype(F32), (1, n_dp)), 0.0
    )
    qkv_rows = qkv_rows.reshape(3, heads, UNIT).transpose(1, 0, 2).reshape(3 * heads, UNIT)
    up_rows = jnp.where(jnp.arange(hidden) // ub == me, jnp.tile(up_bias.astype(F32), n_dp), 0.0)
    bias_rows = jnp.concatenate([qkv_rows, up_rows.reshape(chunks, UNIT)])
    spare = -bias_rows.shape[0] % 8
    sp = jnp.concatenate([norm_rows, jnp.pad(bias_rows, ((0, spare), (0, 0)))])

    out, dx, dqkv, dout, dup, ddown, _, so, sb = run_layer(
        d,
        lengths,
        sp,
        rope_pair(T),
        block_input,
        cotangent,
        qkv_weight,
        out_weight,
        up_weight,
        down_weight,
    )
    F1 = F0 + 4 * heads
    dqkv_b = sb[F0:F1].reshape(heads, 4, UNIT)[:, :3].transpose(1, 0, 2).reshape(3, width)
    dup_b = jnp.concatenate([sb[:F0], sb[F1:U]]).reshape(chunks, 2, UNIT)[:, 0].reshape(hidden)
    return (
        out,
        dx,
        so[0],
        so[1],
        so[2],
        so[3],
        dqkv,
        lax.dynamic_slice_in_dim(dqkv_b, me * nb, nb, axis=1),
        dout,
        so[4],
        dup,
        lax.dynamic_slice_in_dim(dup_b, me * ub, ub, axis=0),
        ddown,
    )


def solution(mesh):
    in_specs = (
        P("dp", None),
        P("dp", None),
        P("dp"),
        P("dp"),
        P("dp"),
        P("dp"),
        P("dp"),
        P(None, "dp", "tensor"),
        P(None, ("tensor", "dp")),
        P("tensor", "dp"),
        P("dp"),
        P("dp", "tensor"),
        P(("tensor", "dp")),
        P("tensor", "dp"),
    )
    out_specs = (
        P("dp", None),
        P("dp", None),
        P("dp"),
        P("dp"),
        P("dp"),
        P("dp"),
        P(None, "dp", "tensor"),
        P(None, ("tensor", "dp")),
        P("tensor", "dp"),
        P("dp"),
        P("dp", "tensor"),
        P(("tensor", "dp")),
        P("tensor", "dp"),
    )
    return jax.shard_map(
        functools.partial(per_device, mesh.shape["dp"], mesh.shape["tensor"]),
        mesh=mesh,
        in_specs=in_specs,
        out_specs=out_specs,
        check_vma=False,
    )
```

```python
import functools
import math
import types

import jax
import jax.numpy as jnp
import numpy as np
from jax import lax
from jax.experimental import pallas as pl
from jax.experimental.pallas import tpu as pltpu
from jax.sharding import PartitionSpec as P

HD = 256
ROT = 64
UNIT = 256
ROWS = 128
SLAB = 64
MESH = pl.DeviceIdType.MESH

norm_eps = 1e-05
rope_base = 10000.0

F32 = jnp.float32
BF16 = jnp.bfloat16


def dot(a, b):
    return lax.dot_general(a, b, (((1,), (0,)), ((), ())), preferred_element_type=F32)


def dot_nt(a, b):
    return lax.dot_general(a, b, (((1,), (1,)), ((), ())), preferred_element_type=F32)


def dot_tn(a, b):
    return lax.dot_general(a, b, (((0,), (0,)), ((), ())), preferred_element_type=F32)


def ds(i, size):
    return pl.ds(pl.multiple_of(i * size, size), size)


def layer_kernel(
    d,
    len_ref,
    ga_ref,
    sa_ref,
    gf_ref,
    sf_ref,
    ob_ref,
    ub_ref,
    qb_ref,
    rope_hbm,
    x_hbm,
    cot_hbm,
    wqkv,
    wout,
    wup,
    wdown,
    o_hbm,
    dx_hbm,
    dqkv_hbm,
    dout_hbm,
    dup_hbm,
    ddown_hbm,
    pr_hbm,
    so_ref,
    W,
    A,
    rope_ref,
    Acc,
    Y,
    G,
    QK,
    PB,
    DS,
    S,
    SB,
    SR,
    LR,
    stage,
    stage_t,
    RP,
    NB,
    BI,
    SM,
    BG,
    BGC,
    RS1,
    RB2,
    ST,
    RT,
    SBT,
    in_sem,
    own_sem,
    line_r,
    sib_r,
    agR,
    agL,
    agS,
    lcredit,
    ready,
    sb_sem,
    sr_sem,
    ls_sem,
    lr_sem,
    out_sem,
    sp_s,
    sp_r,
    sm_s,
    sm_r,
    st_s,
    st_r,
    s1_s,
    s1_r,
    s2_s,
    s2_r,
    f1_s,
    f1_r,
    f2_s,
    f2_r,
    loc_sem,
    raw_sem,
    p2_s,
    p2_r,
    rope_sem,
    SP,
    SW,
):
    n, tn, T, D, Dsl, U, heads = d.n, d.tn, d.T, d.D, d.Dsl, d.U, d.heads
    n_dp, NS, NSR, NLR = 2 * d.n, d.NS, d.NSR, d.NLR
    Tr = T // tn
    F0 = d.F0
    F1 = F0 + 4 * heads
    chunks = d.chunks
    me = lax.axis_index("dp")
    mt = lax.axis_index("tensor")
    z = me // 2
    c = me % 2
    right, left, sib = me + 2, me - 2, z * 2 + (1 - c)
    has_r = z < n - 1
    has_l = z > 0
    seq_len = len_ref[0]

    def rcopy_to(src, dst, ss, rs, where):
        return pltpu.make_async_remote_copy(
            src_ref=src,
            dst_ref=dst,
            send_sem=ss,
            recv_sem=rs,
            device_id=where,
            device_id_type=MESH,
        )

    def rcopy(src, dst, ss, rs, dev):
        return rcopy_to(src, dst, ss, rs, {"dp": dev})

    def signal(sem, dev, axis="dp"):
        pl.semaphore_signal(sem, inc=1, device_id={axis: dev}, device_id_type=MESH)

    def is_attn(u):
        return (u >= F0) & (u < F1)

    def chunk_of(u):
        return jnp.where(u < F0, u // 2, (u - 4 * heads) // 2)

    def head_of(u):
        return (u - F0) // 4

    def aidx(u):
        attn = jnp.where(u % 4 == 3, 2, 0)
        ffn = jnp.where(u % 2 == 0, 1, 2)
        return jnp.where(is_attn(u), attn, ffn)

    def by_kind(u, qkv, o, up, down):
        ffn = jnp.logical_not(is_attn(u))

        @pl.when(is_attn(u) & (u % 4 != 3))
        def _():
            qkv()

        @pl.when(is_attn(u) & (u % 4 == 3))
        def _():
            o()

        @pl.when(ffn & (u % 2 == 0))
        def _():
            up()

        @pl.when(ffn & (u % 2 == 1))
        def _():
            down()

    def each_dp(f):
        for p in range(n_dp):

            @pl.when(p != me)
            def _(p=p):
                f(p)

    def each_tensor(f):
        for p in range(tn):

            @pl.when(p != mt)
            def _(p=p):
                f(p)

    def own_tile(u, f):
        by_kind(
            u,
            lambda: f(wqkv.at[u % 4, :, ds(head_of(u), UNIT)]),
            lambda: f(W.at[u, me]),
            lambda: f(wup.at[:, ds(chunk_of(u), UNIT)]),
            lambda: f(W.at[u, me]),
        )

    def to_line(u, j, src, sems, dev):
        return rcopy(src, W.at[u, j * 2 + c], sems.at[j], line_r.at[u, j], dev)

    def to_sib(u, j, src):
        return rcopy(src, W.at[u, j * 2 + c], agS.at[j], sib_r.at[u], sib)

    def own_all():
        span = W.at[0 : 3 * heads + chunks, 0]
        return pltpu.make_async_copy(span, span, own_sem.at[0])

    def own_load(src, u):
        return pltpu.make_async_copy(src, W.at[u, me], own_sem.at[0])

    def ag_self(u):
        def go(src):
            to_sib(u, z, src).start()

        own_tile(u, go)

    def ag_own(u, has_next, sems, dev):
        @pl.when(has_next)
        def _():
            def go(src):
                to_line(u, z, src, sems, dev).start()

            own_tile(u, go)

    def relay(u, j, has_next, sems, dev):
        tile = W.at[u, j * 2 + c]
        to_line(u, j, tile, sems, dev).wait_recv()

        @pl.when(has_next)
        def _():
            to_line(u, j, tile, sems, dev).start()

        to_sib(u, j, tile).start()

    def ag_line(u, has_next, sems, dev, sign):
        for k in range(1, n):
            j = z + sign * k

            @pl.when((j >= 0) & (j < n))
            def _(j=j):
                relay(u, j, has_next, sems, dev)

    def guarded(v, f):
        @pl.when((v >= 0) & (v < U))
        def _():
            f(v)

    def ahead(h):
        return d.ahead[0] if h == 0 else d.ahead[1] + d.ahead[2] * (h - 1)

    def ahead_of(h):
        total = jnp.int32(0)
        for k in range(n):
            total = jnp.where(h == k, ahead(k), total)
        return total

    to_r, to_l = n - 1 - z, z

    def ag_step(s):
        def late(v, f):
            @pl.when((v >= d.burst) & (v < U))
            def _():
                f(v)

        late(s + d.own, ag_self)

        @pl.when(has_l)
        def _():
            late(s + ahead_of(to_r) + 1, lambda u: ag_own(u, has_r, agR, right))

        @pl.when(has_r)
        def _():
            late(s + ahead_of(to_l) + 1, lambda u: ag_own(u, has_l, agL, left))

        guarded(s + ahead_of(to_r), lambda u: ag_line(u, has_r, agR, right, -1))
        guarded(s + ahead_of(to_l), lambda u: ag_line(u, has_l, agL, left, 1))

    def ag_wait(u):
        span = W.at[u, 0:n]
        rcopy(span, span, agS.at[0], sib_r.at[u], sib).wait_recv()

    def units_sent(sem):
        span = W.at[:, 0]
        rcopy(span, span, sem, line_r.at[0, 0], sib).wait_send()

    def ag_finish():
        for j in range(n):

            @pl.when(has_r & (j <= z))
            def _(j=j):
                units_sent(agR.at[j])

            @pl.when(has_l & (j >= z))
            def _(j=j):
                units_sent(agL.at[j])

            units_sent(agS.at[j])

    def dead(v, j):
        return W.at[v, j * 2 + 1 - c]

    def part_ref(v, zt):
        if zt == 0 or zt == n - 1:
            return dead(v, zt)
        return S.at[v % NS, zt - 1]

    def sb_copy(u):
        return rcopy(SB.at[u % 2], SR.at[u % NSR], sb_sem.at[u % 2], sr_sem.at[u % NSR], sib)

    def ls_copy(v, zt, to_right):
        slot = zt if to_right else (zt - 1) % n
        if isinstance(zt, int):
            src = part_ref(v, zt)
        else:
            src = S.at[v % NS, zt - 1]
        return rcopy(
            src,
            LR.at[v % NLR, slot],
            ls_sem.at[v % NS],
            lr_sem.at[v % NLR, slot],
            right if to_right else left,
        )

    def dw_half(u, core, put):
        a = aidx(u)
        g = G[u % 4]
        for j in range(n):
            put(j, dot_tn(A[a, :, ds(j * 2 + core, Dsl)], g).astype(BF16))

    def dw_sib(u):
        @pl.when(u >= 2)
        def _():
            sb_copy(u - 2).wait_send()

        def put(j, v):
            SB[u % 2, j] = v

        dw_half(u, 1 - c, put)
        sb_copy(u).start()

    def rs_finish(v):
        def sent(count):
            span = W.at[0, 0:count]
            rcopy(span, span, ls_sem.at[v % NS], line_r.at[0, 0], sib).wait_send()

        ends = (z == 0) | (z == n - 1)
        pl.when(ends)(lambda: sent(n - 1))
        pl.when(jnp.logical_not(ends))(lambda: sent(n - 3))

    def dw_own(u):
        @pl.when(u >= NS)
        def _():
            rs_finish(u - NS)

        def put(j, v):
            part_ref(u, j)[...] = v

        dw_half(u, c, put)

    def add_into(ref, other):
        ref[...] = (ref[...].astype(F32) + other[...].astype(F32)).astype(BF16)

    def combine(v):
        sb_copy(v).wait_recv()
        for zt in range(n):
            add_into(part_ref(v, zt), SR.at[v % NSR, zt])

    def send_right(v):
        @pl.when((z + 1 <= n - 2) & (v >= NLR))
        def _():
            pl.semaphore_wait(lcredit.at[0], 1)

        for zt in range(1, n):
            inner = zt < n - 1

            def take(zt=zt):
                ls_copy(v, zt, True).wait_recv()
                add_into(part_ref(v, zt), LR.at[v % NLR, zt])

            def go(zt=zt):
                ls_copy(v, zt, True).start()

            if inner:

                @pl.when(zt > z)
                def _(take=take, go=go):
                    pl.when(has_l)(take)
                    go()

            else:
                pl.when(z == 0)(go)
                pl.when(z == 1)(take)

    def send_left(v):
        @pl.when((z - 1 >= 1) & (v >= NLR))
        def _():
            pl.semaphore_wait(lcredit.at[1], 1)

        for zt in range(n - 2, -1, -1):
            inner = zt > 0

            def take(zt=zt):
                ls_copy(v, zt, False).wait_recv()
                add_into(part_ref(v, zt), LR.at[v % NLR, (zt - 1) % n])

            def go(zt=zt):
                ls_copy(v, zt, False).start()

            if inner:

                @pl.when(zt < z)
                def _(take=take, go=go):
                    pl.when(has_r)(take)
                    go()

            else:
                pl.when(z == n - 1)(go)
                pl.when(z == n - 2)(take)

    def out_wait(v):
        pltpu.make_async_copy(
            stage.at[v % 2], dup_hbm.at[:, 0:UNIT], out_sem.at[v % 2]
        ).wait()

    def out_start(v):
        slot = v % 2

        def put(src, dst):
            pltpu.make_async_copy(src.at[slot], dst, out_sem.at[slot]).start()

        @pl.when(is_attn(v) & (v % 4 == 3) | jnp.logical_not(is_attn(v)) & (v % 2 == 1))
        def _():
            stage_t[slot] = jnp.transpose(stage[slot])

        by_kind(
            v,
            lambda: put(stage, dqkv_hbm.at[v % 4, :, ds(head_of(v), UNIT)]),
            lambda: put(stage_t, dout_hbm.at[ds(head_of(v), UNIT), :]),
            lambda: put(stage, dup_hbm.at[:, ds(chunk_of(v), UNIT)]),
            lambda: put(stage_t, ddown_hbm.at[ds(chunk_of(v), UNIT), :]),
        )

    def final(v):
        @pl.when((z >= 1) & (z <= n - 2))
        def _():
            @pl.when(v >= 2)
            def _():
                out_wait(v - 2)

            slot = v % 2
            ls_copy(v, z, True).wait_recv()
            ls_copy(v, z, False).wait_recv()
            stage[slot] = (
                S[v % NS, z - 1].astype(F32)
                + LR[v % NLR, z].astype(F32)
                + LR[v % NLR, z - 1].astype(F32)
            )
            out_start(v)

            @pl.when(v + NLR < U)
            def _():
                signal(lcredit.at[0], left)
                signal(lcredit.at[1], right)

    def behind(h):
        return jnp.where(h == 0, 0, d.lag + (h - 1) * d.lag2)

    def rs_step(q):
        guarded(q - 1 - behind(z), send_right)
        guarded(q - 1 - behind(n - 1 - z), send_left)
        guarded(q - 1 - behind(jnp.maximum(z, n - 1 - z)), final)

    def p2_copy(u, to_right):
        side = 0 if to_right else 1
        return rcopy(
            dead(u, n - 1 if to_right else 0),
            dead(u, 1 if to_right else n - 2),
            p2_s.at[side],
            p2_r.at[side, u],
            right if to_right else left,
        )

    def p2_side(u, to_right):
        has_prev, has_next = (z >= 2, has_r) if to_right else (z <= n - 3, has_l)
        mine = dead(u, n - 1 if to_right else 0)
        got = dead(u, 1 if to_right else n - 2)
        cp = p2_copy(u, to_right)

        @pl.when(has_prev)
        def _():
            cp.wait_recv()

        @pl.when(has_next)
        def _():
            @pl.when(has_prev)
            def _():
                add_into(mine, got)

            cp.start()

        @pl.when(jnp.logical_not(has_next))
        def _():
            @pl.when(u >= 2)
            def _():
                out_wait(u - 2)

            stage[u % 2] = mine[...].astype(F32) + got[...].astype(F32)
            out_start(u)

    def p2_first(u):
        @pl.when(z == 1)
        def _():
            p2_side(u, True)

        @pl.when(z == n - 2)
        def _():
            p2_side(u, False)

    def p2_step(i):
        @pl.when(z >= 2)
        def _():
            guarded(i - d.hop * (z - 2), lambda u: p2_side(u, True))

        @pl.when(z <= n - 3)
        def _():
            guarded(i - d.hop * (n - 3 - z), lambda u: p2_side(u, False))

    def layer_norm(x):
        mean = jnp.mean(x, axis=-1, keepdims=True)
        cen = x - mean
        inv = lax.rsqrt(jnp.mean(cen * cen, axis=-1, keepdims=True) + norm_eps)
        return cen * inv, inv

    def slabs(first, count, f):
        def one(j, carry):
            f(pl.ds(pl.multiple_of(first + j * SLAB, SLAB), SLAB), first + j * SLAB)
            return carry

        lax.fori_loop(0, count // SLAB, one, 0)

    def ln_block(i):
        def normalize(rows, at):
            normed, _ = layer_norm(A[0, rows, :].astype(F32))
            A[0, rows, :] = (normed * NB[0:1, :] + NB[1:2, :]).astype(BF16)
            A[1, rows, :] = (normed * NB[2:3, :] + NB[3:4, :]).astype(BF16)
            pos = lax.broadcasted_iota(jnp.int32, (SLAB, D), 0) + at
            grad = jnp.where(pos < seq_len, A[2, rows, :].astype(F32), 0.0)
            A[2, rows, :] = grad.astype(BF16)
            SM[4:5, :] += jnp.sum(grad, axis=0, keepdims=True)

        slabs(i * ROWS, ROWS, normalize)
        for a in range(3):
            Acc[a, ds(i, ROWS), :] = jnp.zeros((ROWS, D), F32)

    def y_step(u):
        ag_wait(u)
        w = W[u].reshape(D, UNIT)
        Y[u % 4] = dot(A[aidx(u)], w)

    def acc_step(u):
        a = aidx(u)
        g = G[u % 4]
        for j in range(2 * n):
            cols = slice(j * Dsl, (j + 1) * Dsl)
            Acc[a, :, cols] += dot_nt(g, W[u, j])

    lane = lax.broadcasted_iota(jnp.int32, (T, 128), 1)

    def rotate(y, sign):
        lo = y[:, :128]
        swapped = jnp.where(lane < 32, pltpu.roll(lo, 96, 1), pltpu.roll(lo, 32, 1))
        lo = lo * rope_ref[0] + swapped * (rope_ref[1] * sign)
        return jnp.concatenate([lo, y[:, 128:]], axis=1)

    def attn_core(s):
        u0 = s - 3
        QK[0] = rotate(Y[0] + BI[u0, 0:1, :], 1.0).astype(BF16)
        QK[1] = rotate(Y[1] + BI[u0 + 1, 0:1, :], 1.0).astype(BF16)
        QK[2] = (Y[2] + BI[u0 + 2, 0:1, :]).astype(BF16)
        QK[3] = Y[3].astype(BF16)
        scale = 1.0 / math.sqrt(HD)

        def block(i, carry):
            rows = ds(i, ROWS)
            raw = dot_nt(QK[0, rows, :], QK[1]) * scale
            qpos = lax.broadcasted_iota(jnp.int32, (ROWS, T), 0) + i * ROWS
            kpos = lax.broadcasted_iota(jnp.int32, (ROWS, T), 1)
            scores = jnp.where((kpos <= qpos) & (kpos < seq_len), raw, -jnp.inf)
            top = jnp.max(scores, axis=-1, keepdims=True)
            e = jnp.exp(scores - top)
            p = e / jnp.sum(e, axis=-1, keepdims=True)
            pb = p.astype(BF16)
            PB[rows, :] = pb
            mixed = dot(pb, QK[2]).astype(BF16)
            G[3, rows, :] = mixed
            mg = QK[3, rows, :]
            delta = jnp.sum(mg.astype(F32) * mixed.astype(F32), axis=-1, keepdims=True)
            dp = dot_nt(mg, QK[2])
            dsb = (p * (dp - delta) * scale).astype(BF16)
            DS[rows, :] = dsb
            Y[0, rows, :] = dot(dsb, QK[1])
            return carry

        lax.fori_loop(0, T // ROWS, block, 0)
        Y[1] = dot_tn(DS[...], QK[0])
        for r in range(3):
            if r == 2:
                g = dot_tn(PB[...], QK[3])
            else:
                g = rotate(Y[r], -1.0)
            BG[u0 + r] = jnp.broadcast_to(jnp.sum(g, axis=0, keepdims=True), (8, UNIT))
            G[r] = g.astype(BF16)

    def ffn_core(s):
        b = BI[s - 1, 0:1, :]
        yu, yd = (s - 1) % 4, s % 4
        step = 64

        def block(i, total):
            rows = ds(i, step)
            v = Y[yu, rows, :] + b
            cdf2 = 1.0 + lax.erf(v * (1.0 / math.sqrt(2.0)))
            G[yd, rows, :] = (0.5 * v * cdf2).astype(BF16)
            slope = 0.5 * cdf2 + v * jnp.exp(-0.5 * v * v) * (1.0 / math.sqrt(2.0 * math.pi))
            g = Y[yd, rows, :] * slope
            G[yu, rows, :] = g.astype(BF16)
            return total + jnp.sum(g, axis=0, keepdims=True)

        total = lax.fori_loop(0, T // step, block, jnp.zeros((1, UNIT), F32))
        BG[s - 1] = jnp.broadcast_to(total, (8, UNIT))

    barrier = pltpu.get_barrier_semaphore()
    each_dp(lambda p: signal(barrier, p))
    each_tensor(lambda p: signal(barrier, p, "tensor"))
    x_in = pltpu.make_async_copy(x_hbm, A.at[0], in_sem.at[0])
    c_in = pltpu.make_async_copy(cot_hbm, A.at[2], in_sem.at[1])
    rope_in = pltpu.make_async_copy(rope_hbm, rope_ref, rope_sem.at[0])
    x_in.start()
    c_in.start()
    rope_in.start()
    spots = [
        buf.at[i, r * UNIT : (r + 1) * UNIT, 0:Dsl]
        for buf in (QK, G)
        for i in range(4)
        for r in range(T // UNIT)
    ]
    raws = [
        pltpu.make_async_copy(
            wout.at[i * UNIT : (i + 1) * UNIT, :]
            if i < heads
            else wdown.at[(i - heads) * UNIT : (i - heads + 1) * UNIT, :],
            spots[i],
            raw_sem.at[i],
        )
        for i in range(heads + chunks)
    ]
    for cp in raws:
        cp.start()

    def load_own(u, carry):
        nothing = lambda: None
        by_kind(
            u,
            lambda: own_load(wqkv.at[u % 4, :, ds(head_of(u), UNIT)], u).start(),
            nothing,
            lambda: own_load(wup.at[:, ds(chunk_of(u), UNIT)], u).start(),
            nothing,
        )
        return carry

    lax.fori_loop(0, U, load_own, 0)
    def lanes_of(ref):
        rows = ref[...].astype(F32)
        return jnp.concatenate([rows[i : i + 1] for i in range(rows.shape[0])], axis=1)

    SP[...] = jnp.zeros_like(SP)
    SW[...] = jnp.zeros_like(SW)
    for i, ref in enumerate((ga_ref, sa_ref, gf_ref, sf_ref, ob_ref)):
        SP[i : i + 1, 0:Dsl] = lanes_of(ref)
    SW[0, 0:3, 0 : d.nb] = qb_ref[...].astype(F32)
    SW[1, 0:1, 0 : d.ub] = lanes_of(ub_ref)[:, 0 : d.ub]
    at_q, at_u = me * d.nb, me * d.ub
    qb = pltpu.roll(SW[0], at_q % UNIT, 1)
    ub = pltpu.roll(SW[1], at_u % UNIT, 1)
    for h in range(heads):
        mine = jnp.where(at_q // UNIT == h, 1.0, 0.0)
        SP[8 + 3 * h : 11 + 3 * h, :] = qb[0:3, :] * mine
    for i in range(chunks):
        mine = jnp.where(at_u // UNIT == i, 1.0, 0.0)
        SP[8 + 3 * heads + i : 9 + 3 * heads + i, :] = ub[0:1, :] * mine
    pl.semaphore_wait(barrier, n_dp - 1 + tn - 1)

    def sp_copy(p, where):
        return rcopy(SP, RP.at[where], sp_s.at[0], sp_r.at[where], p)

    each_dp(lambda p: sp_copy(p, me).start())
    RP[me] = SP[...]

    def burst(u, carry):
        ag_own(u, has_r, agR, right)
        ag_own(u, has_l, agL, left)
        ag_self(u)
        return carry

    lax.fori_loop(0, d.burst, burst, 0)
    for i, cp in enumerate(raws):
        cp.wait()
        u = 4 * i + 3 if i < heads else F1 + 2 * (i - heads) + 1
        W[u, me] = jnp.transpose(spots[i][...])

    def end_chip(u, carry):
        @pl.when(z == 0)
        def _():
            ag_own(u, has_r, agR, right)

        @pl.when(z == n - 1)
        def _():
            ag_own(u, has_l, agL, left)

        return carry

    lax.fori_loop(d.burst, U, end_chip, 0)
    SM[...] = jnp.zeros_like(SM)
    BG[...] = jnp.zeros_like(BG)
    BI[...] = jnp.zeros_like(BI)
    each_dp(lambda p: sp_copy(p, p).wait_recv())
    for p in range(n_dp):
        NB[:, p * Dsl : (p + 1) * Dsl] = RP[p, 0:8, 0:Dsl]
    for i in range(3 * heads + chunks):
        row = RP[0, 8 + i : 9 + i, :]
        for p in range(1, n_dp):
            row = row + RP[p, 8 + i : 9 + i, :]
        if i < 3 * heads:
            u = F0 + 4 * (i // 3) + i % 3
        else:
            u = 2 * (i - 3 * heads)
            u = u if u < F0 else u + 4 * heads
        BI[u] = jnp.broadcast_to(row, (8, UNIT))
    x_in.wait()
    c_in.wait()
    rope_in.wait()
    own_all().wait()
    blocks = T // ROWS

    fills = max(ahead(h) for h in range(n - 1))

    def fill(i, carry):
        @pl.when(i < fills)
        def _():
            ag_step(i - fills)

        @pl.when(i < blocks)
        def _():
            ln_block(i)

        return carry

    lax.fori_loop(0, max(fills, blocks), fill, 0)

    def made(s):
        return jnp.maximum(jnp.where(s < F1, s - 2, jnp.where(s == F1, s - 1, s)), 0)

    sent_early = max(0, U - d.held - 1 - d.lag)

    def early(q):
        return jnp.clip(jnp.minimum(2 * (q - d.Q0 + 1), q - d.lag), 0, sent_early)

    def first_one(u, carry):
        p2_first(u)
        return carry

    def make(q, carry):
        dw_sib(q)
        guarded(q - 1, combine)

        @pl.when(q < U - d.held)
        def _():
            rs_step(q)

        acc_step(q)
        dw_own(q)
        lax.fori_loop(early(q - 1), early(q), first_one, 0)
        return carry

    def body(s, carry):
        ag_step(s)
        guarded(s, y_step)

        @pl.when(s == F1 + 2)
        def _():
            x_in.start()

        @pl.when(is_attn(s) & (s % 4 == 3))
        def _():
            attn_core(s)

        @pl.when(jnp.logical_not(is_attn(s)) & (s < U) & (s % 2 == 1))
        def _():
            ffn_core(s)

        lax.fori_loop(made(s - 1), made(s), make, 0)
        return carry

    lax.fori_loop(0, U + 1, body, 0)
    x_in.wait()

    @pl.when(has_r)
    def _():
        signal(ready.at[1], right)

    @pl.when(has_l)
    def _():
        signal(ready.at[0], left)

    lo = d.lo
    hi = tn // lo
    size = ((lo, hi), (hi, lo))
    coord = ((mt % lo, mt // lo), (mt // lo, mt % lo))
    acc_of = (2, 0)
    own = ds(mt, Tr)

    def block_of(k, a, b):
        return b * lo + a if k == 0 else a * lo + b

    def packed(mine, theirs):
        return mine - jnp.where(mine > theirs, 1, 0)

    def s1_copy(k, a, b, sender):
        s2 = size[k][1]
        return rcopy_to(
            A.at[k, ds(block_of(k, a, b), Tr), :],
            pr_hbm.at[k, packed(sender, a) * s2 + b],
            s1_s.at[k, a * s2 + b],
            s1_r.at[k, sender * s2 + b],
            {"tensor": block_of(k, a, coord[k][1])},
        )

    def s1_wait(k, q, b):
        s2 = size[k][1]
        c1 = coord[k][0]
        return rcopy_to(
            A.at[k, own, :],
            pr_hbm.at[k, packed(q, c1) * s2 + b],
            s1_s.at[k, q * s2 + b],
            s1_r.at[k, q * s2 + b],
            {"tensor": block_of(k, q, coord[k][1])},
        )

    def s2_copy(k, b, sender):
        c1 = coord[k][0]
        return rcopy_to(
            A.at[k, ds(block_of(k, c1, b), Tr), :],
            pr_hbm.at[k, d.P1 + packed(sender, b)],
            s2_s.at[k, b],
            s2_r.at[k, sender],
            {"tensor": block_of(k, c1, b)},
        )

    def s2_wait(k, q):
        c1, c2 = coord[k]
        return rcopy_to(
            A.at[k, own, :],
            pr_hbm.at[k, d.P1 + packed(q, c2)],
            s2_s.at[k, q],
            s2_r.at[k, q],
            {"tensor": block_of(k, c1, q)},
        )

    def others(k, which, f):
        for q in range(size[k][which]):

            @pl.when(q != coord[k][which])
            def _(q=q):
                f(q)

    def s1_send(i):
        @pl.when(i >= 0)
        def _():
            for k in range(2):
                a = i % lo if k == 0 else i // lo
                b = i // lo if k == 0 else i % lo

                @pl.when(a != coord[k][0])
                def _(k=k, a=a, b=b):
                    s1_copy(k, a, b, coord[k][0]).start()

    def partial(i, carry):
        @pl.when(i == mt)
        def _():
            A[2, ds((mt + 1) % tn, Tr), :] = A[0, ds(i, Tr), :]

        def rows_of(rows, at):
            normed, _ = layer_norm(A[0, rows, :].astype(F32))
            ab = Acc[0, rows, :]
            fb = Acc[1, rows, :]
            SM[0:1, :] += jnp.sum(ab * normed, axis=0, keepdims=True)
            SM[1:2, :] += jnp.sum(ab, axis=0, keepdims=True)
            SM[2:3, :] += jnp.sum(fb * normed, axis=0, keepdims=True)
            SM[3:4, :] += jnp.sum(fb, axis=0, keepdims=True)
            ng = ab * NB[0:1, :] + fb * NB[2:3, :]
            Acc[0, rows, :] = ng
            A[1, rows, :] = ng.astype(BF16)
            A[0, rows, :] = Acc[2, rows, :].astype(BF16)

        slabs(i * Tr, Tr, rows_of)
        s1_send(i - 1)
        return carry

    lax.fori_loop(0, tn, partial, 0)
    for u in range(U):
        BGC[u : u + 1, :] = BG[u, 0:1, :]
    s1_send(tn - 1)

    def sm_copy(p, where):
        return rcopy(
            SM.at[:, ds(p, Dsl)], RS1.at[where], sm_s.at[0], sm_r.at[0, where], p
        )

    def bg_copy(p, where):
        return rcopy(BGC, RB2.at[where], sm_s.at[1], sm_r.at[1, where], p)

    def small_send(p):
        sm_copy(p, me).start()
        bg_copy(p, me).start()

    each_dp(small_send)
    RS1[me] = SM[:, ds(me, Dsl)]
    RB2[me] = BGC[...]

    @pl.when(has_r)
    def _():
        pl.semaphore_wait(ready.at[0], 1)

    @pl.when(has_l)
    def _():
        pl.semaphore_wait(ready.at[1], 1)

    rest = d.held + d.lag + (n - 3) * d.lag2 + 1
    steps = U + d.hop * (n - 3)

    def p2_count(i):
        fed = jnp.minimum(d.pace * (i + 1), sent_early + i)
        return jnp.clip(jnp.where(i < rest, fed, steps), 0, steps)

    def p2_one(i, carry):
        p2_step(i)
        return carry

    def drain(i, carry):
        rs_step(i + U - d.held)
        guarded(i + sent_early, p2_first)
        lax.fori_loop(p2_count(i - 1), p2_count(i), p2_one, 0)
        return carry

    marks = [min(m, rest) for m in d.marks]
    combine(U - 1)
    lax.fori_loop(0, marks[0], drain, 0)

    def load(k, slot, b):
        return pltpu.make_async_copy(
            pr_hbm.at[k, slot], A.at[k, ds(b, Tr), :], loc_sem.at[k, slot]
        )

    def gather_in(k, do):
        s1, s2 = size[k]
        for b in range(s2):
            do(b, block_of(k, coord[k][0], b))

    for k in range(2):
        s1, s2 = size[k]

        def take(q, k=k, s2=s2):
            for b in range(s2):
                s1_wait(k, q, b).wait_recv()

        others(k, 0, take)
        for q in range(s1 - 1):
            for b in range(s2):
                load(k, q * s2 + b, block_of(k, coord[k][0], b)).start()
            for b in range(s2):
                row_b = block_of(k, coord[k][0], b)
                load(k, q * s2 + b, row_b).wait()
                rows = ds(row_b, Tr)
                Acc[acc_of[k], rows, :] += A[k, rows, :].astype(F32)

        def pass_on(b, k=k):
            rows = ds(block_of(k, coord[k][0], b), Tr)
            A[k, rows, :] = Acc[acc_of[k], rows, :].astype(BF16)
            s2_copy(k, b, coord[k][1]).start()

        others(k, 1, pass_on)

    lax.fori_loop(marks[0], marks[1], drain, 0)

    def small_wait(p):
        sm_copy(p, p).wait_recv()
        bg_copy(p, p).wait_recv()

    each_dp(small_wait)
    total = RS1[0]
    bias_total = RB2[0]
    for p in range(1, n_dp):
        total = total + RS1[p]
        bias_total = bias_total + RB2[p]
    SBT[...] = bias_total
    ST[...] = total

    for k in range(2):
        others(k, 1, lambda q, k=k: s2_wait(k, q).wait_recv())
        for q in range(size[k][1] - 1):
            cp = load(k, d.P1 + q, mt)
            cp.start()
            cp.wait()
            Acc[acc_of[k], own, :] += A[k, own, :].astype(F32)

    def st_copy(p, where):
        return rcopy_to(ST, RT.at[where], st_s.at[0], st_r.at[where], {"tensor": p})

    each_tensor(lambda p: st_copy(p, mt).start())
    def finish(rows, at):
        off = pl.multiple_of((mt + 1) % tn * Tr + at - mt * Tr, SLAB)
        xr = A[2, pl.ds(off, SLAB), :].astype(F32)
        normed, inv = layer_norm(xr)
        ng = Acc[0, rows, :]
        gm = jnp.mean(ng, axis=-1, keepdims=True)
        gp = jnp.mean(ng * normed, axis=-1, keepdims=True)
        A[0, rows, :] = (xr + Acc[2, rows, :] + NB[4:5, :]).astype(BF16)
        A[1, rows, :] = (A[2, rows, :].astype(F32) + inv * (ng - gm - normed * gp)).astype(BF16)

    slabs(mt * Tr, Tr, finish)
    outs = (o_hbm, dx_hbm)

    def f1_copy(k, b, sender):
        c1 = coord[k][0]
        return rcopy_to(
            A.at[k, own, :],
            outs[k].at[ds(block_of(k, c1, sender), Tr), :],
            f1_s.at[k, b],
            f1_r.at[k, sender],
            {"tensor": block_of(k, c1, b)},
        )

    def f2_copy(k, a, b, sender, src):
        s2 = size[k][1]
        return rcopy_to(
            src,
            outs[k].at[ds(block_of(k, sender, b), Tr), :],
            f2_s.at[k, a * s2 + b],
            f2_r.at[k, sender * s2 + b],
            {"tensor": block_of(k, a, coord[k][1])},
        )

    home = [
        pltpu.make_async_copy(A.at[k, own, :], outs[k].at[own, :], in_sem.at[k])
        for k in range(2)
    ]
    for k in range(2):
        c1, c2 = coord[k]
        others(k, 1, lambda b, k=k, c2=c2: f1_copy(k, b, c2).start())
    for k in range(2):
        c1, c2 = coord[k]

        def mine_on(a, k=k, c1=c1, c2=c2):
            f2_copy(k, a, c2, c1, A.at[k, own, :]).start()

        others(k, 0, mine_on)
        home[k].start()
    lax.fori_loop(marks[1], marks[2], drain, 0)
    for k in range(2):
        c1, c2 = coord[k]

        def forward(b, k=k, c1=c1):
            f1_copy(k, b, b).wait_recv()
            rows = ds(block_of(k, c1, b), Tr)
            others(k, 0, lambda a: f2_copy(k, a, b, c1, outs[k].at[rows, :]).start())

        others(k, 1, forward)
    lax.fori_loop(marks[2], rest, drain, 0)
    lax.fori_loop(p2_count(rest - 1), steps, p2_one, 0)

    each_tensor(lambda p: st_copy(p, p).wait_recv())
    RT[mt] = ST[...]
    whole = RT[0]
    for p in range(1, tn):
        whole = whole + RT[p]
    row = lax.broadcasted_iota(jnp.int32, (8, Dsl), 0)
    so_ref[0:8, 0:Dsl] = jnp.where(row < 4, whole, ST[...])

    def share(first, stride, size):
        at = me * size
        one = SBT[pl.ds(first + stride * (at // UNIT), 1), :]
        wide = jnp.broadcast_to(one, (8, UNIT))
        return pltpu.roll(wide, (UNIT - at % UNIT) % UNIT, 1)[0:1, :]

    so_ref[8:9, :] = share(F1, 2, d.ub)
    for r in range(3):
        so_ref[9 + r : 10 + r, :] = share(r, 4, d.nb)

    for k in range(2):
        c1, c2 = coord[k]
        s1, s2 = size[k]

        def end0(q, k=k, c1=c1, s2=s2):
            for b in range(s2):
                s1_copy(k, q, b, c1).wait_send()
                f2_copy(k, q, b, c1, A.at[k, own, :]).wait_send()
                f2_copy(k, q, b, q, A.at[k, own, :]).wait_recv()

        def end1(b, k=k, c2=c2):
            s2_copy(k, b, c2).wait_send()
            f1_copy(k, b, c2).wait_send()

        others(k, 0, end0)
        others(k, 1, end1)

    for buf, sem, count in (
        (RP, sp_s.at[0], n_dp - 1),
        (RS1, sm_s.at[0], n_dp - 1),
        (RB2, sm_s.at[1], n_dp - 1),
        (RT, st_s.at[0], tn - 1),
    ):
        if count:
            span = buf.at[0:count]
            rcopy(span, span, sem, sp_r.at[0], sib).wait_send()
    for cp in home:
        cp.wait()

    ag_finish()

    @pl.when(has_r & has_l)
    def _():
        units_sent(p2_s.at[0])
        units_sent(p2_s.at[1])

    for v in range(max(0, U - NS), U):
        rs_finish(v)
    for v in range(max(0, U - 2), U):
        sb_copy(v).wait_send()
        out_wait(v)


def run_layer(d, seq_len, small, rope, x, cot, wqkv, wout, wup, wdown):
    n, tn, T, D, Dsl, U = d.n, d.tn, d.T, d.D, d.Dsl, d.U
    n_dp = 2 * n
    width, hidden = d.heads * UNIT, d.chunks * UNIT
    rp, up = (8 + 3 * d.heads + d.chunks + 7) // 8 * 8, (U + 7) // 8 * 8
    dma = pltpu.SemaphoreType.DMA
    reg = pltpu.SemaphoreType.REGULAR
    vm = pl.BlockSpec(memory_space=pltpu.VMEM)
    hbm = pl.BlockSpec(memory_space=pl.ANY)
    tile = (Dsl, UNIT)
    return pl.pallas_call(
        functools.partial(layer_kernel, d),
        out_shape=(
            pltpu.VMEM((T, D), BF16),
            jax.ShapeDtypeStruct((T, D), BF16),
            jax.ShapeDtypeStruct((3, Dsl, width), F32),
            jax.ShapeDtypeStruct((width, Dsl), F32),
            jax.ShapeDtypeStruct((Dsl, hidden), F32),
            jax.ShapeDtypeStruct((hidden, Dsl), F32),
            jax.ShapeDtypeStruct((2, d.P1 + d.P2, T // tn, D), BF16),
            jax.ShapeDtypeStruct((16, UNIT), F32),
        ),
        in_specs=[pl.BlockSpec(memory_space=pltpu.SMEM)] + [vm] * 7 + [hbm] * 7,
        out_specs=(hbm,) * 7 + (vm,),
        scratch_shapes=[
            pltpu.VMEM((U, n_dp) + tile, BF16),
            pltpu.VMEM((3, T, D), BF16),
            pltpu.VMEM((2, T, 128), F32),
            pltpu.VMEM((3, T, D), F32),
            pltpu.VMEM((4, T, UNIT), F32),
            pltpu.VMEM((4, T, UNIT), BF16),
            pltpu.VMEM((4, T, UNIT), BF16),
            pltpu.VMEM((T, T), BF16),
            pltpu.VMEM((T, T), BF16),
            pltpu.VMEM((d.NS, n - 2) + tile, BF16),
            pltpu.VMEM((2, n) + tile, BF16),
            pltpu.VMEM((d.NSR, n) + tile, BF16),
            pltpu.VMEM((d.NLR, n) + tile, BF16),
            pltpu.VMEM((2,) + tile, F32),
            pltpu.VMEM((2, UNIT, Dsl), F32),
            pltpu.VMEM((n_dp, rp, UNIT), F32),
            pltpu.VMEM((8, D), F32),
            pltpu.VMEM((U, 8, UNIT), F32),
            pltpu.VMEM((8, D), F32),
            pltpu.VMEM((U, 8, UNIT), F32),
            pltpu.VMEM((up, UNIT), F32),
            pltpu.VMEM((n_dp, 8, Dsl), F32),
            pltpu.VMEM((n_dp, up, UNIT), F32),
            pltpu.VMEM((8, Dsl), F32),
            pltpu.VMEM((tn, 8, Dsl), F32),
            pltpu.VMEM((up, UNIT), F32),
            dma((2,)),
            dma((1,)),
            dma((U, n)),
            dma((U,)),
            dma((n,)),
            dma((n,)),
            dma((n,)),
            reg((2,)),
            reg((2,)),
            dma((2,)),
            dma((d.NSR,)),
            dma((d.NS,)),
            dma((d.NLR, n)),
            dma((2,)),
            dma((1,)),
            dma((n_dp,)),
            dma((2,)),
            dma((2, n_dp)),
            dma((1,)),
            dma((tn,)),
            dma((2, tn)),
            dma((2, tn)),
            dma((2, tn)),
            dma((2, tn)),
            dma((2, tn)),
            dma((2, tn)),
            dma((2, tn)),
            dma((2, tn)),
            dma((2, d.P1 + d.P2)),
            dma((d.heads + d.chunks,)),
            dma((2,)),
            dma((2, U)),
            dma((1,)),
            pltpu.VMEM((rp, UNIT), F32),
            pltpu.VMEM((2, 8, UNIT), F32),
        ],
        compiler_params=pltpu.CompilerParams(
            collective_id=0, has_side_effects=True, vmem_limit_bytes=64_850_000
        ),
        cost_estimate=pl.CostEstimate(
            flops=6 * U * T * D * UNIT,
            bytes_accessed=6 * U * Dsl * UNIT + 8 * T * D,
            transcendentals=T * UNIT * U,
        ),
    )(seq_len, *small, rope, x, cot, wqkv, wout, wup, wdown)


def rope_pair(rows):
    half = ROT // 2
    inv_freq = np.exp(-(2.0 * np.arange(half) / ROT) * math.log(rope_base))
    angles = np.arange(rows)[:, None] * inv_freq[None, :]
    table = np.zeros((2, rows, 128), np.float32)
    table[0] = 1.0
    table[0, :, :half] = table[0, :, half:ROT] = np.cos(angles)
    table[1, :, :half] = -np.sin(angles)
    table[1, :, half:ROT] = np.sin(angles)
    return jnp.asarray(table)


def per_device(
    n_dp,
    tn,
    block_input,
    cotangent,
    lengths,
    attn_gain,
    attn_shift,
    ffn_gain,
    ffn_shift,
    qkv_weight,
    qkv_bias,
    out_weight,
    out_bias,
    up_weight,
    up_bias,
    down_weight,
):
    T, D = block_input.shape
    n = n_dp // 2
    Dsl = D // n_dp
    width = qkv_weight.shape[2]
    heads = width // HD
    hidden = up_weight.shape[1]
    chunks = hidden // UNIT
    U = 4 * heads + 2 * chunks
    F0, lag, lag2 = 0, 5, 2
    nb, ub = qkv_bias.shape[1], up_bias.shape[0]
    hi = 2 if tn % 2 == 0 else 1
    lo = tn // hi
    d = types.SimpleNamespace(
        n=n,
        tn=tn,
        T=T,
        D=D,
        Dsl=Dsl,
        U=U,
        heads=heads,
        chunks=chunks,
        F0=F0,
        held=3,
        ahead=(1, 4, 2),
        own=5,
        burst=3,
        hop=2,
        lag=lag,
        lag2=lag2,
        nb=nb,
        ub=ub,
        pace=3,
        Q0=U - 8,
        NS=min(U, lag + (n - 3) * lag2 + 4),
        NSR=4,
        NLR=min(U, lag + (n - 3) * lag2 + 1),
        lo=lo,
        P1=max((lo - 1) * hi, (hi - 1) * lo),
        P2=max(lo, hi) - 1,
        marks=(3, 4, 5),
    )
    flat = (attn_gain, attn_shift, ffn_gain, ffn_shift, out_bias, jnp.pad(up_bias, (0, -ub % 128)))
    small = [v.reshape(-1, 128) for v in flat] + [qkv_bias]
    out, dx, dqkv, dout, dup, ddown, _, so = run_layer(
        d,
        lengths,
        small,
        rope_pair(T),
        block_input,
        cotangent,
        qkv_weight,
        out_weight,
        up_weight,
        down_weight,
    )
    return (
        out,
        dx,
        so[0, :Dsl],
        so[1, :Dsl],
        so[2, :Dsl],
        so[3, :Dsl],
        dqkv,
        so[9:12, :nb],
        dout,
        so[4, :Dsl],
        dup,
        so[8, :ub],
        ddown,
    )


def solution(mesh):
    in_specs = (
        P("dp", None),
        P("dp", None),
        P("dp"),
        P("dp"),
        P("dp"),
        P("dp"),
        P("dp"),
        P(None, "dp", "tensor"),
        P(None, ("tensor", "dp")),
        P("tensor", "dp"),
        P("dp"),
        P("dp", "tensor"),
        P(("tensor", "dp")),
        P("tensor", "dp"),
    )
    out_specs = (
        P("dp", None),
        P("dp", None),
        P("dp"),
        P("dp"),
        P("dp"),
        P("dp"),
        P(None, "dp", "tensor"),
        P(None, ("tensor", "dp")),
        P("tensor", "dp"),
        P("dp"),
        P("dp", "tensor"),
        P(("tensor", "dp")),
        P("tensor", "dp"),
    )
    return jax.shard_map(
        functools.partial(per_device, mesh.shape["dp"], mesh.shape["tensor"]),
        mesh=mesh,
        in_specs=in_specs,
        out_specs=out_specs,
        check_vma=False,
    )
```

```python
import functools
import math
import types

import jax
import jax.numpy as jnp
import numpy as np
from jax import lax
from jax.experimental import pallas as pl
from jax.experimental.pallas import tpu as pltpu
from jax.sharding import PartitionSpec as P

HD = 256
ROT = 64
UNIT = 256
ROWS = 128
SLAB = 64
MESH = pl.DeviceIdType.MESH

norm_eps = 1e-05
rope_base = 10000.0

F32 = jnp.float32
BF16 = jnp.bfloat16


def dot(a, b):
    return lax.dot_general(a, b, (((1,), (0,)), ((), ())), preferred_element_type=F32)


def dot_nt(a, b):
    return lax.dot_general(a, b, (((1,), (1,)), ((), ())), preferred_element_type=F32)


def dot_tn(a, b):
    return lax.dot_general(a, b, (((0,), (0,)), ((), ())), preferred_element_type=F32)


def ds(i, size):
    return pl.ds(pl.multiple_of(i * size, size), size)


def layer_kernel(
    d,
    len_ref,
    ga_ref,
    sa_ref,
    gf_ref,
    sf_ref,
    ob_ref,
    ub_ref,
    qb_ref,
    rope_hbm,
    x_hbm,
    cot_hbm,
    wqkv,
    wout,
    wup,
    wdown,
    o_hbm,
    dx_hbm,
    dqkv_hbm,
    dout_hbm,
    dup_hbm,
    ddown_hbm,
    pr_hbm,
    so_ref,
    W,
    A,
    rope_ref,
    Acc,
    Y,
    G,
    QK,
    PB,
    DS,
    S,
    SB,
    SR,
    LR,
    stage,
    stage_t,
    RP,
    NB,
    BI,
    SM,
    BG,
    BGC,
    RS1,
    RB2,
    ST,
    RT,
    SBT,
    in_sem,
    own_sem,
    line_r,
    sib_r,
    agR,
    agL,
    agS,
    lcredit,
    ready,
    sb_sem,
    sr_sem,
    ls_sem,
    lr_sem,
    out_sem,
    sp_s,
    sp_r,
    sm_s,
    sm_r,
    st_s,
    st_r,
    s1_s,
    s1_r,
    s2_s,
    s2_r,
    f1_s,
    f1_r,
    f2_s,
    f2_r,
    loc_sem,
    raw_sem,
    p2_s,
    p2_r,
    rope_sem,
    SP,
    SW,
):
    n, tn, T, D, Dsl, U, heads = d.n, d.tn, d.T, d.D, d.Dsl, d.U, d.heads
    n_dp, NS, NSR, NLR = 2 * d.n, d.NS, d.NSR, d.NLR
    Tr = T // tn
    F0 = d.F0
    F1 = F0 + 4 * heads
    chunks = d.chunks
    me = lax.axis_index("dp")
    mt = lax.axis_index("tensor")
    z = me // 2
    c = me % 2
    right, left, sib = me + 2, me - 2, z * 2 + (1 - c)
    has_r = z < n - 1
    has_l = z > 0
    seq_len = len_ref[0]

    def rcopy_to(src, dst, ss, rs, where):
        return pltpu.make_async_remote_copy(
            src_ref=src,
            dst_ref=dst,
            send_sem=ss,
            recv_sem=rs,
            device_id=where,
            device_id_type=MESH,
        )

    def rcopy(src, dst, ss, rs, dev):
        return rcopy_to(src, dst, ss, rs, {"dp": dev})

    def signal(sem, dev, axis="dp"):
        pl.semaphore_signal(sem, inc=1, device_id={axis: dev}, device_id_type=MESH)

    def is_attn(u):
        return (u >= F0) & (u < F1)

    def chunk_of(u):
        return jnp.where(u < F0, u // 2, (u - 4 * heads) // 2)

    def head_of(u):
        return (u - F0) // 4

    def aidx(u):
        attn = jnp.where(u % 4 == 3, 2, 0)
        ffn = jnp.where(u % 2 == 0, 1, 2)
        return jnp.where(is_attn(u), attn, ffn)

    def by_kind(u, qkv, o, up, down):
        ffn = jnp.logical_not(is_attn(u))

        @pl.when(is_attn(u) & (u % 4 != 3))
        def _():
            qkv()

        @pl.when(is_attn(u) & (u % 4 == 3))
        def _():
            o()

        @pl.when(ffn & (u % 2 == 0))
        def _():
            up()

        @pl.when(ffn & (u % 2 == 1))
        def _():
            down()

    def each_dp(f):
        for p in range(n_dp):

            @pl.when(p != me)
            def _(p=p):
                f(p)

    def each_tensor(f):
        for p in range(tn):

            @pl.when(p != mt)
            def _(p=p):
                f(p)

    def own_tile(u, f):
        by_kind(
            u,
            lambda: f(wqkv.at[u % 4, :, ds(head_of(u), UNIT)]),
            lambda: f(W.at[u, me]),
            lambda: f(wup.at[:, ds(chunk_of(u), UNIT)]),
            lambda: f(W.at[u, me]),
        )

    def to_line(u, j, src, sems, dev):
        return rcopy(src, W.at[u, j * 2 + c], sems.at[j], line_r.at[u, j], dev)

    def to_sib(u, j, src):
        return rcopy(src, W.at[u, j * 2 + c], agS.at[j], sib_r.at[u], sib)

    def own_all():
        span = W.at[0 : 3 * heads + chunks, 0]
        return pltpu.make_async_copy(span, span, own_sem.at[0])

    def own_load(src, u):
        return pltpu.make_async_copy(src, W.at[u, me], own_sem.at[0])

    def ag_self(u):
        def go(src):
            to_sib(u, z, src).start()

        own_tile(u, go)

    def ag_own(u, has_next, sems, dev):
        @pl.when(has_next)
        def _():
            def go(src):
                to_line(u, z, src, sems, dev).start()

            own_tile(u, go)

    def relay(u, j, has_next, sems, dev):
        tile = W.at[u, j * 2 + c]
        to_line(u, j, tile, sems, dev).wait_recv()

        @pl.when(has_next)
        def _():
            to_line(u, j, tile, sems, dev).start()

        to_sib(u, j, tile).start()

    def ag_line(u, has_next, sems, dev, sign):
        for k in range(1, n):
            j = z + sign * k

            @pl.when((j >= 0) & (j < n))
            def _(j=j):
                relay(u, j, has_next, sems, dev)

    def guarded(v, f):
        @pl.when((v >= 0) & (v < U))
        def _():
            f(v)

    def ahead(h):
        return d.ahead[0] if h == 0 else d.ahead[1] + d.ahead[2] * (h - 1)

    def ahead_of(h):
        total = jnp.int32(0)
        for k in range(n):
            total = jnp.where(h == k, ahead(k), total)
        return total

    to_r, to_l = n - 1 - z, z

    def ag_step(s):
        def late(v, f):
            @pl.when((v >= d.burst) & (v < U))
            def _():
                f(v)

        late(s + d.own, ag_self)

        @pl.when(has_l)
        def _():
            late(s + ahead_of(to_r) + 1, lambda u: ag_own(u, has_r, agR, right))

        @pl.when(has_r)
        def _():
            late(s + ahead_of(to_l) + 1, lambda u: ag_own(u, has_l, agL, left))

        guarded(s + ahead_of(to_r), lambda u: ag_line(u, has_r, agR, right, -1))
        guarded(s + ahead_of(to_l), lambda u: ag_line(u, has_l, agL, left, 1))

    def ag_wait(u):
        span = W.at[u, 0:n]
        rcopy(span, span, agS.at[0], sib_r.at[u], sib).wait_recv()

    def units_sent(sem):
        span = W.at[:, 0]
        rcopy(span, span, sem, line_r.at[0, 0], sib).wait_send()

    def ag_finish():
        for j in range(n):

            @pl.when(has_r & (j <= z))
            def _(j=j):
                units_sent(agR.at[j])

            @pl.when(has_l & (j >= z))
            def _(j=j):
                units_sent(agL.at[j])

            units_sent(agS.at[j])

    def dead(v, j):
        return W.at[v, j * 2 + 1 - c]

    def part_ref(v, zt):
        if zt == 0 or zt == n - 1:
            return dead(v, zt)
        return S.at[v % NS, zt - 1]

    def sb_copy(u):
        return rcopy(SB.at[u % 2], SR.at[u % NSR], sb_sem.at[u % 2], sr_sem.at[u % NSR], sib)

    def ls_copy(v, zt, to_right):
        slot = zt if to_right else (zt - 1) % n
        if isinstance(zt, int):
            src = part_ref(v, zt)
        else:
            src = S.at[v % NS, zt - 1]
        return rcopy(
            src,
            LR.at[v % NLR, slot],
            ls_sem.at[v % NS],
            lr_sem.at[v % NLR, slot],
            right if to_right else left,
        )

    def dw_half(u, core, put):
        a = aidx(u)
        g = G[u % 4]
        for j in range(n):
            put(j, dot_tn(A[a, :, ds(j * 2 + core, Dsl)], g).astype(BF16))

    def dw_sib(u):
        @pl.when(u >= 2)
        def _():
            sb_copy(u - 2).wait_send()

        def put(j, v):
            SB[u % 2, j] = v

        dw_half(u, 1 - c, put)
        sb_copy(u).start()

    def rs_finish(v):
        def sent(count):
            span = W.at[0, 0:count]
            rcopy(span, span, ls_sem.at[v % NS], line_r.at[0, 0], sib).wait_send()

        ends = (z == 0) | (z == n - 1)
        pl.when(ends)(lambda: sent(n - 1))
        pl.when(jnp.logical_not(ends))(lambda: sent(n - 3))

    def dw_own(u):
        @pl.when(u >= NS)
        def _():
            rs_finish(u - NS)

        def put(j, v):
            part_ref(u, j)[...] = v

        dw_half(u, c, put)

    def add_into(ref, other):
        ref[...] = (ref[...].astype(F32) + other[...].astype(F32)).astype(BF16)

    def combine(v):
        sb_copy(v).wait_recv()
        for zt in range(n):
            add_into(part_ref(v, zt), SR.at[v % NSR, zt])

    def send_right(v):
        @pl.when((z + 1 <= n - 2) & (v >= NLR))
        def _():
            pl.semaphore_wait(lcredit.at[0], 1)

        for zt in range(1, n):
            inner = zt < n - 1

            def take(zt=zt):
                ls_copy(v, zt, True).wait_recv()
                add_into(part_ref(v, zt), LR.at[v % NLR, zt])

            def go(zt=zt):
                ls_copy(v, zt, True).start()

            if inner:

                @pl.when(zt > z)
                def _(take=take, go=go):
                    pl.when(has_l)(take)
                    go()

            else:
                pl.when(z == 0)(go)
                pl.when(z == 1)(take)

    def send_left(v):
        @pl.when((z - 1 >= 1) & (v >= NLR))
        def _():
            pl.semaphore_wait(lcredit.at[1], 1)

        for zt in range(n - 2, -1, -1):
            inner = zt > 0

            def take(zt=zt):
                ls_copy(v, zt, False).wait_recv()
                add_into(part_ref(v, zt), LR.at[v % NLR, (zt - 1) % n])

            def go(zt=zt):
                ls_copy(v, zt, False).start()

            if inner:

                @pl.when(zt < z)
                def _(take=take, go=go):
                    pl.when(has_r)(take)
                    go()

            else:
                pl.when(z == n - 1)(go)
                pl.when(z == n - 2)(take)

    def out_wait(v):
        pltpu.make_async_copy(
            stage.at[v % 2], dup_hbm.at[:, 0:UNIT], out_sem.at[v % 2]
        ).wait()

    def out_start(v):
        slot = v % 2

        def put(src, dst):
            pltpu.make_async_copy(src.at[slot], dst, out_sem.at[slot]).start()

        @pl.when(is_attn(v) & (v % 4 == 3) | jnp.logical_not(is_attn(v)) & (v % 2 == 1))
        def _():
            stage_t[slot] = jnp.transpose(stage[slot])

        by_kind(
            v,
            lambda: put(stage, dqkv_hbm.at[v % 4, :, ds(head_of(v), UNIT)]),
            lambda: put(stage_t, dout_hbm.at[ds(head_of(v), UNIT), :]),
            lambda: put(stage, dup_hbm.at[:, ds(chunk_of(v), UNIT)]),
            lambda: put(stage_t, ddown_hbm.at[ds(chunk_of(v), UNIT), :]),
        )

    def final(v):
        @pl.when((z >= 1) & (z <= n - 2))
        def _():
            @pl.when(v >= 2)
            def _():
                out_wait(v - 2)

            slot = v % 2
            ls_copy(v, z, True).wait_recv()
            ls_copy(v, z, False).wait_recv()
            stage[slot] = (
                S[v % NS, z - 1].astype(F32)
                + LR[v % NLR, z].astype(F32)
                + LR[v % NLR, z - 1].astype(F32)
            )
            out_start(v)

            @pl.when(v + NLR < U)
            def _():
                signal(lcredit.at[0], left)
                signal(lcredit.at[1], right)

    def behind(h):
        return jnp.where(h == 0, 0, d.lag + (h - 1) * d.lag2)

    def rs_step(q):
        guarded(q - 1 - behind(z), send_right)
        guarded(q - 1 - behind(n - 1 - z), send_left)
        guarded(q - 1 - behind(jnp.maximum(z, n - 1 - z)), final)

    def p2_copy(u, to_right):
        side = 0 if to_right else 1
        return rcopy(
            dead(u, n - 1 if to_right else 0),
            dead(u, 1 if to_right else n - 2),
            p2_s.at[side],
            p2_r.at[side, u],
            right if to_right else left,
        )

    def p2_side(u, to_right):
        has_prev, has_next = (z >= 2, has_r) if to_right else (z <= n - 3, has_l)
        mine = dead(u, n - 1 if to_right else 0)
        got = dead(u, 1 if to_right else n - 2)
        cp = p2_copy(u, to_right)

        @pl.when(has_prev)
        def _():
            cp.wait_recv()

        @pl.when(has_next)
        def _():
            @pl.when(has_prev)
            def _():
                add_into(mine, got)

            cp.start()

        @pl.when(jnp.logical_not(has_next))
        def _():
            @pl.when(u >= 2)
            def _():
                out_wait(u - 2)

            stage[u % 2] = mine[...].astype(F32) + got[...].astype(F32)
            out_start(u)

    def p2_first(u):
        @pl.when(z == 1)
        def _():
            p2_side(u, True)

        @pl.when(z == n - 2)
        def _():
            p2_side(u, False)

    def p2_step(i):
        @pl.when(z >= 2)
        def _():
            guarded(i - d.hop * (z - 2), lambda u: p2_side(u, True))

        @pl.when(z <= n - 3)
        def _():
            guarded(i - d.hop * (n - 3 - z), lambda u: p2_side(u, False))

    def layer_norm(x):
        mean = jnp.mean(x, axis=-1, keepdims=True)
        cen = x - mean
        inv = lax.rsqrt(jnp.mean(cen * cen, axis=-1, keepdims=True) + norm_eps)
        return cen * inv, inv

    def slabs(first, count, f):
        def one(j, carry):
            f(pl.ds(pl.multiple_of(first + j * SLAB, SLAB), SLAB), first + j * SLAB)
            return carry

        lax.fori_loop(0, count // SLAB, one, 0)

    def ln_block(i):
        def normalize(rows, at):
            normed, _ = layer_norm(A[0, rows, :].astype(F32))
            A[0, rows, :] = (normed * NB[0:1, :] + NB[1:2, :]).astype(BF16)
            A[1, rows, :] = (normed * NB[2:3, :] + NB[3:4, :]).astype(BF16)
            pos = lax.broadcasted_iota(jnp.int32, (SLAB, D), 0) + at
            grad = jnp.where(pos < seq_len, A[2, rows, :].astype(F32), 0.0)
            A[2, rows, :] = grad.astype(BF16)
            SM[4:5, :] += jnp.sum(grad, axis=0, keepdims=True)

        slabs(i * ROWS, ROWS, normalize)
        for a in range(3):
            Acc[a, ds(i, ROWS), :] = jnp.zeros((ROWS, D), F32)

    def y_step(u):
        ag_wait(u)
        w = W[u].reshape(D, UNIT)
        Y[u % 4] = dot(A[aidx(u)], w)

    def acc_step(u):
        a = aidx(u)
        g = G[u % 4]
        for j in range(2 * n):
            cols = slice(j * Dsl, (j + 1) * Dsl)
            Acc[a, :, cols] += dot_nt(g, W[u, j])

    lane = lax.broadcasted_iota(jnp.int32, (T, 128), 1)

    def rotate(y, sign):
        lo = y[:, :128]
        swapped = jnp.where(lane < 32, pltpu.roll(lo, 96, 1), pltpu.roll(lo, 32, 1))
        table = rope_ref[...]
        cosine = jnp.where(lane < ROT, table, 1.0)
        sine = jnp.where(lane < ROT, pltpu.roll(table, 128 - ROT, 1), 0.0)
        lo = lo * cosine + swapped * (sine * sign)
        return jnp.concatenate([lo, y[:, 128:]], axis=1)

    def attn_core(s):
        u0 = s - 3
        QK[0] = rotate(Y[0] + BI[u0, 0:1, :], 1.0).astype(BF16)
        QK[1] = rotate(Y[1] + BI[u0 + 1, 0:1, :], 1.0).astype(BF16)
        QK[2] = (Y[2] + BI[u0 + 2, 0:1, :]).astype(BF16)
        QK[3] = Y[3].astype(BF16)
        scale = 1.0 / math.sqrt(HD)

        def block(i, carry):
            rows = ds(i, ROWS)
            raw = dot_nt(QK[0, rows, :], QK[1]) * scale
            qpos = lax.broadcasted_iota(jnp.int32, (ROWS, T), 0) + i * ROWS
            kpos = lax.broadcasted_iota(jnp.int32, (ROWS, T), 1)
            scores = jnp.where((kpos <= qpos) & (kpos < seq_len), raw, -jnp.inf)
            top = jnp.max(scores, axis=-1, keepdims=True)
            e = jnp.exp(scores - top)
            p = e / jnp.sum(e, axis=-1, keepdims=True)
            pb = p.astype(BF16)
            PB[rows, :] = pb
            mixed = dot(pb, QK[2]).astype(BF16)
            G[3, rows, :] = mixed
            mg = QK[3, rows, :]
            delta = jnp.sum(mg.astype(F32) * mixed.astype(F32), axis=-1, keepdims=True)
            dp = dot_nt(mg, QK[2])
            dsb = (p * (dp - delta) * scale).astype(BF16)
            DS[rows, :] = dsb
            Y[0, rows, :] = dot(dsb, QK[1])
            return carry

        lax.fori_loop(0, T // ROWS, block, 0)
        Y[1] = dot_tn(DS[...], QK[0])
        for r in range(3):
            if r == 2:
                g = dot_tn(PB[...], QK[3])
            else:
                g = rotate(Y[r], -1.0)
            BG[u0 + r] = jnp.broadcast_to(jnp.sum(g, axis=0, keepdims=True), (8, UNIT))
            G[r] = g.astype(BF16)

    def ffn_core(s):
        b = BI[s - 1, 0:1, :]
        yu, yd = (s - 1) % 4, s % 4
        step = 64

        def block(i, total):
            rows = ds(i, step)
            v = Y[yu, rows, :] + b
            cdf2 = 1.0 + lax.erf(v * (1.0 / math.sqrt(2.0)))
            G[yd, rows, :] = (0.5 * v * cdf2).astype(BF16)
            slope = 0.5 * cdf2 + v * jnp.exp(-0.5 * v * v) * (1.0 / math.sqrt(2.0 * math.pi))
            g = Y[yd, rows, :] * slope
            G[yu, rows, :] = g.astype(BF16)
            return total + jnp.sum(g, axis=0, keepdims=True)

        total = lax.fori_loop(0, T // step, block, jnp.zeros((1, UNIT), F32))
        BG[s - 1] = jnp.broadcast_to(total, (8, UNIT))

    barrier = pltpu.get_barrier_semaphore()
    each_dp(lambda p: signal(barrier, p))
    each_tensor(lambda p: signal(barrier, p, "tensor"))
    x_in = pltpu.make_async_copy(x_hbm, A.at[0], in_sem.at[0])
    c_in = pltpu.make_async_copy(cot_hbm, A.at[2], in_sem.at[1])
    rope_in = pltpu.make_async_copy(rope_hbm, rope_ref, rope_sem.at[0])
    x_in.start()
    c_in.start()
    rope_in.start()
    spots = [
        buf.at[i, r * UNIT : (r + 1) * UNIT, 0:Dsl]
        for buf in (QK, G)
        for i in range(4)
        for r in range(T // UNIT)
    ]
    raws = [
        pltpu.make_async_copy(
            wout.at[i * UNIT : (i + 1) * UNIT, :]
            if i < heads
            else wdown.at[(i - heads) * UNIT : (i - heads + 1) * UNIT, :],
            spots[i],
            raw_sem.at[i],
        )
        for i in range(heads + chunks)
    ]
    for cp in raws:
        cp.start()

    def load_own(u, carry):
        nothing = lambda: None
        by_kind(
            u,
            lambda: own_load(wqkv.at[u % 4, :, ds(head_of(u), UNIT)], u).start(),
            nothing,
            lambda: own_load(wup.at[:, ds(chunk_of(u), UNIT)], u).start(),
            nothing,
        )
        return carry

    lax.fori_loop(0, U, load_own, 0)
    def lanes_of(ref):
        rows = ref[...].astype(F32)
        return jnp.concatenate([rows[i : i + 1] for i in range(rows.shape[0])], axis=1)

    SP[...] = jnp.zeros_like(SP)
    SW[...] = jnp.zeros_like(SW)
    for i, ref in enumerate((ga_ref, sa_ref, gf_ref, sf_ref, ob_ref)):
        SP[i : i + 1, 0:Dsl] = lanes_of(ref)
    SW[0, 0:3, 0 : d.nb] = qb_ref[...].astype(F32)
    SW[1, 0:1, 0 : d.ub] = lanes_of(ub_ref)[:, 0 : d.ub]
    at_q, at_u = me * d.nb, me * d.ub
    qb = pltpu.roll(SW[0], at_q % UNIT, 1)
    ub = pltpu.roll(SW[1], at_u % UNIT, 1)
    for h in range(heads):
        mine = jnp.where(at_q // UNIT == h, 1.0, 0.0)
        SP[8 + 3 * h : 11 + 3 * h, :] = qb[0:3, :] * mine
    for i in range(chunks):
        mine = jnp.where(at_u // UNIT == i, 1.0, 0.0)
        SP[8 + 3 * heads + i : 9 + 3 * heads + i, :] = ub[0:1, :] * mine
    pl.semaphore_wait(barrier, n_dp - 1 + tn - 1)

    def sp_copy(p, where):
        return rcopy(SP, RP.at[where], sp_s.at[0], sp_r.at[where], p)

    each_dp(lambda p: sp_copy(p, me).start())
    RP[me] = SP[...]

    def burst(u, carry):
        ag_own(u, has_r, agR, right)
        ag_own(u, has_l, agL, left)
        ag_self(u)
        return carry

    lax.fori_loop(0, d.burst, burst, 0)
    for i, cp in enumerate(raws):
        cp.wait()
        u = 4 * i + 3 if i < heads else F1 + 2 * (i - heads) + 1
        W[u, me] = jnp.transpose(spots[i][...])

    def end_chip(u, carry):
        @pl.when(z == 0)
        def _():
            ag_own(u, has_r, agR, right)

        @pl.when(z == n - 1)
        def _():
            ag_own(u, has_l, agL, left)

        return carry

    lax.fori_loop(d.burst, U, end_chip, 0)
    SM[...] = jnp.zeros_like(SM)
    BG[...] = jnp.zeros_like(BG)
    BI[...] = jnp.zeros_like(BI)
    each_dp(lambda p: sp_copy(p, p).wait_recv())
    for p in range(n_dp):
        NB[:, p * Dsl : (p + 1) * Dsl] = RP[p, 0:8, 0:Dsl]
    for i in range(3 * heads + chunks):
        row = RP[0, 8 + i : 9 + i, :]
        for p in range(1, n_dp):
            row = row + RP[p, 8 + i : 9 + i, :]
        if i < 3 * heads:
            u = F0 + 4 * (i // 3) + i % 3
        else:
            u = 2 * (i - 3 * heads)
            u = u if u < F0 else u + 4 * heads
        BI[u] = jnp.broadcast_to(row, (8, UNIT))
    x_in.wait()
    c_in.wait()
    rope_in.wait()
    own_all().wait()
    blocks = T // ROWS

    fills = max(ahead(h) for h in range(n - 1))

    def fill(i, carry):
        @pl.when(i < fills)
        def _():
            ag_step(i - fills)

        @pl.when(i < blocks)
        def _():
            ln_block(i)

        return carry

    lax.fori_loop(0, max(fills, blocks), fill, 0)

    def made(s):
        return jnp.maximum(jnp.where(s < F1, s - 2, jnp.where(s == F1, s - 1, s)), 0)

    whole_by = U - d.held - 1 - d.lag
    sent_early = max(0, whole_by)

    def early(q):
        return jnp.clip(jnp.minimum(2 * (q - d.Q0 + 1), q - d.lag), 0, sent_early)

    def first_one(u, carry):
        p2_first(u)
        return carry

    def make(q, carry):
        dw_sib(q)
        guarded(q - 1, combine)

        @pl.when(q < U - d.held)
        def _():
            rs_step(q)

        acc_step(q)
        dw_own(q)
        lax.fori_loop(early(q - 1), early(q), first_one, 0)
        return carry

    def body(s, carry):
        ag_step(s)
        guarded(s, y_step)

        @pl.when(s == F1 + 2)
        def _():
            x_in.start()

        @pl.when(is_attn(s) & (s % 4 == 3))
        def _():
            attn_core(s)

        @pl.when(jnp.logical_not(is_attn(s)) & (s < U) & (s % 2 == 1))
        def _():
            ffn_core(s)

        lax.fori_loop(made(s - 1), made(s), make, 0)
        return carry

    lax.fori_loop(0, U + 1, body, 0)
    x_in.wait()

    @pl.when(has_r)
    def _():
        signal(ready.at[1], right)

    @pl.when(has_l)
    def _():
        signal(ready.at[0], left)

    lo = d.lo
    hi = tn // lo
    size = ((lo, hi), (hi, lo))
    coord = ((mt % lo, mt // lo), (mt // lo, mt % lo))
    acc_of = (2, 0)
    own = ds(mt, Tr)

    def block_of(k, a, b):
        return b * lo + a if k == 0 else a * lo + b

    def packed(mine, theirs):
        return mine - jnp.where(mine > theirs, 1, 0)

    def s1_copy(k, a, b, sender):
        s2 = size[k][1]
        return rcopy_to(
            A.at[k, ds(block_of(k, a, b), Tr), :],
            pr_hbm.at[k, packed(sender, a) * s2 + b],
            s1_s.at[k, a * s2 + b],
            s1_r.at[k, sender * s2 + b],
            {"tensor": block_of(k, a, coord[k][1])},
        )

    def s1_wait(k, q, b):
        s2 = size[k][1]
        c1 = coord[k][0]
        return rcopy_to(
            A.at[k, own, :],
            pr_hbm.at[k, packed(q, c1) * s2 + b],
            s1_s.at[k, q * s2 + b],
            s1_r.at[k, q * s2 + b],
            {"tensor": block_of(k, q, coord[k][1])},
        )

    def s2_copy(k, b, sender):
        c1 = coord[k][0]
        return rcopy_to(
            A.at[k, ds(block_of(k, c1, b), Tr), :],
            pr_hbm.at[k, d.P1 + packed(sender, b)],
            s2_s.at[k, b],
            s2_r.at[k, sender],
            {"tensor": block_of(k, c1, b)},
        )

    def s2_wait(k, q):
        c1, c2 = coord[k]
        return rcopy_to(
            A.at[k, own, :],
            pr_hbm.at[k, d.P1 + packed(q, c2)],
            s2_s.at[k, q],
            s2_r.at[k, q],
            {"tensor": block_of(k, c1, q)},
        )

    def others(k, which, f):
        for q in range(size[k][which]):

            @pl.when(q != coord[k][which])
            def _(q=q):
                f(q)

    def s1_send(j):
        i = block_at(j)

        @pl.when(j >= 0)
        def _():
            for k in range(2):
                a = i % lo if k == 0 else i // lo
                b = i // lo if k == 0 else i % lo

                @pl.when(a != coord[k][0])
                def _(k=k, a=a, b=b):
                    s1_copy(k, a, b, coord[k][0]).start()

    def block_at(j):
        o = tn - 1 - j
        return (mt // lo + o // lo) % hi * lo + (mt % lo + o % lo) % lo

    def partial(j, carry):
        i = block_at(j)

        @pl.when(i == mt)
        def _():
            A[2, ds((mt + 1) % tn, Tr), :] = A[0, ds(i, Tr), :]

        def rows_of(rows, at):
            normed, _ = layer_norm(A[0, rows, :].astype(F32))
            ab = Acc[0, rows, :]
            fb = Acc[1, rows, :]
            SM[0:1, :] += jnp.sum(ab * normed, axis=0, keepdims=True)
            SM[1:2, :] += jnp.sum(ab, axis=0, keepdims=True)
            SM[2:3, :] += jnp.sum(fb * normed, axis=0, keepdims=True)
            SM[3:4, :] += jnp.sum(fb, axis=0, keepdims=True)
            ng = ab * NB[0:1, :] + fb * NB[2:3, :]
            Acc[0, rows, :] = ng
            A[1, rows, :] = ng.astype(BF16)
            A[0, rows, :] = Acc[2, rows, :].astype(BF16)

        slabs(i * Tr, Tr, rows_of)
        s1_send(j - 1)
        return carry

    lax.fori_loop(0, tn, partial, 0)
    for u in range(U):
        BGC[u : u + 1, :] = BG[u, 0:1, :]
    s1_send(tn - 1)

    def sm_copy(p, where):
        return rcopy(
            SM.at[:, ds(p, Dsl)], RS1.at[where], sm_s.at[0], sm_r.at[0, where], p
        )

    def bg_copy(p, where):
        return rcopy(BGC, RB2.at[where], sm_s.at[1], sm_r.at[1, where], p)

    def small_send(p):
        sm_copy(p, me).start()
        bg_copy(p, me).start()

    each_dp(small_send)
    RS1[me] = SM[:, ds(me, Dsl)]
    RB2[me] = BGC[...]

    @pl.when(has_r)
    def _():
        pl.semaphore_wait(ready.at[0], 1)

    @pl.when(has_l)
    def _():
        pl.semaphore_wait(ready.at[1], 1)

    rest = d.held + d.lag + (n - 3) * d.lag2 + 1
    steps = U + d.hop * (n - 3)

    def p2_count(i):
        fed = jnp.minimum(d.pace * (i + 1), whole_by + i)
        return jnp.clip(jnp.where(i < rest, fed, steps), 0, steps)

    def p2_one(i, carry):
        p2_step(i)
        return carry

    def drain(i, carry):
        rs_step(i + U - d.held)
        guarded(i + whole_by, p2_first)
        lax.fori_loop(p2_count(i - 1), p2_count(i), p2_one, 0)
        return carry

    marks = [min(m, rest) for m in d.marks]
    combine(U - 1)
    lax.fori_loop(0, marks[0], drain, 0)

    def load(k, slot, b):
        return pltpu.make_async_copy(
            pr_hbm.at[k, slot], A.at[k, ds(b, Tr), :], loc_sem.at[k, slot]
        )

    def s1_take(k, b):
        s1, s2 = size[k]
        row_b = block_of(k, coord[k][0], b)
        rows = ds(row_b, Tr)
        others(k, 0, lambda q: s1_wait(k, q, b).wait_recv())
        for q in range(s1 - 1):
            cp = load(k, q * s2 + b, row_b)
            cp.start()
            cp.wait()
            Acc[acc_of[k], rows, :] += A[k, rows, :].astype(F32)

    for k in range(2):

        def pass_on(b, k=k):
            s1_take(k, b)
            rows = ds(block_of(k, coord[k][0], b), Tr)
            A[k, rows, :] = Acc[acc_of[k], rows, :].astype(BF16)
            s2_copy(k, b, coord[k][1]).start()

        others(k, 1, pass_on)

    lax.fori_loop(marks[0], marks[1], drain, 0)

    def small_wait(p):
        sm_copy(p, p).wait_recv()
        bg_copy(p, p).wait_recv()

    each_dp(small_wait)
    total = RS1[0]
    bias_total = RB2[0]
    for p in range(1, n_dp):
        total = total + RS1[p]
        bias_total = bias_total + RB2[p]
    SBT[...] = bias_total
    ST[...] = total

    for k in range(2):
        s1_take(k, coord[k][1])
        others(k, 1, lambda q, k=k: s2_wait(k, q).wait_recv())
        for q in range(size[k][1] - 1):
            cp = load(k, d.P1 + q, mt)
            cp.start()
            cp.wait()
            Acc[acc_of[k], own, :] += A[k, own, :].astype(F32)

    def st_copy(p, where):
        return rcopy_to(ST, RT.at[where], st_s.at[0], st_r.at[where], {"tensor": p})

    each_tensor(lambda p: st_copy(p, mt).start())
    def finish(rows, at):
        off = pl.multiple_of((mt + 1) % tn * Tr + at - mt * Tr, SLAB)
        xr = A[2, pl.ds(off, SLAB), :].astype(F32)
        normed, inv = layer_norm(xr)
        ng = Acc[0, rows, :]
        gm = jnp.mean(ng, axis=-1, keepdims=True)
        gp = jnp.mean(ng * normed, axis=-1, keepdims=True)
        A[0, rows, :] = (xr + Acc[2, rows, :] + NB[4:5, :]).astype(BF16)
        A[1, rows, :] = (A[2, rows, :].astype(F32) + inv * (ng - gm - normed * gp)).astype(BF16)

    slabs(mt * Tr, Tr, finish)
    outs = (o_hbm, dx_hbm)

    def f1_copy(k, b, sender):
        c1 = coord[k][0]
        return rcopy_to(
            A.at[k, own, :],
            outs[k].at[ds(block_of(k, c1, sender), Tr), :],
            f1_s.at[k, b],
            f1_r.at[k, sender],
            {"tensor": block_of(k, c1, b)},
        )

    def f2_copy(k, a, b, sender, src):
        s2 = size[k][1]
        return rcopy_to(
            src,
            outs[k].at[ds(block_of(k, sender, b), Tr), :],
            f2_s.at[k, a * s2 + b],
            f2_r.at[k, sender * s2 + b],
            {"tensor": block_of(k, a, coord[k][1])},
        )

    home = [
        pltpu.make_async_copy(A.at[k, own, :], outs[k].at[own, :], in_sem.at[k])
        for k in range(2)
    ]
    for k in range(2):
        c1, c2 = coord[k]
        others(k, 1, lambda b, k=k, c2=c2: f1_copy(k, b, c2).start())
    for k in range(2):
        c1, c2 = coord[k]

        def mine_on(a, k=k, c1=c1, c2=c2):
            f2_copy(k, a, c2, c1, A.at[k, own, :]).start()

        others(k, 0, mine_on)
        home[k].start()
    lax.fori_loop(marks[1], marks[2], drain, 0)
    for k in range(2):
        c1, c2 = coord[k]

        def forward(b, k=k, c1=c1):
            f1_copy(k, b, b).wait_recv()
            rows = ds(block_of(k, c1, b), Tr)
            others(k, 0, lambda a: f2_copy(k, a, b, c1, outs[k].at[rows, :]).start())

        others(k, 1, forward)
    lax.fori_loop(marks[2], rest, drain, 0)
    lax.fori_loop(p2_count(rest - 1), steps, p2_one, 0)

    each_tensor(lambda p: st_copy(p, p).wait_recv())
    RT[mt] = ST[...]
    whole = RT[0]
    for p in range(1, tn):
        whole = whole + RT[p]
    row = lax.broadcasted_iota(jnp.int32, (8, Dsl), 0)
    so_ref[0:8, 0:Dsl] = jnp.where(row < 4, whole, ST[...])

    def share(first, stride, size):
        at = me * size
        one = SBT[pl.ds(first + stride * (at // UNIT), 1), :]
        wide = jnp.broadcast_to(one, (8, UNIT))
        return pltpu.roll(wide, (UNIT - at % UNIT) % UNIT, 1)[0:1, :]

    so_ref[8:9, :] = share(F1, 2, d.ub)
    for r in range(3):
        so_ref[9 + r : 10 + r, :] = share(r, 4, d.nb)

    for k in range(2):
        c1, c2 = coord[k]
        s1, s2 = size[k]

        def end0(q, k=k, c1=c1, s2=s2):
            for b in range(s2):
                s1_copy(k, q, b, c1).wait_send()
                f2_copy(k, q, b, c1, A.at[k, own, :]).wait_send()
                f2_copy(k, q, b, q, A.at[k, own, :]).wait_recv()

        def end1(b, k=k, c2=c2):
            s2_copy(k, b, c2).wait_send()
            f1_copy(k, b, c2).wait_send()

        others(k, 0, end0)
        others(k, 1, end1)

    for buf, sem, count in (
        (RP, sp_s.at[0], n_dp - 1),
        (RS1, sm_s.at[0], n_dp - 1),
        (RB2, sm_s.at[1], n_dp - 1),
        (RT, st_s.at[0], tn - 1),
    ):
        if count:
            span = buf.at[0:count]
            rcopy(span, span, sem, sp_r.at[0], sib).wait_send()
    for cp in home:
        cp.wait()

    ag_finish()

    @pl.when(has_r & has_l)
    def _():
        units_sent(p2_s.at[0])
        units_sent(p2_s.at[1])

    for v in range(max(0, U - NS), U):
        rs_finish(v)
    for v in range(max(0, U - 2), U):
        sb_copy(v).wait_send()
        out_wait(v)


def run_layer(d, seq_len, small, rope, x, cot, wqkv, wout, wup, wdown):
    n, tn, T, D, Dsl, U = d.n, d.tn, d.T, d.D, d.Dsl, d.U
    n_dp = 2 * n
    width, hidden = d.heads * UNIT, d.chunks * UNIT
    rp, up = (8 + 3 * d.heads + d.chunks + 7) // 8 * 8, (U + 7) // 8 * 8
    dma = pltpu.SemaphoreType.DMA
    reg = pltpu.SemaphoreType.REGULAR
    vm = pl.BlockSpec(memory_space=pltpu.VMEM)
    hbm = pl.BlockSpec(memory_space=pl.ANY)
    tile = (Dsl, UNIT)
    return pl.pallas_call(
        functools.partial(layer_kernel, d),
        out_shape=(
            pltpu.VMEM((T, D), BF16),
            jax.ShapeDtypeStruct((T, D), BF16),
            jax.ShapeDtypeStruct((3, Dsl, width), F32),
            jax.ShapeDtypeStruct((width, Dsl), F32),
            jax.ShapeDtypeStruct((Dsl, hidden), F32),
            jax.ShapeDtypeStruct((hidden, Dsl), F32),
            jax.ShapeDtypeStruct((2, d.P1 + d.P2, T // tn, D), BF16),
            jax.ShapeDtypeStruct((16, UNIT), F32),
        ),
        in_specs=[pl.BlockSpec(memory_space=pltpu.SMEM)] + [vm] * 7 + [hbm] * 7,
        out_specs=(hbm,) * 7 + (vm,),
        scratch_shapes=[
            pltpu.VMEM((U, n_dp) + tile, BF16),
            pltpu.VMEM((3, T, D), BF16),
            pltpu.VMEM((T, 128), F32),
            pltpu.VMEM((3, T, D), F32),
            pltpu.VMEM((4, T, UNIT), F32),
            pltpu.VMEM((4, T, UNIT), BF16),
            pltpu.VMEM((4, T, UNIT), BF16),
            pltpu.VMEM((T, T), BF16),
            pltpu.VMEM((T, T), BF16),
            pltpu.VMEM((d.NS, n - 2) + tile, BF16),
            pltpu.VMEM((2, n) + tile, BF16),
            pltpu.VMEM((d.NSR, n) + tile, BF16),
            pltpu.VMEM((d.NLR, n) + tile, BF16),
            pltpu.VMEM((2,) + tile, F32),
            pltpu.VMEM((2, UNIT, Dsl), F32),
            pltpu.VMEM((n_dp, rp, UNIT), F32),
            pltpu.VMEM((8, D), F32),
            pltpu.VMEM((U, 8, UNIT), F32),
            pltpu.VMEM((8, D), F32),
            pltpu.VMEM((U, 8, UNIT), F32),
            pltpu.VMEM((up, UNIT), F32),
            pltpu.VMEM((n_dp, 8, Dsl), F32),
            pltpu.VMEM((n_dp, up, UNIT), F32),
            pltpu.VMEM((8, Dsl), F32),
            pltpu.VMEM((tn, 8, Dsl), F32),
            pltpu.VMEM((up, UNIT), F32),
            dma((2,)),
            dma((1,)),
            dma((U, n)),
            dma((U,)),
            dma((n,)),
            dma((n,)),
            dma((n,)),
            reg((2,)),
            reg((2,)),
            dma((2,)),
            dma((d.NSR,)),
            dma((d.NS,)),
            dma((d.NLR, n)),
            dma((2,)),
            dma((1,)),
            dma((n_dp,)),
            dma((2,)),
            dma((2, n_dp)),
            dma((1,)),
            dma((tn,)),
            dma((2, tn)),
            dma((2, tn)),
            dma((2, tn)),
            dma((2, tn)),
            dma((2, tn)),
            dma((2, tn)),
            dma((2, tn)),
            dma((2, tn)),
            dma((2, d.P1 + d.P2)),
            dma((d.heads + d.chunks,)),
            dma((2,)),
            dma((2, U)),
            dma((1,)),
            pltpu.VMEM((rp, UNIT), F32),
            pltpu.VMEM((2, 8, UNIT), F32),
        ],
        compiler_params=pltpu.CompilerParams(
            collective_id=0, has_side_effects=True, vmem_limit_bytes=64_850_000
        ),
        cost_estimate=pl.CostEstimate(
            flops=6 * U * T * D * UNIT,
            bytes_accessed=6 * U * Dsl * UNIT + 8 * T * D,
            transcendentals=T * UNIT * U,
        ),
    )(seq_len, *small, rope, x, cot, wqkv, wout, wup, wdown)


def rope_pair(rows):
    half = ROT // 2
    inv_freq = np.exp(-(2.0 * np.arange(half) / ROT) * math.log(rope_base))
    angles = np.arange(rows)[:, None] * inv_freq[None, :]
    cosine, sine = np.cos(angles), np.sin(angles)
    table = np.concatenate([cosine, cosine, -sine, sine], axis=1).astype(np.float32)
    return jnp.asarray(table)


def per_device(
    n_dp,
    tn,
    block_input,
    cotangent,
    lengths,
    attn_gain,
    attn_shift,
    ffn_gain,
    ffn_shift,
    qkv_weight,
    qkv_bias,
    out_weight,
    out_bias,
    up_weight,
    up_bias,
    down_weight,
):
    T, D = block_input.shape
    n = n_dp // 2
    Dsl = D // n_dp
    width = qkv_weight.shape[2]
    heads = width // HD
    hidden = up_weight.shape[1]
    chunks = hidden // UNIT
    U = 4 * heads + 2 * chunks
    F0, lag, lag2 = 0, 5, 2
    nb, ub = qkv_bias.shape[1], up_bias.shape[0]
    hi = 2 if tn % 2 == 0 else 1
    lo = tn // hi
    d = types.SimpleNamespace(
        n=n,
        tn=tn,
        T=T,
        D=D,
        Dsl=Dsl,
        U=U,
        heads=heads,
        chunks=chunks,
        F0=F0,
        held=3,
        ahead=(1, 4, 2),
        own=5,
        burst=3,
        hop=2,
        lag=lag,
        lag2=lag2,
        nb=nb,
        ub=ub,
        pace=3,
        Q0=U - 8,
        NS=min(U, lag + (n - 3) * lag2 + 4),
        NSR=4,
        NLR=min(U, lag + (n - 3) * lag2 + 1),
        lo=lo,
        P1=max((lo - 1) * hi, (hi - 1) * lo),
        P2=max(lo, hi) - 1,
        marks=(3, 4, 5),
    )
    flat = (attn_gain, attn_shift, ffn_gain, ffn_shift, out_bias, jnp.pad(up_bias, (0, -ub % 128)))
    small = [v.reshape(-1, 128) for v in flat] + [qkv_bias]
    out, dx, dqkv, dout, dup, ddown, _, so = run_layer(
        d,
        lengths,
        small,
        rope_pair(T),
        block_input,
        cotangent,
        qkv_weight,
        out_weight,
        up_weight,
        down_weight,
    )
    return (
        out,
        dx,
        so[0, :Dsl],
        so[1, :Dsl],
        so[2, :Dsl],
        so[3, :Dsl],
        dqkv,
        so[9:12, :nb],
        dout,
        so[4, :Dsl],
        dup,
        so[8, :ub],
        ddown,
    )


def solution(mesh):
    in_specs = (
        P("dp", None),
        P("dp", None),
        P("dp"),
        P("dp"),
        P("dp"),
        P("dp"),
        P("dp"),
        P(None, "dp", "tensor"),
        P(None, ("tensor", "dp")),
        P("tensor", "dp"),
        P("dp"),
        P("dp", "tensor"),
        P(("tensor", "dp")),
        P("tensor", "dp"),
    )
    out_specs = (
        P("dp", None),
        P("dp", None),
        P("dp"),
        P("dp"),
        P("dp"),
        P("dp"),
        P(None, "dp", "tensor"),
        P(None, ("tensor", "dp")),
        P("tensor", "dp"),
        P("dp"),
        P("dp", "tensor"),
        P(("tensor", "dp")),
        P("tensor", "dp"),
    )
    return jax.shard_map(
        functools.partial(per_device, mesh.shape["dp"], mesh.shape["tensor"]),
        mesh=mesh,
        in_specs=in_specs,
        out_specs=out_specs,
        check_vma=False,
    )
```

```python
import functools
import math
import types

import jax
import jax.numpy as jnp
import numpy as np
from jax import lax
from jax.experimental import pallas as pl
from jax.experimental.pallas import tpu as pltpu
from jax.sharding import PartitionSpec as P

HD = 256
ROT = 64
UNIT = 256
ROWS = 128
SLAB = 64
MESH = pl.DeviceIdType.MESH

norm_eps = 1e-05
rope_base = 10000.0

F32 = jnp.float32
BF16 = jnp.bfloat16


def dot(a, b):
    return lax.dot_general(a, b, (((1,), (0,)), ((), ())), preferred_element_type=F32)


def dot_nt(a, b):
    return lax.dot_general(a, b, (((1,), (1,)), ((), ())), preferred_element_type=F32)


def dot_tn(a, b):
    return lax.dot_general(a, b, (((0,), (0,)), ((), ())), preferred_element_type=F32)


def ds(i, size):
    return pl.ds(pl.multiple_of(i * size, size), size)


def layer_kernel(
    d,
    len_ref,
    ga_ref,
    sa_ref,
    gf_ref,
    sf_ref,
    ob_ref,
    ub_ref,
    qb_ref,
    rope_hbm,
    x_hbm,
    cot_hbm,
    wqkv,
    wout,
    wup,
    wdown,
    o_hbm,
    dx_hbm,
    dqkv_hbm,
    dout_hbm,
    dup_hbm,
    ddown_hbm,
    pr_hbm,
    so_ref,
    W,
    A,
    rope_ref,
    Acc,
    Y,
    G,
    QK,
    PB,
    DS,
    S,
    SB,
    SR,
    LR,
    stage,
    stage_t,
    RP,
    NB,
    BI,
    SM,
    BG,
    BGC,
    RS1,
    RB2,
    ST,
    RT,
    SBT,
    in_sem,
    own_sem,
    line_r,
    sib_r,
    agR,
    agL,
    agS,
    lcredit,
    ready,
    sb_sem,
    sr_sem,
    ls_sem,
    lr_sem,
    out_sem,
    sp_s,
    sp_r,
    sm_s,
    sm_r,
    st_s,
    st_r,
    s1_s,
    s1_r,
    s2_s,
    s2_r,
    f1_s,
    f1_r,
    f2_s,
    f2_r,
    loc_sem,
    raw_sem,
    p2_s,
    p2_r,
    rope_sem,
    SP,
    SW,
):
    n, tn, T, D, Dsl, U, heads = d.n, d.tn, d.T, d.D, d.Dsl, d.U, d.heads
    n_dp, NS, NSR, NLR = 2 * d.n, d.NS, d.NSR, d.NLR
    Tr = T // tn
    F0 = d.F0
    F1 = F0 + 4 * heads
    chunks = d.chunks
    me = lax.axis_index("dp")
    mt = lax.axis_index("tensor")
    z = me // 2
    c = me % 2
    right, left, sib = me + 2, me - 2, z * 2 + (1 - c)
    has_r = z < n - 1
    has_l = z > 0
    seq_len = len_ref[0]

    def rcopy_to(src, dst, ss, rs, where):
        return pltpu.make_async_remote_copy(
            src_ref=src,
            dst_ref=dst,
            send_sem=ss,
            recv_sem=rs,
            device_id=where,
            device_id_type=MESH,
        )

    def rcopy(src, dst, ss, rs, dev):
        return rcopy_to(src, dst, ss, rs, {"dp": dev})

    def signal(sem, dev, axis="dp"):
        pl.semaphore_signal(sem, inc=1, device_id={axis: dev}, device_id_type=MESH)

    def is_attn(u):
        return (u >= F0) & (u < F1)

    def chunk_of(u):
        return jnp.where(u < F0, u // 2, (u - 4 * heads) // 2)

    def head_of(u):
        return (u - F0) // 4

    def aidx(u):
        attn = jnp.where(u % 4 == 3, 2, 0)
        ffn = jnp.where(u % 2 == 0, 1, 2)
        return jnp.where(is_attn(u), attn, ffn)

    def by_kind(u, qkv, o, up, down):
        ffn = jnp.logical_not(is_attn(u))

        @pl.when(is_attn(u) & (u % 4 != 3))
        def _():
            qkv()

        @pl.when(is_attn(u) & (u % 4 == 3))
        def _():
            o()

        @pl.when(ffn & (u % 2 == 0))
        def _():
            up()

        @pl.when(ffn & (u % 2 == 1))
        def _():
            down()

    def each_dp(f):
        for p in range(n_dp):

            @pl.when(p != me)
            def _(p=p):
                f(p)

    def each_tensor(f):
        for p in range(tn):

            @pl.when(p != mt)
            def _(p=p):
                f(p)

    def own_tile(u, f):
        by_kind(
            u,
            lambda: f(wqkv.at[u % 4, :, ds(head_of(u), UNIT)]),
            lambda: f(W.at[u, me]),
            lambda: f(wup.at[:, ds(chunk_of(u), UNIT)]),
            lambda: f(W.at[u, me]),
        )

    def to_line(u, j, src, sems, dev):
        return rcopy(src, W.at[u, j * 2 + c], sems.at[j], line_r.at[u, j], dev)

    def to_sib(u, j, src):
        return rcopy(src, W.at[u, j * 2 + c], agS.at[j], sib_r.at[u], sib)

    def own_all():
        span = W.at[0 : 3 * heads + chunks, 0]
        return pltpu.make_async_copy(span, span, own_sem.at[0])

    def own_load(src, u):
        return pltpu.make_async_copy(src, W.at[u, me], own_sem.at[0])

    def ag_self(u):
        def go(src):
            to_sib(u, z, src).start()

        own_tile(u, go)

    def ag_own(u, has_next, sems, dev):
        @pl.when(has_next)
        def _():
            def go(src):
                to_line(u, z, src, sems, dev).start()

            own_tile(u, go)

    def relay(u, j, has_next, sems, dev):
        tile = W.at[u, j * 2 + c]
        to_line(u, j, tile, sems, dev).wait_recv()

        @pl.when(has_next)
        def _():
            to_line(u, j, tile, sems, dev).start()

        to_sib(u, j, tile).start()

    def ag_line(u, has_next, sems, dev, sign):
        for k in range(1, n):
            j = z + sign * k

            @pl.when((j >= 0) & (j < n))
            def _(j=j):
                relay(u, j, has_next, sems, dev)

    def guarded(v, f):
        @pl.when((v >= 0) & (v < U))
        def _():
            f(v)

    def ahead(h):
        return d.ahead[0] if h == 0 else d.ahead[1] + d.ahead[2] * (h - 1)

    def ahead_of(h):
        total = jnp.int32(0)
        for k in range(n):
            total = jnp.where(h == k, ahead(k), total)
        return total

    to_r, to_l = n - 1 - z, z

    def ag_step(s):
        def late(v, f):
            @pl.when((v >= d.burst) & (v < U))
            def _():
                f(v)

        late(s + d.own, ag_self)

        @pl.when(has_l)
        def _():
            late(s + ahead_of(to_r) + 1, lambda u: ag_own(u, has_r, agR, right))

        @pl.when(has_r)
        def _():
            late(s + ahead_of(to_l) + 1, lambda u: ag_own(u, has_l, agL, left))

        guarded(s + ahead_of(to_r), lambda u: ag_line(u, has_r, agR, right, -1))
        guarded(s + ahead_of(to_l), lambda u: ag_line(u, has_l, agL, left, 1))

    def ag_wait(u):
        span = W.at[u, 0:n]
        rcopy(span, span, agS.at[0], sib_r.at[u], sib).wait_recv()

    def units_sent(sem):
        span = W.at[:, 0]
        rcopy(span, span, sem, line_r.at[0, 0], sib).wait_send()

    def ag_finish():
        for j in range(n):

            @pl.when(has_r & (j <= z))
            def _(j=j):
                units_sent(agR.at[j])

            @pl.when(has_l & (j >= z))
            def _(j=j):
                units_sent(agL.at[j])

            units_sent(agS.at[j])

    def dead(v, j):
        return W.at[v, j * 2 + 1 - c]

    def part_ref(v, zt):
        if zt == 0 or zt == n - 1:
            return dead(v, zt)
        return S.at[v % NS, zt - 1]

    def sb_copy(u):
        return rcopy(SB.at[u % 2], SR.at[u % NSR], sb_sem.at[u % 2], sr_sem.at[u % NSR], sib)

    def ls_copy(v, zt, to_right):
        slot = zt if to_right else (zt - 1) % n
        if isinstance(zt, int):
            src = part_ref(v, zt)
        else:
            src = S.at[v % NS, zt - 1]
        return rcopy(
            src,
            LR.at[v % NLR, slot],
            ls_sem.at[v % NS],
            lr_sem.at[v % NLR, slot],
            right if to_right else left,
        )

    def dw_half(u, core, put):
        a = aidx(u)
        g = G[u % 4]
        for j in range(n):
            put(j, dot_tn(A[a, :, ds(j * 2 + core, Dsl)], g).astype(BF16))

    def dw_sib(u):
        @pl.when(u >= 2)
        def _():
            sb_copy(u - 2).wait_send()

        def put(j, v):
            SB[u % 2, j] = v

        dw_half(u, 1 - c, put)
        sb_copy(u).start()

    def rs_finish(v):
        def sent(count):
            span = W.at[0, 0:count]
            rcopy(span, span, ls_sem.at[v % NS], line_r.at[0, 0], sib).wait_send()

        ends = (z == 0) | (z == n - 1)
        pl.when(ends)(lambda: sent(n - 1))
        pl.when(jnp.logical_not(ends))(lambda: sent(n - 3))

    def dw_own(u):
        @pl.when(u >= NS)
        def _():
            rs_finish(u - NS)

        def put(j, v):
            part_ref(u, j)[...] = v

        dw_half(u, c, put)

    def add_into(ref, other):
        ref[...] = (ref[...].astype(F32) + other[...].astype(F32)).astype(BF16)

    def combine(v):
        sb_copy(v).wait_recv()
        for zt in range(n):
            add_into(part_ref(v, zt), SR.at[v % NSR, zt])

    def send_right(v):
        @pl.when((z + 1 <= n - 2) & (v >= NLR))
        def _():
            pl.semaphore_wait(lcredit.at[0], 1)

        for zt in range(1, n):
            inner = zt < n - 1

            def take(zt=zt):
                ls_copy(v, zt, True).wait_recv()
                add_into(part_ref(v, zt), LR.at[v % NLR, zt])

            def go(zt=zt):
                ls_copy(v, zt, True).start()

            if inner:

                @pl.when(zt > z)
                def _(take=take, go=go):
                    pl.when(has_l)(take)
                    go()

            else:
                pl.when(z == 0)(go)
                pl.when(z == 1)(take)

    def send_left(v):
        @pl.when((z - 1 >= 1) & (v >= NLR))
        def _():
            pl.semaphore_wait(lcredit.at[1], 1)

        for zt in range(n - 2, -1, -1):
            inner = zt > 0

            def take(zt=zt):
                ls_copy(v, zt, False).wait_recv()
                add_into(part_ref(v, zt), LR.at[v % NLR, (zt - 1) % n])

            def go(zt=zt):
                ls_copy(v, zt, False).start()

            if inner:

                @pl.when(zt < z)
                def _(take=take, go=go):
                    pl.when(has_r)(take)
                    go()

            else:
                pl.when(z == n - 1)(go)
                pl.when(z == n - 2)(take)

    def out_wait(v):
        pltpu.make_async_copy(
            stage.at[v % 2], dup_hbm.at[:, 0:UNIT], out_sem.at[v % 2]
        ).wait()

    def out_start(v):
        slot = v % 2

        def put(src, dst):
            pltpu.make_async_copy(src.at[slot], dst, out_sem.at[slot]).start()

        @pl.when(is_attn(v) & (v % 4 == 3) | jnp.logical_not(is_attn(v)) & (v % 2 == 1))
        def _():
            stage_t[slot] = jnp.transpose(stage[slot])

        by_kind(
            v,
            lambda: put(stage, dqkv_hbm.at[v % 4, :, ds(head_of(v), UNIT)]),
            lambda: put(stage_t, dout_hbm.at[ds(head_of(v), UNIT), :]),
            lambda: put(stage, dup_hbm.at[:, ds(chunk_of(v), UNIT)]),
            lambda: put(stage_t, ddown_hbm.at[ds(chunk_of(v), UNIT), :]),
        )

    def final(v):
        @pl.when((z >= 1) & (z <= n - 2))
        def _():
            @pl.when(v >= 2)
            def _():
                out_wait(v - 2)

            slot = v % 2
            ls_copy(v, z, True).wait_recv()
            ls_copy(v, z, False).wait_recv()
            stage[slot] = (
                S[v % NS, z - 1].astype(F32)
                + LR[v % NLR, z].astype(F32)
                + LR[v % NLR, z - 1].astype(F32)
            )
            out_start(v)

            @pl.when(v + NLR < U)
            def _():
                signal(lcredit.at[0], left)
                signal(lcredit.at[1], right)

    def behind(h):
        return jnp.where(h == 0, 0, d.lag + (h - 1) * d.lag2)

    def rs_step(q):
        guarded(q - 1 - behind(z), send_right)
        guarded(q - 1 - behind(n - 1 - z), send_left)
        guarded(q - 1 - behind(jnp.maximum(z, n - 1 - z)), final)

    def p2_copy(u, to_right):
        side = 0 if to_right else 1
        return rcopy(
            dead(u, n - 1 if to_right else 0),
            dead(u, 1 if to_right else n - 2),
            p2_s.at[side],
            p2_r.at[side, u],
            right if to_right else left,
        )

    def p2_side(u, to_right):
        has_prev, has_next = (z >= 2, has_r) if to_right else (z <= n - 3, has_l)
        mine = dead(u, n - 1 if to_right else 0)
        got = dead(u, 1 if to_right else n - 2)
        cp = p2_copy(u, to_right)

        @pl.when(has_prev)
        def _():
            cp.wait_recv()

        @pl.when(has_next)
        def _():
            @pl.when(has_prev)
            def _():
                add_into(mine, got)

            cp.start()

        @pl.when(jnp.logical_not(has_next))
        def _():
            @pl.when(u >= 2)
            def _():
                out_wait(u - 2)

            stage[u % 2] = mine[...].astype(F32) + got[...].astype(F32)
            out_start(u)

    def p2_first(u):
        @pl.when(z == 1)
        def _():
            p2_side(u, True)

        @pl.when(z == n - 2)
        def _():
            p2_side(u, False)

    def p2_step(i):
        @pl.when(z >= 2)
        def _():
            guarded(i - d.hop * (z - 2), lambda u: p2_side(u, True))

        @pl.when(z <= n - 3)
        def _():
            guarded(i - d.hop * (n - 3 - z), lambda u: p2_side(u, False))

    def layer_norm(x):
        mean = jnp.mean(x, axis=-1, keepdims=True)
        cen = x - mean
        inv = lax.rsqrt(jnp.mean(cen * cen, axis=-1, keepdims=True) + norm_eps)
        return cen * inv, inv

    def slabs(first, count, f):
        def one(j, carry):
            f(pl.ds(pl.multiple_of(first + j * SLAB, SLAB), SLAB), first + j * SLAB)
            return carry

        lax.fori_loop(0, count // SLAB, one, 0)

    def ln_block(i):
        def normalize(rows, at):
            normed, _ = layer_norm(A[0, rows, :].astype(F32))
            A[0, rows, :] = (normed * NB[0:1, :] + NB[1:2, :]).astype(BF16)
            A[1, rows, :] = (normed * NB[2:3, :] + NB[3:4, :]).astype(BF16)
            pos = lax.broadcasted_iota(jnp.int32, (SLAB, D), 0) + at
            grad = jnp.where(pos < seq_len, A[2, rows, :].astype(F32), 0.0)
            A[2, rows, :] = grad.astype(BF16)
            SM[4:5, :] += jnp.sum(grad, axis=0, keepdims=True)

        slabs(i * ROWS, ROWS, normalize)
        for a in range(3):
            Acc[a, ds(i, ROWS), :] = jnp.zeros((ROWS, D), F32)

    def y_step(u):
        ag_wait(u)
        w = W[u].reshape(D, UNIT)
        Y[u % 4] = dot(A[aidx(u)], w)

    def acc_step(u):
        a = aidx(u)
        g = G[u % 4]
        for j in range(2 * n):
            cols = slice(j * Dsl, (j + 1) * Dsl)
            Acc[a, :, cols] += dot_nt(g, W[u, j])

    lane = lax.broadcasted_iota(jnp.int32, (T, 128), 1)

    def rotate(y, sign):
        lo = y[:, :128]
        swapped = jnp.where(lane < 32, pltpu.roll(lo, 96, 1), pltpu.roll(lo, 32, 1))
        table = rope_ref[...]
        cosine = jnp.where(lane < ROT, table, 1.0)
        sine = jnp.where(lane < ROT, pltpu.roll(table, 128 - ROT, 1), 0.0)
        lo = lo * cosine + swapped * (sine * sign)
        return jnp.concatenate([lo, y[:, 128:]], axis=1)

    def attn_core(s):
        u0 = s - 3
        QK[0] = rotate(Y[0] + BI[u0, 0:1, :], 1.0).astype(BF16)
        QK[1] = rotate(Y[1] + BI[u0 + 1, 0:1, :], 1.0).astype(BF16)
        QK[2] = (Y[2] + BI[u0 + 2, 0:1, :]).astype(BF16)
        QK[3] = Y[3].astype(BF16)
        scale = 1.0 / math.sqrt(HD)

        def block(i, carry):
            rows = ds(i, ROWS)
            raw = dot_nt(QK[0, rows, :], QK[1]) * scale
            qpos = lax.broadcasted_iota(jnp.int32, (ROWS, T), 0) + i * ROWS
            kpos = lax.broadcasted_iota(jnp.int32, (ROWS, T), 1)
            scores = jnp.where((kpos <= qpos) & (kpos < seq_len), raw, -jnp.inf)
            top = jnp.max(scores, axis=-1, keepdims=True)
            e = jnp.exp(scores - top)
            p = e / jnp.sum(e, axis=-1, keepdims=True)
            pb = p.astype(BF16)
            PB[rows, :] = pb
            mixed = dot(pb, QK[2]).astype(BF16)
            G[3, rows, :] = mixed
            mg = QK[3, rows, :]
            delta = jnp.sum(mg.astype(F32) * mixed.astype(F32), axis=-1, keepdims=True)
            dp = dot_nt(mg, QK[2])
            dsb = (p * (dp - delta) * scale).astype(BF16)
            DS[rows, :] = dsb
            Y[0, rows, :] = dot(dsb, QK[1])
            return carry

        lax.fori_loop(0, T // ROWS, block, 0)
        Y[1] = dot_tn(DS[...], QK[0])
        for r in range(3):
            if r == 2:
                g = dot_tn(PB[...], QK[3])
            else:
                g = rotate(Y[r], -1.0)
            BG[u0 + r] = jnp.broadcast_to(jnp.sum(g, axis=0, keepdims=True), (8, UNIT))
            G[r] = g.astype(BF16)

    def ffn_core(s):
        b = BI[s - 1, 0:1, :]
        yu, yd = (s - 1) % 4, s % 4
        step = 64

        def block(i, total):
            rows = ds(i, step)
            v = Y[yu, rows, :] + b
            cdf2 = 1.0 + lax.erf(v * (1.0 / math.sqrt(2.0)))
            G[yd, rows, :] = (0.5 * v * cdf2).astype(BF16)
            slope = 0.5 * cdf2 + v * jnp.exp(-0.5 * v * v) * (1.0 / math.sqrt(2.0 * math.pi))
            g = Y[yd, rows, :] * slope
            G[yu, rows, :] = g.astype(BF16)
            return total + jnp.sum(g, axis=0, keepdims=True)

        total = lax.fori_loop(0, T // step, block, jnp.zeros((1, UNIT), F32))
        BG[s - 1] = jnp.broadcast_to(total, (8, UNIT))

    barrier = pltpu.get_barrier_semaphore()
    each_dp(lambda p: signal(barrier, p))
    each_tensor(lambda p: signal(barrier, p, "tensor"))
    x_in = pltpu.make_async_copy(x_hbm, A.at[0], in_sem.at[0])
    c_in = pltpu.make_async_copy(cot_hbm, A.at[2], in_sem.at[1])
    rope_in = pltpu.make_async_copy(rope_hbm, rope_ref, rope_sem.at[0])
    x_in.start()
    c_in.start()
    rope_in.start()
    spots = [
        buf.at[i, r * UNIT : (r + 1) * UNIT, 0:Dsl]
        for buf in (QK, G)
        for i in range(4)
        for r in range(T // UNIT)
    ]
    raws = [
        pltpu.make_async_copy(
            wout.at[i * UNIT : (i + 1) * UNIT, :]
            if i < heads
            else wdown.at[(i - heads) * UNIT : (i - heads + 1) * UNIT, :],
            spots[i],
            raw_sem.at[i],
        )
        for i in range(heads + chunks)
    ]
    for cp in raws:
        cp.start()

    def load_own(u, carry):
        nothing = lambda: None
        by_kind(
            u,
            lambda: own_load(wqkv.at[u % 4, :, ds(head_of(u), UNIT)], u).start(),
            nothing,
            lambda: own_load(wup.at[:, ds(chunk_of(u), UNIT)], u).start(),
            nothing,
        )
        return carry

    lax.fori_loop(0, U, load_own, 0)
    def lanes_of(ref):
        rows = ref[...].astype(F32)
        return jnp.concatenate([rows[i : i + 1] for i in range(rows.shape[0])], axis=1)

    SP[...] = jnp.zeros_like(SP)
    SW[...] = jnp.zeros_like(SW)
    for i, ref in enumerate((ga_ref, sa_ref, gf_ref, sf_ref, ob_ref)):
        SP[i : i + 1, 0:Dsl] = lanes_of(ref)
    SW[0, 0:3, 0 : d.nb] = qb_ref[...].astype(F32)
    SW[1, 0:1, 0 : d.ub] = lanes_of(ub_ref)[:, 0 : d.ub]
    at_q, at_u = me * d.nb, me * d.ub
    qb = pltpu.roll(SW[0], at_q % UNIT, 1)
    ub = pltpu.roll(SW[1], at_u % UNIT, 1)
    for h in range(heads):
        mine = jnp.where(at_q // UNIT == h, 1.0, 0.0)
        SP[8 + 3 * h : 11 + 3 * h, :] = qb[0:3, :] * mine
    for i in range(chunks):
        mine = jnp.where(at_u // UNIT == i, 1.0, 0.0)
        SP[8 + 3 * heads + i : 9 + 3 * heads + i, :] = ub[0:1, :] * mine
    pl.semaphore_wait(barrier, n_dp - 1 + tn - 1)

    def sp_copy(p, where):
        return rcopy(SP, RP.at[where], sp_s.at[0], sp_r.at[where], p)

    each_dp(lambda p: sp_copy(p, me).start())
    RP[me] = SP[...]

    def burst(u, carry):
        ag_own(u, has_r, agR, right)
        ag_own(u, has_l, agL, left)
        ag_self(u)
        return carry

    lax.fori_loop(0, d.burst, burst, 0)
    for i, cp in enumerate(raws):
        cp.wait()
        u = 4 * i + 3 if i < heads else F1 + 2 * (i - heads) + 1
        W[u, me] = jnp.transpose(spots[i][...])

    def end_chip(u, carry):
        @pl.when(z == 0)
        def _():
            ag_own(u, has_r, agR, right)

        @pl.when(z == n - 1)
        def _():
            ag_own(u, has_l, agL, left)

        return carry

    lax.fori_loop(d.burst, U, end_chip, 0)
    SM[...] = jnp.zeros_like(SM)
    BG[...] = jnp.zeros_like(BG)
    BI[...] = jnp.zeros_like(BI)
    each_dp(lambda p: sp_copy(p, p).wait_recv())
    for p in range(n_dp):
        NB[:, p * Dsl : (p + 1) * Dsl] = RP[p, 0:8, 0:Dsl]
    for i in range(3 * heads + chunks):
        row = RP[0, 8 + i : 9 + i, :]
        for p in range(1, n_dp):
            row = row + RP[p, 8 + i : 9 + i, :]
        if i < 3 * heads:
            u = F0 + 4 * (i // 3) + i % 3
        else:
            u = 2 * (i - 3 * heads)
            u = u if u < F0 else u + 4 * heads
        BI[u] = jnp.broadcast_to(row, (8, UNIT))
    x_in.wait()
    c_in.wait()
    rope_in.wait()
    own_all().wait()
    blocks = T // ROWS

    fills = max(ahead(h) for h in range(n - 1))

    def fill(i, carry):
        @pl.when(i < fills)
        def _():
            ag_step(i - fills)

        @pl.when(i < blocks)
        def _():
            ln_block(i)

        return carry

    lax.fori_loop(0, max(fills, blocks), fill, 0)

    def made(s):
        return jnp.maximum(jnp.where(s < F1, s - 2, jnp.where(s == F1, s - 1, s)), 0)

    whole_by = U - d.held - 1 - d.lag
    sent_early = max(0, whole_by)

    def early(q):
        return jnp.clip(jnp.minimum(2 * (q - d.Q0 + 1), q - d.lag), 0, sent_early)

    def first_one(u, carry):
        p2_first(u)
        return carry

    def make(q, carry):
        dw_sib(q)
        guarded(q - 1, combine)

        @pl.when(q < U - d.held)
        def _():
            rs_step(q)

        acc_step(q)
        dw_own(q)
        lax.fori_loop(early(q - 1), early(q), first_one, 0)
        return carry

    def body(s, carry):
        ag_step(s)
        guarded(s, y_step)

        @pl.when(s == F1 + 2)
        def _():
            x_in.start()

        @pl.when(is_attn(s) & (s % 4 == 3))
        def _():
            attn_core(s)

        @pl.when(jnp.logical_not(is_attn(s)) & (s < U) & (s % 2 == 1))
        def _():
            ffn_core(s)

        lax.fori_loop(made(s - 1), made(s), make, 0)
        return carry

    lax.fori_loop(0, U + 1, body, 0)
    x_in.wait()

    @pl.when(has_r)
    def _():
        signal(ready.at[1], right)

    @pl.when(has_l)
    def _():
        signal(ready.at[0], left)

    lo = d.lo
    hi = tn // lo
    size = ((lo, hi), (hi, lo))
    coord = ((mt % lo, mt // lo), (mt // lo, mt % lo))
    acc_of = (2, 0)
    own = ds(mt, Tr)

    def block_of(k, a, b):
        return b * lo + a if k == 0 else a * lo + b

    def packed(mine, theirs):
        return mine - jnp.where(mine > theirs, 1, 0)

    def s1_copy(k, a, b, sender):
        s2 = size[k][1]
        return rcopy_to(
            A.at[k, ds(block_of(k, a, b), Tr), :],
            pr_hbm.at[k, packed(sender, a) * s2 + b],
            s1_s.at[k, a * s2 + b],
            s1_r.at[k, sender * s2 + b],
            {"tensor": block_of(k, a, coord[k][1])},
        )

    def s1_wait(k, q, b):
        s2 = size[k][1]
        c1 = coord[k][0]
        return rcopy_to(
            A.at[k, own, :],
            pr_hbm.at[k, packed(q, c1) * s2 + b],
            s1_s.at[k, q * s2 + b],
            s1_r.at[k, q * s2 + b],
            {"tensor": block_of(k, q, coord[k][1])},
        )

    def s2_copy(k, b, sender):
        c1 = coord[k][0]
        return rcopy_to(
            A.at[k, ds(block_of(k, c1, b), Tr), :],
            pr_hbm.at[k, d.P1 + packed(sender, b)],
            s2_s.at[k, b],
            s2_r.at[k, sender],
            {"tensor": block_of(k, c1, b)},
        )

    def s2_wait(k, q):
        c1, c2 = coord[k]
        return rcopy_to(
            A.at[k, own, :],
            pr_hbm.at[k, d.P1 + packed(q, c2)],
            s2_s.at[k, q],
            s2_r.at[k, q],
            {"tensor": block_of(k, c1, q)},
        )

    def others(k, which, f):
        for q in range(size[k][which]):

            @pl.when(q != coord[k][which])
            def _(q=q):
                f(q)

    def s1_send(j):
        i = block_at(j)

        @pl.when(j >= 0)
        def _():
            for k in range(2):
                a = i % lo if k == 0 else i // lo
                b = i // lo if k == 0 else i % lo

                @pl.when(a != coord[k][0])
                def _(k=k, a=a, b=b):
                    s1_copy(k, a, b, coord[k][0]).start()

    def block_at(j):
        o = tn - 1 - j
        return (mt // lo + o // lo) % hi * lo + (mt % lo + o % lo) % lo

    def partial(j, carry):
        i = block_at(j)

        @pl.when(i == mt)
        def _():
            A[2, ds((mt + 1) % tn, Tr), :] = A[0, ds(i, Tr), :]

        def rows_of(rows, at):
            normed, _ = layer_norm(A[0, rows, :].astype(F32))
            ab = Acc[0, rows, :]
            fb = Acc[1, rows, :]
            SM[0:1, :] += jnp.sum(ab * normed, axis=0, keepdims=True)
            SM[1:2, :] += jnp.sum(ab, axis=0, keepdims=True)
            SM[2:3, :] += jnp.sum(fb * normed, axis=0, keepdims=True)
            SM[3:4, :] += jnp.sum(fb, axis=0, keepdims=True)
            ng = ab * NB[0:1, :] + fb * NB[2:3, :]
            Acc[0, rows, :] = ng
            A[1, rows, :] = ng.astype(BF16)
            A[0, rows, :] = Acc[2, rows, :].astype(BF16)

        slabs(i * Tr, Tr, rows_of)
        s1_send(j - 1)
        return carry

    lax.fori_loop(0, tn, partial, 0)
    for u in range(U):
        BGC[u : u + 1, :] = BG[u, 0:1, :]
    s1_send(tn - 1)

    def sm_copy(p, where):
        return rcopy(
            SM.at[:, ds(p, Dsl)], RS1.at[where], sm_s.at[0], sm_r.at[0, where], p
        )

    def bg_copy(p, where):
        return rcopy(BGC, RB2.at[where], sm_s.at[1], sm_r.at[1, where], p)

    def small_send(p):
        sm_copy(p, me).start()
        bg_copy(p, me).start()

    each_dp(small_send)
    RS1[me] = SM[:, ds(me, Dsl)]
    RB2[me] = BGC[...]

    @pl.when(has_r)
    def _():
        pl.semaphore_wait(ready.at[0], 1)

    @pl.when(has_l)
    def _():
        pl.semaphore_wait(ready.at[1], 1)

    rest = d.held + d.lag + (n - 3) * d.lag2 + 1
    steps = U + d.hop * (n - 3)

    def p2_count(i):
        fed = jnp.minimum(d.pace * (i + 1), whole_by + i)
        return jnp.clip(jnp.where(i < rest, fed, steps), 0, steps)

    def p2_one(i, carry):
        p2_step(i)
        return carry

    def drain(i, carry):
        rs_step(i + U - d.held)
        guarded(i + whole_by, p2_first)
        lax.fori_loop(p2_count(i - 1), p2_count(i), p2_one, 0)
        return carry

    marks = [min(m, rest) for m in d.marks]
    combine(U - 1)
    lax.fori_loop(0, marks[0], drain, 0)

    def load(k, slot, b):
        return pltpu.make_async_copy(
            pr_hbm.at[k, slot], A.at[k, ds(b, Tr), :], loc_sem.at[k, slot]
        )

    def s1_take(k, b):
        s1, s2 = size[k]
        row_b = block_of(k, coord[k][0], b)
        rows = ds(row_b, Tr)
        others(k, 0, lambda q: s1_wait(k, q, b).wait_recv())
        for q in range(s1 - 1):
            cp = load(k, q * s2 + b, row_b)
            cp.start()
            cp.wait()
            Acc[acc_of[k], rows, :] += A[k, rows, :].astype(F32)

    for k in range(2):

        def pass_on(b, k=k):
            s1_take(k, b)
            rows = ds(block_of(k, coord[k][0], b), Tr)
            A[k, rows, :] = Acc[acc_of[k], rows, :].astype(BF16)
            s2_copy(k, b, coord[k][1]).start()

        others(k, 1, pass_on)

    lax.fori_loop(marks[0], marks[1], drain, 0)

    def small_wait(p):
        sm_copy(p, p).wait_recv()
        bg_copy(p, p).wait_recv()

    each_dp(small_wait)
    total = RS1[0]
    bias_total = RB2[0]
    for p in range(1, n_dp):
        total = total + RS1[p]
        bias_total = bias_total + RB2[p]
    SBT[...] = bias_total
    ST[...] = total

    for k in range(2):
        s1_take(k, coord[k][1])
        others(k, 1, lambda q, k=k: s2_wait(k, q).wait_recv())
        for q in range(size[k][1] - 1):
            cp = load(k, d.P1 + q, mt)
            cp.start()
            cp.wait()
            Acc[acc_of[k], own, :] += A[k, own, :].astype(F32)

    def st_copy(p, where):
        return rcopy_to(ST, RT.at[where], st_s.at[0], st_r.at[where], {"tensor": p})

    each_tensor(lambda p: st_copy(p, mt).start())
    def finish(rows, at):
        off = pl.multiple_of((mt + 1) % tn * Tr + at - mt * Tr, SLAB)
        xr = A[2, pl.ds(off, SLAB), :].astype(F32)
        normed, inv = layer_norm(xr)
        ng = Acc[0, rows, :]
        gm = jnp.mean(ng, axis=-1, keepdims=True)
        gp = jnp.mean(ng * normed, axis=-1, keepdims=True)
        A[0, rows, :] = (xr + Acc[2, rows, :] + NB[4:5, :]).astype(BF16)
        A[1, rows, :] = (A[2, rows, :].astype(F32) + inv * (ng - gm - normed * gp)).astype(BF16)

    slabs(mt * Tr, Tr, finish)
    outs = (o_hbm, dx_hbm)

    def f1_copy(k, b, sender):
        c1 = coord[k][0]
        return rcopy_to(
            A.at[k, own, :],
            outs[k].at[ds(block_of(k, c1, sender), Tr), :],
            f1_s.at[k, b],
            f1_r.at[k, sender],
            {"tensor": block_of(k, c1, b)},
        )

    def f2_copy(k, a, b, sender, src):
        s2 = size[k][1]
        return rcopy_to(
            src,
            outs[k].at[ds(block_of(k, sender, b), Tr), :],
            f2_s.at[k, a * s2 + b],
            f2_r.at[k, sender * s2 + b],
            {"tensor": block_of(k, a, coord[k][1])},
        )

    home = [
        pltpu.make_async_copy(A.at[k, own, :], outs[k].at[own, :], in_sem.at[k])
        for k in range(2)
    ]
    for k in range(2):
        c1, c2 = coord[k]
        others(k, 1, lambda b, k=k, c2=c2: f1_copy(k, b, c2).start())
    for k in range(2):
        c1, c2 = coord[k]

        def mine_on(a, k=k, c1=c1, c2=c2):
            f2_copy(k, a, c2, c1, A.at[k, own, :]).start()

        others(k, 0, mine_on)
        home[k].start()
    lax.fori_loop(marks[1], marks[2], drain, 0)
    for k in range(2):
        c1, c2 = coord[k]

        def forward(b, k=k, c1=c1):
            f1_copy(k, b, b).wait_recv()
            rows = ds(block_of(k, c1, b), Tr)
            others(k, 0, lambda a: f2_copy(k, a, b, c1, outs[k].at[rows, :]).start())

        others(k, 1, forward)
    lax.fori_loop(marks[2], rest, drain, 0)
    lax.fori_loop(p2_count(rest - 1), steps, p2_one, 0)

    each_tensor(lambda p: st_copy(p, p).wait_recv())
    RT[mt] = ST[...]
    whole = RT[0]
    for p in range(1, tn):
        whole = whole + RT[p]
    row = lax.broadcasted_iota(jnp.int32, (8, Dsl), 0)
    so_ref[0:8, 0:Dsl] = jnp.where(row < 4, whole, ST[...])

    def share(first, stride, size):
        at = me * size
        one = SBT[pl.ds(first + stride * (at // UNIT), 1), :]
        wide = jnp.broadcast_to(one, (8, UNIT))
        return pltpu.roll(wide, (UNIT - at % UNIT) % UNIT, 1)[0:1, :]

    so_ref[8:9, :] = share(F1, 2, d.ub)
    for r in range(3):
        so_ref[9 + r : 10 + r, :] = share(r, 4, d.nb)

    for k in range(2):
        c1, c2 = coord[k]
        s1, s2 = size[k]

        def end0(q, k=k, c1=c1, s2=s2):
            for b in range(s2):
                s1_copy(k, q, b, c1).wait_send()
                f2_copy(k, q, b, c1, A.at[k, own, :]).wait_send()
                f2_copy(k, q, b, q, A.at[k, own, :]).wait_recv()

        def end1(b, k=k, c2=c2):
            s2_copy(k, b, c2).wait_send()
            f1_copy(k, b, c2).wait_send()

        others(k, 0, end0)
        others(k, 1, end1)

    for buf, sem, count in (
        (RP, sp_s.at[0], n_dp - 1),
        (RS1, sm_s.at[0], n_dp - 1),
        (RB2, sm_s.at[1], n_dp - 1),
        (RT, st_s.at[0], tn - 1),
    ):
        if count:
            span = buf.at[0:count]
            rcopy(span, span, sem, sp_r.at[0], sib).wait_send()
    for cp in home:
        cp.wait()

    ag_finish()

    @pl.when(has_r & has_l)
    def _():
        units_sent(p2_s.at[0])
        units_sent(p2_s.at[1])

    for v in range(max(0, U - NS), U):
        rs_finish(v)
    for v in range(max(0, U - 2), U):
        sb_copy(v).wait_send()
        out_wait(v)


def run_layer(d, seq_len, small, rope, x, cot, wqkv, wout, wup, wdown):
    n, tn, T, D, Dsl, U = d.n, d.tn, d.T, d.D, d.Dsl, d.U
    n_dp = 2 * n
    width, hidden = d.heads * UNIT, d.chunks * UNIT
    rp, up = (8 + 3 * d.heads + d.chunks + 7) // 8 * 8, (U + 7) // 8 * 8
    dma = pltpu.SemaphoreType.DMA
    reg = pltpu.SemaphoreType.REGULAR
    vm = pl.BlockSpec(memory_space=pltpu.VMEM)
    hbm = pl.BlockSpec(memory_space=pl.ANY)
    tile = (Dsl, UNIT)
    return pl.pallas_call(
        functools.partial(layer_kernel, d),
        out_shape=(
            pltpu.VMEM((T, D), BF16),
            jax.ShapeDtypeStruct((T, D), BF16),
            jax.ShapeDtypeStruct((3, Dsl, width), F32),
            jax.ShapeDtypeStruct((width, Dsl), F32),
            jax.ShapeDtypeStruct((Dsl, hidden), F32),
            jax.ShapeDtypeStruct((hidden, Dsl), F32),
            jax.ShapeDtypeStruct((2, d.P1 + d.P2, T // tn, D), BF16),
            jax.ShapeDtypeStruct((16, UNIT), F32),
        ),
        in_specs=[pl.BlockSpec(memory_space=pltpu.SMEM)] + [vm] * 7 + [hbm] * 7,
        out_specs=(hbm,) * 7 + (vm,),
        scratch_shapes=[
            pltpu.VMEM((U, n_dp) + tile, BF16),
            pltpu.VMEM((3, T, D), BF16),
            pltpu.VMEM((T, 128), F32),
            pltpu.VMEM((3, T, D), F32),
            pltpu.VMEM((4, T, UNIT), F32),
            pltpu.VMEM((4, T, UNIT), BF16),
            pltpu.VMEM((4, T, UNIT), BF16),
            pltpu.VMEM((T, T), BF16),
            pltpu.VMEM((T, T), BF16),
            pltpu.VMEM((d.NS, n - 2) + tile, BF16),
            pltpu.VMEM((2, n) + tile, BF16),
            pltpu.VMEM((d.NSR, n) + tile, BF16),
            pltpu.VMEM((d.NLR, n) + tile, BF16),
            pltpu.VMEM((2,) + tile, F32),
            pltpu.VMEM((2, UNIT, Dsl), F32),
            pltpu.VMEM((n_dp, rp, UNIT), F32),
            pltpu.VMEM((8, D), F32),
            pltpu.VMEM((U, 8, UNIT), F32),
            pltpu.VMEM((8, D), F32),
            pltpu.VMEM((U, 8, UNIT), F32),
            pltpu.VMEM((up, UNIT), F32),
            pltpu.VMEM((n_dp, 8, Dsl), F32),
            pltpu.VMEM((n_dp, up, UNIT), F32),
            pltpu.VMEM((8, Dsl), F32),
            pltpu.VMEM((tn, 8, Dsl), F32),
            pltpu.VMEM((up, UNIT), F32),
            dma((2,)),
            dma((1,)),
            dma((U, n)),
            dma((U,)),
            dma((n,)),
            dma((n,)),
            dma((n,)),
            reg((2,)),
            reg((2,)),
            dma((2,)),
            dma((d.NSR,)),
            dma((d.NS,)),
            dma((d.NLR, n)),
            dma((2,)),
            dma((1,)),
            dma((n_dp,)),
            dma((2,)),
            dma((2, n_dp)),
            dma((1,)),
            dma((tn,)),
            dma((2, tn)),
            dma((2, tn)),
            dma((2, tn)),
            dma((2, tn)),
            dma((2, tn)),
            dma((2, tn)),
            dma((2, tn)),
            dma((2, tn)),
            dma((2, d.P1 + d.P2)),
            dma((d.heads + d.chunks,)),
            dma((2,)),
            dma((2, U)),
            dma((1,)),
            pltpu.VMEM((rp, UNIT), F32),
            pltpu.VMEM((2, 8, UNIT), F32),
        ],
        compiler_params=pltpu.CompilerParams(
            collective_id=0, has_side_effects=True, vmem_limit_bytes=64_850_000
        ),
        cost_estimate=pl.CostEstimate(
            flops=6 * U * T * D * UNIT,
            bytes_accessed=6 * U * Dsl * UNIT + 8 * T * D,
            transcendentals=T * UNIT * U,
        ),
    )(seq_len, *small, rope, x, cot, wqkv, wout, wup, wdown)


def rope_pair(rows):
    half = ROT // 2
    inv_freq = np.exp(-(2.0 * np.arange(half) / ROT) * math.log(rope_base))
    angles = np.arange(rows)[:, None] * inv_freq[None, :]
    cosine, sine = np.cos(angles), np.sin(angles)
    table = np.concatenate([cosine, cosine, -sine, sine], axis=1).astype(np.float32)
    return jnp.asarray(table)


def per_device(
    n_dp,
    tn,
    block_input,
    cotangent,
    lengths,
    attn_gain,
    attn_shift,
    ffn_gain,
    ffn_shift,
    qkv_weight,
    qkv_bias,
    out_weight,
    out_bias,
    up_weight,
    up_bias,
    down_weight,
):
    T, D = block_input.shape
    n = n_dp // 2
    Dsl = D // n_dp
    width = qkv_weight.shape[2]
    heads = width // HD
    hidden = up_weight.shape[1]
    chunks = hidden // UNIT
    U = 4 * heads + 2 * chunks
    F0, lag, lag2 = 0, 5, 1
    nb, ub = qkv_bias.shape[1], up_bias.shape[0]
    hi = 2 if tn % 2 == 0 else 1
    lo = tn // hi
    d = types.SimpleNamespace(
        n=n,
        tn=tn,
        T=T,
        D=D,
        Dsl=Dsl,
        U=U,
        heads=heads,
        chunks=chunks,
        F0=F0,
        held=3,
        ahead=(1, 4, 2),
        own=5,
        burst=3,
        hop=2,
        lag=lag,
        lag2=lag2,
        nb=nb,
        ub=ub,
        pace=3,
        Q0=U - 8,
        NS=min(U, lag + (n - 3) * lag2 + 4),
        NSR=4,
        NLR=min(U, lag + (n - 3) * lag2 + 1),
        lo=lo,
        P1=max((lo - 1) * hi, (hi - 1) * lo),
        P2=max(lo, hi) - 1,
        marks=(3, 4, 6),
    )
    flat = (attn_gain, attn_shift, ffn_gain, ffn_shift, out_bias, jnp.pad(up_bias, (0, -ub % 128)))
    small = [v.reshape(-1, 128) for v in flat] + [qkv_bias]
    out, dx, dqkv, dout, dup, ddown, _, so = run_layer(
        d,
        lengths,
        small,
        rope_pair(T),
        block_input,
        cotangent,
        qkv_weight,
        out_weight,
        up_weight,
        down_weight,
    )
    return (
        out,
        dx,
        so[0, :Dsl],
        so[1, :Dsl],
        so[2, :Dsl],
        so[3, :Dsl],
        dqkv,
        so[9:12, :nb],
        dout,
        so[4, :Dsl],
        dup,
        so[8, :ub],
        ddown,
    )


def solution(mesh):
    in_specs = (
        P("dp", None),
        P("dp", None),
        P("dp"),
        P("dp"),
        P("dp"),
        P("dp"),
        P("dp"),
        P(None, "dp", "tensor"),
        P(None, ("tensor", "dp")),
        P("tensor", "dp"),
        P("dp"),
        P("dp", "tensor"),
        P(("tensor", "dp")),
        P("tensor", "dp"),
    )
    out_specs = (
        P("dp", None),
        P("dp", None),
        P("dp"),
        P("dp"),
        P("dp"),
        P("dp"),
        P(None, "dp", "tensor"),
        P(None, ("tensor", "dp")),
        P("tensor", "dp"),
        P("dp"),
        P("dp", "tensor"),
        P(("tensor", "dp")),
        P("tensor", "dp"),
    )
    return jax.shard_map(
        functools.partial(per_device, mesh.shape["dp"], mesh.shape["tensor"]),
        mesh=mesh,
        in_specs=in_specs,
        out_specs=out_specs,
        check_vma=False,
    )
```

```python
import functools
import math
import types

import jax
import jax.numpy as jnp
import numpy as np
from jax import lax
from jax.experimental import pallas as pl
from jax.experimental.pallas import tpu as pltpu
from jax.sharding import PartitionSpec as P

HD = 256
ROT = 64
UNIT = 256
ROWS = 128
SLAB = 64
MESH = pl.DeviceIdType.MESH

norm_eps = 1e-05
rope_base = 10000.0

F32 = jnp.float32
BF16 = jnp.bfloat16


def dot(a, b):
    return lax.dot_general(a, b, (((1,), (0,)), ((), ())), preferred_element_type=F32)


def dot_nt(a, b):
    return lax.dot_general(a, b, (((1,), (1,)), ((), ())), preferred_element_type=F32)


def dot_tn(a, b):
    return lax.dot_general(a, b, (((0,), (0,)), ((), ())), preferred_element_type=F32)


def ds(i, size):
    return pl.ds(pl.multiple_of(i * size, size), size)


def layer_kernel(
    d,
    len_ref,
    ga_ref,
    sa_ref,
    gf_ref,
    sf_ref,
    ob_ref,
    ub_ref,
    qb_ref,
    rope_hbm,
    x_hbm,
    cot_hbm,
    wqkv,
    wout,
    wup,
    wdown,
    o_hbm,
    dx_hbm,
    dqkv_hbm,
    dout_hbm,
    dup_hbm,
    ddown_hbm,
    pr_hbm,
    so_ref,
    W,
    A,
    rope_ref,
    Acc,
    Y,
    G,
    QK,
    PB,
    DS,
    S,
    SB,
    SR,
    LR,
    stage,
    stage_t,
    RP,
    NB,
    BI,
    SM,
    BG,
    BGC,
    RS1,
    RB2,
    ST,
    RT,
    SBT,
    in_sem,
    own_sem,
    line_r,
    sib_r,
    agR,
    agL,
    agS,
    lcredit,
    ready,
    sb_sem,
    sr_sem,
    ls_sem,
    lr_sem,
    out_sem,
    sp_s,
    sp_r,
    sm_s,
    sm_r,
    st_s,
    st_r,
    s1_s,
    s1_r,
    s2_s,
    s2_r,
    f1_s,
    f1_r,
    f2_s,
    f2_r,
    loc_sem,
    raw_sem,
    p2_s,
    p2_r,
    rope_sem,
    SP,
    SW,
):
    n, tn, T, D, Dsl, U, heads = d.n, d.tn, d.T, d.D, d.Dsl, d.U, d.heads
    n_dp, NS, NSR, NLR = 2 * d.n, d.NS, d.NSR, d.NLR
    Tr = T // tn
    F0 = d.F0
    F1 = F0 + 4 * heads
    chunks = d.chunks
    me = lax.axis_index("dp")
    mt = lax.axis_index("tensor")
    z = me // 2
    c = me % 2
    right, left, sib = me + 2, me - 2, z * 2 + (1 - c)
    has_r = z < n - 1
    has_l = z > 0
    seq_len = len_ref[0]

    def rcopy_to(src, dst, ss, rs, where):
        return pltpu.make_async_remote_copy(
            src_ref=src,
            dst_ref=dst,
            send_sem=ss,
            recv_sem=rs,
            device_id=where,
            device_id_type=MESH,
        )

    def rcopy(src, dst, ss, rs, dev):
        return rcopy_to(src, dst, ss, rs, {"dp": dev})

    def signal(sem, dev, axis="dp"):
        pl.semaphore_signal(sem, inc=1, device_id={axis: dev}, device_id_type=MESH)

    def is_attn(u):
        return (u >= F0) & (u < F1)

    def chunk_of(u):
        return jnp.where(u < F0, u // 2, (u - 4 * heads) // 2)

    def head_of(u):
        return (u - F0) // 4

    def aidx(u):
        attn = jnp.where(u % 4 == 3, 2, 0)
        ffn = jnp.where(u % 2 == 0, 1, 2)
        return jnp.where(is_attn(u), attn, ffn)

    def by_kind(u, qkv, o, up, down):
        ffn = jnp.logical_not(is_attn(u))

        @pl.when(is_attn(u) & (u % 4 != 3))
        def _():
            qkv()

        @pl.when(is_attn(u) & (u % 4 == 3))
        def _():
            o()

        @pl.when(ffn & (u % 2 == 0))
        def _():
            up()

        @pl.when(ffn & (u % 2 == 1))
        def _():
            down()

    def each_dp(f):
        for p in range(n_dp):

            @pl.when(p != me)
            def _(p=p):
                f(p)

    def each_tensor(f):
        for p in range(tn):

            @pl.when(p != mt)
            def _(p=p):
                f(p)

    def own_tile(u, f):
        by_kind(
            u,
            lambda: f(wqkv.at[u % 4, :, ds(head_of(u), UNIT)]),
            lambda: f(W.at[u, me]),
            lambda: f(wup.at[:, ds(chunk_of(u), UNIT)]),
            lambda: f(W.at[u, me]),
        )

    def to_line(u, j, src, sems, dev):
        return rcopy(src, W.at[u, j * 2 + c], sems.at[j], line_r.at[u, j], dev)

    def to_sib(u, j, src):
        return rcopy(src, W.at[u, j * 2 + c], agS.at[j], sib_r.at[u], sib)

    def own_all():
        span = W.at[0 : 3 * heads + chunks, 0]
        return pltpu.make_async_copy(span, span, own_sem.at[0])

    def own_load(src, u):
        return pltpu.make_async_copy(src, W.at[u, me], own_sem.at[0])

    def ag_self(u):
        def go(src):
            to_sib(u, z, src).start()

        own_tile(u, go)

    def ag_own(u, has_next, sems, dev):
        @pl.when(has_next)
        def _():
            def go(src):
                to_line(u, z, src, sems, dev).start()

            own_tile(u, go)

    def relay(u, j, has_next, sems, dev):
        tile = W.at[u, j * 2 + c]
        to_line(u, j, tile, sems, dev).wait_recv()

        @pl.when(has_next)
        def _():
            to_line(u, j, tile, sems, dev).start()

        to_sib(u, j, tile).start()

    def ag_line(u, has_next, sems, dev, sign):
        for k in range(1, n):
            j = z + sign * k

            @pl.when((j >= 0) & (j < n))
            def _(j=j):
                relay(u, j, has_next, sems, dev)

    def guarded(v, f):
        @pl.when((v >= 0) & (v < U))
        def _():
            f(v)

    def ahead(h):
        return d.ahead[0] if h == 0 else d.ahead[1] + d.ahead[2] * (h - 1)

    def ahead_of(h):
        total = jnp.int32(0)
        for k in range(n):
            total = jnp.where(h == k, ahead(k), total)
        return total

    to_r, to_l = n - 1 - z, z

    def ag_step(s):
        def late(v, f):
            @pl.when((v >= d.burst) & (v < U))
            def _():
                f(v)

        late(s + d.own, ag_self)

        @pl.when(has_l)
        def _():
            late(s + ahead_of(to_r) + 1, lambda u: ag_own(u, has_r, agR, right))

        @pl.when(has_r)
        def _():
            late(s + ahead_of(to_l) + 1, lambda u: ag_own(u, has_l, agL, left))

        guarded(s + ahead_of(to_r), lambda u: ag_line(u, has_r, agR, right, -1))
        guarded(s + ahead_of(to_l), lambda u: ag_line(u, has_l, agL, left, 1))

    def ag_wait(u):
        span = W.at[u, 0:n]
        rcopy(span, span, agS.at[0], sib_r.at[u], sib).wait_recv()

    def units_sent(sem):
        span = W.at[:, 0]
        rcopy(span, span, sem, line_r.at[0, 0], sib).wait_send()

    def ag_finish():
        for j in range(n):

            @pl.when(has_r & (j <= z))
            def _(j=j):
                units_sent(agR.at[j])

            @pl.when(has_l & (j >= z))
            def _(j=j):
                units_sent(agL.at[j])

            units_sent(agS.at[j])

    def dead(v, j):
        return W.at[v, j * 2 + 1 - c]

    def part_ref(v, zt):
        if zt == 0 or zt == n - 1:
            return dead(v, zt)
        return S.at[v % NS, zt - 1]

    def sb_copy(u):
        return rcopy(SB.at[u % 2], SR.at[u % NSR], sb_sem.at[u % 2], sr_sem.at[u % NSR], sib)

    def ls_copy(v, zt, to_right):
        slot = zt if to_right else (zt - 1) % n
        if isinstance(zt, int):
            src = part_ref(v, zt)
        else:
            src = S.at[v % NS, zt - 1]
        return rcopy(
            src,
            LR.at[v % NLR, slot],
            ls_sem.at[v % NS],
            lr_sem.at[v % NLR, slot],
            right if to_right else left,
        )

    def dw_half(u, core, put):
        a = aidx(u)
        g = G[u % 4]
        for j in range(n):
            put(j, dot_tn(A[a, :, ds(j * 2 + core, Dsl)], g).astype(BF16))

    def dw_sib(u):
        @pl.when(u >= 2)
        def _():
            sb_copy(u - 2).wait_send()

        def put(j, v):
            SB[u % 2, j] = v

        dw_half(u, 1 - c, put)
        sb_copy(u).start()

    def rs_finish(v):
        def sent(count):
            span = W.at[0, 0:count]
            rcopy(span, span, ls_sem.at[v % NS], line_r.at[0, 0], sib).wait_send()

        ends = (z == 0) | (z == n - 1)
        pl.when(ends)(lambda: sent(n - 1))
        pl.when(jnp.logical_not(ends))(lambda: sent(n - 3))

    def dw_own(u):
        @pl.when(u >= NS)
        def _():
            rs_finish(u - NS)

        def put(j, v):
            part_ref(u, j)[...] = v

        dw_half(u, c, put)

    def add_into(ref, other):
        ref[...] = (ref[...].astype(F32) + other[...].astype(F32)).astype(BF16)

    def combine(v):
        sb_copy(v).wait_recv()
        for zt in range(n):
            add_into(part_ref(v, zt), SR.at[v % NSR, zt])

    def send_right(v):
        @pl.when((z + 1 <= n - 2) & (v >= NLR))
        def _():
            pl.semaphore_wait(lcredit.at[0], 1)

        for zt in range(1, n):
            inner = zt < n - 1

            def take(zt=zt):
                ls_copy(v, zt, True).wait_recv()
                add_into(part_ref(v, zt), LR.at[v % NLR, zt])

            def go(zt=zt):
                ls_copy(v, zt, True).start()

            if inner:

                @pl.when(zt > z)
                def _(take=take, go=go):
                    pl.when(has_l)(take)
                    go()

            else:
                pl.when(z == 0)(go)
                pl.when(z == 1)(take)

    def send_left(v):
        @pl.when((z - 1 >= 1) & (v >= NLR))
        def _():
            pl.semaphore_wait(lcredit.at[1], 1)

        for zt in range(n - 2, -1, -1):
            inner = zt > 0

            def take(zt=zt):
                ls_copy(v, zt, False).wait_recv()
                add_into(part_ref(v, zt), LR.at[v % NLR, (zt - 1) % n])

            def go(zt=zt):
                ls_copy(v, zt, False).start()

            if inner:

                @pl.when(zt < z)
                def _(take=take, go=go):
                    pl.when(has_r)(take)
                    go()

            else:
                pl.when(z == n - 1)(go)
                pl.when(z == n - 2)(take)

    def out_wait(v):
        pltpu.make_async_copy(
            stage.at[v % 2], dup_hbm.at[:, 0:UNIT], out_sem.at[v % 2]
        ).wait()

    def out_start(v):
        slot = v % 2

        def put(src, dst):
            pltpu.make_async_copy(src.at[slot], dst, out_sem.at[slot]).start()

        @pl.when(is_attn(v) & (v % 4 == 3) | jnp.logical_not(is_attn(v)) & (v % 2 == 1))
        def _():
            stage_t[slot] = jnp.transpose(stage[slot])

        by_kind(
            v,
            lambda: put(stage, dqkv_hbm.at[v % 4, :, ds(head_of(v), UNIT)]),
            lambda: put(stage_t, dout_hbm.at[ds(head_of(v), UNIT), :]),
            lambda: put(stage, dup_hbm.at[:, ds(chunk_of(v), UNIT)]),
            lambda: put(stage_t, ddown_hbm.at[ds(chunk_of(v), UNIT), :]),
        )

    def final(v):
        @pl.when((z >= 1) & (z <= n - 2))
        def _():
            @pl.when(v >= 2)
            def _():
                out_wait(v - 2)

            slot = v % 2
            ls_copy(v, z, True).wait_recv()
            ls_copy(v, z, False).wait_recv()
            stage[slot] = (
                S[v % NS, z - 1].astype(F32)
                + LR[v % NLR, z].astype(F32)
                + LR[v % NLR, z - 1].astype(F32)
            )
            out_start(v)

            @pl.when(v + NLR < U)
            def _():
                signal(lcredit.at[0], left)
                signal(lcredit.at[1], right)

    def behind(h):
        return jnp.where(h == 0, 0, d.lag + (h - 1) * d.lag2)

    def rs_step(q):
        guarded(q - 1 - behind(z), send_right)
        guarded(q - 1 - behind(n - 1 - z), send_left)
        guarded(q - 1 - behind(jnp.maximum(z, n - 1 - z)), final)

    def p2_copy(u, to_right):
        side = 0 if to_right else 1
        return rcopy(
            dead(u, n - 1 if to_right else 0),
            dead(u, 1 if to_right else n - 2),
            p2_s.at[side],
            p2_r.at[side, u],
            right if to_right else left,
        )

    def p2_side(u, to_right):
        has_prev, has_next = (z >= 2, has_r) if to_right else (z <= n - 3, has_l)
        mine = dead(u, n - 1 if to_right else 0)
        got = dead(u, 1 if to_right else n - 2)
        cp = p2_copy(u, to_right)

        @pl.when(has_prev)
        def _():
            cp.wait_recv()

        @pl.when(has_next)
        def _():
            @pl.when(has_prev)
            def _():
                add_into(mine, got)

            cp.start()

        @pl.when(jnp.logical_not(has_next))
        def _():
            @pl.when(u >= 2)
            def _():
                out_wait(u - 2)

            stage[u % 2] = mine[...].astype(F32) + got[...].astype(F32)
            out_start(u)

    def p2_first(u):
        @pl.when(z == 1)
        def _():
            p2_side(u, True)

        @pl.when(z == n - 2)
        def _():
            p2_side(u, False)

    def p2_step(i):
        @pl.when(z >= 2)
        def _():
            guarded(i - d.hop * (z - 2), lambda u: p2_side(u, True))

        @pl.when(z <= n - 3)
        def _():
            guarded(i - d.hop * (n - 3 - z), lambda u: p2_side(u, False))

    def layer_norm(x):
        mean = jnp.mean(x, axis=-1, keepdims=True)
        cen = x - mean
        inv = lax.rsqrt(jnp.mean(cen * cen, axis=-1, keepdims=True) + norm_eps)
        return cen * inv, inv

    def slabs(first, count, f):
        def one(j, carry):
            f(pl.ds(pl.multiple_of(first + j * SLAB, SLAB), SLAB), first + j * SLAB)
            return carry

        lax.fori_loop(0, count // SLAB, one, 0)

    def ln_block(i):
        def normalize(rows, at):
            normed, _ = layer_norm(A[0, rows, :].astype(F32))
            A[0, rows, :] = (normed * NB[0:1, :] + NB[1:2, :]).astype(BF16)
            A[1, rows, :] = (normed * NB[2:3, :] + NB[3:4, :]).astype(BF16)
            pos = lax.broadcasted_iota(jnp.int32, (SLAB, D), 0) + at
            grad = jnp.where(pos < seq_len, A[2, rows, :].astype(F32), 0.0)
            A[2, rows, :] = grad.astype(BF16)
            SM[4:5, :] += jnp.sum(grad, axis=0, keepdims=True)

        slabs(i * ROWS, ROWS, normalize)
        for a in range(3):
            Acc[a, ds(i, ROWS), :] = jnp.zeros((ROWS, D), F32)

    def y_step(u):
        ag_wait(u)
        w = W[u].reshape(D, UNIT)
        Y[u % 4] = dot(A[aidx(u)], w)

    def acc_step(u):
        a = aidx(u)
        g = G[u % 4]
        for j in range(2 * n):
            cols = slice(j * Dsl, (j + 1) * Dsl)
            Acc[a, :, cols] += dot_nt(g, W[u, j])

    lane = lax.broadcasted_iota(jnp.int32, (T, 128), 1)

    def rotate(y, sign):
        lo = y[:, :128]
        swapped = jnp.where(lane < 32, pltpu.roll(lo, 96, 1), pltpu.roll(lo, 32, 1))
        table = rope_ref[...]
        cosine = jnp.where(lane < ROT, table, 1.0)
        sine = jnp.where(lane < ROT, pltpu.roll(table, 128 - ROT, 1), 0.0)
        lo = lo * cosine + swapped * (sine * sign)
        return jnp.concatenate([lo, y[:, 128:]], axis=1)

    def attn_core(s):
        u0 = s - 3
        QK[0] = rotate(Y[0] + BI[u0, 0:1, :], 1.0).astype(BF16)
        QK[1] = rotate(Y[1] + BI[u0 + 1, 0:1, :], 1.0).astype(BF16)
        QK[2] = (Y[2] + BI[u0 + 2, 0:1, :]).astype(BF16)
        QK[3] = Y[3].astype(BF16)
        scale = 1.0 / math.sqrt(HD)

        def block(i, carry):
            rows = ds(i, ROWS)
            raw = dot_nt(QK[0, rows, :], QK[1]) * scale
            qpos = lax.broadcasted_iota(jnp.int32, (ROWS, T), 0) + i * ROWS
            kpos = lax.broadcasted_iota(jnp.int32, (ROWS, T), 1)
            scores = jnp.where((kpos <= qpos) & (kpos < seq_len), raw, -jnp.inf)
            top = jnp.max(scores, axis=-1, keepdims=True)
            e = jnp.exp(scores - top)
            p = e / jnp.sum(e, axis=-1, keepdims=True)
            pb = p.astype(BF16)
            PB[rows, :] = pb
            mixed = dot(pb, QK[2]).astype(BF16)
            G[3, rows, :] = mixed
            mg = QK[3, rows, :]
            delta = jnp.sum(mg.astype(F32) * mixed.astype(F32), axis=-1, keepdims=True)
            dp = dot_nt(mg, QK[2])
            dsb = (p * (dp - delta) * scale).astype(BF16)
            DS[rows, :] = dsb
            Y[0, rows, :] = dot(dsb, QK[1])
            return carry

        lax.fori_loop(0, T // ROWS, block, 0)
        Y[1] = dot_tn(DS[...], QK[0])
        for r in range(3):
            if r == 2:
                g = dot_tn(PB[...], QK[3])
            else:
                g = rotate(Y[r], -1.0)
            BG[u0 + r] = jnp.broadcast_to(jnp.sum(g, axis=0, keepdims=True), (8, UNIT))
            G[r] = g.astype(BF16)

    def ffn_core(s):
        b = BI[s - 1, 0:1, :]
        yu, yd = (s - 1) % 4, s % 4
        step = 64

        def block(i, total):
            rows = ds(i, step)
            v = Y[yu, rows, :] + b
            cdf2 = 1.0 + lax.erf(v * (1.0 / math.sqrt(2.0)))
            G[yd, rows, :] = (0.5 * v * cdf2).astype(BF16)
            slope = 0.5 * cdf2 + v * jnp.exp(-0.5 * v * v) * (1.0 / math.sqrt(2.0 * math.pi))
            g = Y[yd, rows, :] * slope
            G[yu, rows, :] = g.astype(BF16)
            return total + jnp.sum(g, axis=0, keepdims=True)

        total = lax.fori_loop(0, T // step, block, jnp.zeros((1, UNIT), F32))
        BG[s - 1] = jnp.broadcast_to(total, (8, UNIT))

    barrier = pltpu.get_barrier_semaphore()
    each_dp(lambda p: signal(barrier, p))
    each_tensor(lambda p: signal(barrier, p, "tensor"))
    x_in = pltpu.make_async_copy(x_hbm, A.at[0], in_sem.at[0])
    c_in = pltpu.make_async_copy(cot_hbm, A.at[2], in_sem.at[1])
    rope_in = pltpu.make_async_copy(rope_hbm, rope_ref, rope_sem.at[0])
    x_in.start()
    c_in.start()
    rope_in.start()
    spots = [
        buf.at[i, r * UNIT : (r + 1) * UNIT, 0:Dsl]
        for buf in (QK, G)
        for i in range(4)
        for r in range(T // UNIT)
    ]
    raws = [
        pltpu.make_async_copy(
            wout.at[i * UNIT : (i + 1) * UNIT, :]
            if i < heads
            else wdown.at[(i - heads) * UNIT : (i - heads + 1) * UNIT, :],
            spots[i],
            raw_sem.at[i],
        )
        for i in range(heads + chunks)
    ]
    for cp in raws:
        cp.start()

    def load_own(u, carry):
        nothing = lambda: None
        by_kind(
            u,
            lambda: own_load(wqkv.at[u % 4, :, ds(head_of(u), UNIT)], u).start(),
            nothing,
            lambda: own_load(wup.at[:, ds(chunk_of(u), UNIT)], u).start(),
            nothing,
        )
        return carry

    lax.fori_loop(0, U, load_own, 0)
    def lanes_of(ref):
        rows = ref[...].astype(F32)
        return jnp.concatenate([rows[i : i + 1] for i in range(rows.shape[0])], axis=1)

    SP[...] = jnp.zeros_like(SP)
    SW[...] = jnp.zeros_like(SW)
    for i, ref in enumerate((ga_ref, sa_ref, gf_ref, sf_ref, ob_ref)):
        SP[i : i + 1, 0:Dsl] = lanes_of(ref)
    SW[0, 0:3, 0 : d.nb] = qb_ref[...].astype(F32)
    SW[1, 0:1, 0 : d.ub] = lanes_of(ub_ref)[:, 0 : d.ub]
    at_q, at_u = me * d.nb, me * d.ub
    qb = pltpu.roll(SW[0], at_q % UNIT, 1)
    ub = pltpu.roll(SW[1], at_u % UNIT, 1)
    for h in range(heads):
        mine = jnp.where(at_q // UNIT == h, 1.0, 0.0)
        SP[8 + 3 * h : 11 + 3 * h, :] = qb[0:3, :] * mine
    for i in range(chunks):
        mine = jnp.where(at_u // UNIT == i, 1.0, 0.0)
        SP[8 + 3 * heads + i : 9 + 3 * heads + i, :] = ub[0:1, :] * mine
    pl.semaphore_wait(barrier, n_dp - 1 + tn - 1)

    def sp_copy(p, where):
        return rcopy(SP, RP.at[where], sp_s.at[0], sp_r.at[where], p)

    each_dp(lambda p: sp_copy(p, me).start())
    RP[me] = SP[...]

    def burst(u, carry):
        ag_own(u, has_r, agR, right)
        ag_own(u, has_l, agL, left)
        ag_self(u)
        return carry

    lax.fori_loop(0, d.burst, burst, 0)
    for i, cp in enumerate(raws):
        cp.wait()
        u = 4 * i + 3 if i < heads else F1 + 2 * (i - heads) + 1
        W[u, me] = jnp.transpose(spots[i][...])

    def end_chip(u, carry):
        @pl.when(z == 0)
        def _():
            ag_own(u, has_r, agR, right)

        @pl.when(z == n - 1)
        def _():
            ag_own(u, has_l, agL, left)

        return carry

    lax.fori_loop(d.burst, U, end_chip, 0)
    SM[...] = jnp.zeros_like(SM)
    BG[...] = jnp.zeros_like(BG)
    BI[...] = jnp.zeros_like(BI)
    each_dp(lambda p: sp_copy(p, p).wait_recv())
    for p in range(n_dp):
        NB[:, p * Dsl : (p + 1) * Dsl] = RP[p, 0:8, 0:Dsl]
    for i in range(3 * heads + chunks):
        row = RP[0, 8 + i : 9 + i, :]
        for p in range(1, n_dp):
            row = row + RP[p, 8 + i : 9 + i, :]
        if i < 3 * heads:
            u = F0 + 4 * (i // 3) + i % 3
        else:
            u = 2 * (i - 3 * heads)
            u = u if u < F0 else u + 4 * heads
        BI[u] = jnp.broadcast_to(row, (8, UNIT))
    x_in.wait()
    c_in.wait()
    rope_in.wait()
    own_all().wait()
    blocks = T // ROWS

    fills = max(ahead(h) for h in range(n - 1))

    def fill(i, carry):
        @pl.when(i < fills)
        def _():
            ag_step(i - fills)

        @pl.when(i < blocks)
        def _():
            ln_block(i)

        return carry

    lax.fori_loop(0, max(fills, blocks), fill, 0)

    def made(s):
        return jnp.maximum(jnp.where(s < F1, s - 2, jnp.where(s == F1, s - 1, s)), 0)

    whole_by = U - d.held - 1 - d.lag
    sent_early = max(0, whole_by)

    def early(q):
        return jnp.clip(jnp.minimum(2 * (q - d.Q0 + 1), q - d.lag), 0, sent_early)

    def first_one(u, carry):
        p2_first(u)
        return carry

    def make(q, carry):
        dw_sib(q)
        guarded(q - 1, combine)

        @pl.when(q < U - d.held)
        def _():
            rs_step(q)

        acc_step(q)
        dw_own(q)
        lax.fori_loop(early(q - 1), early(q), first_one, 0)
        return carry

    def body(s, carry):
        ag_step(s)
        guarded(s, y_step)

        @pl.when(s == F1 + 2)
        def _():
            x_in.start()

        @pl.when(is_attn(s) & (s % 4 == 3))
        def _():
            attn_core(s)

        @pl.when(jnp.logical_not(is_attn(s)) & (s < U) & (s % 2 == 1))
        def _():
            ffn_core(s)

        lax.fori_loop(made(s - 1), made(s), make, 0)
        return carry

    lax.fori_loop(0, U + 1, body, 0)
    x_in.wait()

    @pl.when(has_r)
    def _():
        signal(ready.at[1], right)

    @pl.when(has_l)
    def _():
        signal(ready.at[0], left)

    lo = d.lo
    hi = tn // lo
    size = ((lo, hi), (hi, lo))
    coord = ((mt % lo, mt // lo), (mt // lo, mt % lo))
    acc_of = (2, 0)
    own = ds(mt, Tr)

    def block_of(k, a, b):
        return b * lo + a if k == 0 else a * lo + b

    def packed(mine, theirs):
        return mine - jnp.where(mine > theirs, 1, 0)

    def s1_copy(k, a, b, sender):
        s2 = size[k][1]
        return rcopy_to(
            A.at[k, ds(block_of(k, a, b), Tr), :],
            pr_hbm.at[k, packed(sender, a) * s2 + b],
            s1_s.at[k, a * s2 + b],
            s1_r.at[k, sender * s2 + b],
            {"tensor": block_of(k, a, coord[k][1])},
        )

    def s1_wait(k, q, b):
        s2 = size[k][1]
        c1 = coord[k][0]
        return rcopy_to(
            A.at[k, own, :],
            pr_hbm.at[k, packed(q, c1) * s2 + b],
            s1_s.at[k, q * s2 + b],
            s1_r.at[k, q * s2 + b],
            {"tensor": block_of(k, q, coord[k][1])},
        )

    def s2_copy(k, b, sender):
        c1 = coord[k][0]
        return rcopy_to(
            A.at[k, ds(block_of(k, c1, b), Tr), :],
            pr_hbm.at[k, d.P1 + packed(sender, b)],
            s2_s.at[k, b],
            s2_r.at[k, sender],
            {"tensor": block_of(k, c1, b)},
        )

    def s2_wait(k, q):
        c1, c2 = coord[k]
        return rcopy_to(
            A.at[k, own, :],
            pr_hbm.at[k, d.P1 + packed(q, c2)],
            s2_s.at[k, q],
            s2_r.at[k, q],
            {"tensor": block_of(k, c1, q)},
        )

    def others(k, which, f):
        for q in range(size[k][which]):

            @pl.when(q != coord[k][which])
            def _(q=q):
                f(q)

    def s1_send(j):
        i = block_at(j)

        @pl.when(j >= 0)
        def _():
            for k in range(2):
                a = i % lo if k == 0 else i // lo
                b = i // lo if k == 0 else i % lo

                @pl.when(a != coord[k][0])
                def _(k=k, a=a, b=b):
                    s1_copy(k, a, b, coord[k][0]).start()

    def block_at(j):
        o = tn - 1 - j
        return (mt // lo + o // lo) % hi * lo + (mt % lo + o % lo) % lo

    def partial(j, carry):
        i = block_at(j)

        @pl.when(i == mt)
        def _():
            A[2, ds((mt + 1) % tn, Tr), :] = A[0, ds(i, Tr), :]

        def rows_of(rows, at):
            normed, _ = layer_norm(A[0, rows, :].astype(F32))
            ab = Acc[0, rows, :]
            fb = Acc[1, rows, :]
            SM[0:1, :] += jnp.sum(ab * normed, axis=0, keepdims=True)
            SM[1:2, :] += jnp.sum(ab, axis=0, keepdims=True)
            SM[2:3, :] += jnp.sum(fb * normed, axis=0, keepdims=True)
            SM[3:4, :] += jnp.sum(fb, axis=0, keepdims=True)
            ng = ab * NB[0:1, :] + fb * NB[2:3, :]
            Acc[0, rows, :] = ng
            A[1, rows, :] = ng.astype(BF16)
            A[0, rows, :] = Acc[2, rows, :].astype(BF16)

        slabs(i * Tr, Tr, rows_of)
        s1_send(j - 1)
        return carry

    lax.fori_loop(0, tn, partial, 0)
    for u in range(U):
        BGC[u : u + 1, :] = BG[u, 0:1, :]
    s1_send(tn - 1)

    def sm_copy(p, where):
        return rcopy(
            SM.at[:, ds(p, Dsl)], RS1.at[where], sm_s.at[0], sm_r.at[0, where], p
        )

    def bg_copy(p, where):
        return rcopy(BGC, RB2.at[where], sm_s.at[1], sm_r.at[1, where], p)

    def small_send(p):
        sm_copy(p, me).start()
        bg_copy(p, me).start()

    each_dp(small_send)
    RS1[me] = SM[:, ds(me, Dsl)]
    RB2[me] = BGC[...]

    @pl.when(has_r)
    def _():
        pl.semaphore_wait(ready.at[0], 1)

    @pl.when(has_l)
    def _():
        pl.semaphore_wait(ready.at[1], 1)

    rest = d.held + d.lag + (n - 3) * d.lag2 + 1
    steps = U + d.hop * (n - 3)

    def p2_count(i):
        fed = jnp.minimum(d.pace * (i + 1), whole_by + i)
        return jnp.clip(jnp.where(i < rest, fed, steps), 0, steps)

    def p2_one(i, carry):
        p2_step(i)
        return carry

    def drain(i, carry):
        rs_step(i + U - d.held)
        guarded(i + whole_by, p2_first)
        lax.fori_loop(p2_count(i - 1), p2_count(i), p2_one, 0)
        return carry

    marks = [min(m, rest) for m in d.marks]
    combine(U - 1)
    lax.fori_loop(0, marks[0], drain, 0)

    def load(k, slot, b):
        return pltpu.make_async_copy(
            pr_hbm.at[k, slot], A.at[k, ds(b, Tr), :], loc_sem.at[k, slot]
        )

    def s1_take(k, b):
        s1, s2 = size[k]
        row_b = block_of(k, coord[k][0], b)
        rows = ds(row_b, Tr)
        others(k, 0, lambda q: s1_wait(k, q, b).wait_recv())
        for q in range(s1 - 1):
            cp = load(k, q * s2 + b, row_b)
            cp.start()
            cp.wait()
            Acc[acc_of[k], rows, :] += A[k, rows, :].astype(F32)

    for k in range(2):

        def pass_on(b, k=k):
            s1_take(k, b)
            rows = ds(block_of(k, coord[k][0], b), Tr)
            A[k, rows, :] = Acc[acc_of[k], rows, :].astype(BF16)
            s2_copy(k, b, coord[k][1]).start()

        others(k, 1, pass_on)

    lax.fori_loop(marks[0], marks[1], drain, 0)

    def small_wait(p):
        sm_copy(p, p).wait_recv()
        bg_copy(p, p).wait_recv()

    each_dp(small_wait)
    total = RS1[0]
    bias_total = RB2[0]
    for p in range(1, n_dp):
        total = total + RS1[p]
        bias_total = bias_total + RB2[p]
    SBT[...] = bias_total
    ST[...] = total

    for k in range(2):
        s1_take(k, coord[k][1])
        others(k, 1, lambda q, k=k: s2_wait(k, q).wait_recv())
        for q in range(size[k][1] - 1):
            cp = load(k, d.P1 + q, mt)
            cp.start()
            cp.wait()
            Acc[acc_of[k], own, :] += A[k, own, :].astype(F32)

    def st_copy(p, where):
        return rcopy_to(ST, RT.at[where], st_s.at[0], st_r.at[where], {"tensor": p})

    each_tensor(lambda p: st_copy(p, mt).start())
    def finish(rows, at):
        off = pl.multiple_of((mt + 1) % tn * Tr + at - mt * Tr, SLAB)
        xr = A[2, pl.ds(off, SLAB), :].astype(F32)
        normed, inv = layer_norm(xr)
        ng = Acc[0, rows, :]
        gm = jnp.mean(ng, axis=-1, keepdims=True)
        gp = jnp.mean(ng * normed, axis=-1, keepdims=True)
        A[0, rows, :] = (xr + Acc[2, rows, :] + NB[4:5, :]).astype(BF16)
        A[1, rows, :] = (A[2, rows, :].astype(F32) + inv * (ng - gm - normed * gp)).astype(BF16)

    slabs(mt * Tr, Tr, finish)
    outs = (o_hbm, dx_hbm)

    def f1_copy(k, b, sender):
        c1 = coord[k][0]
        return rcopy_to(
            A.at[k, own, :],
            outs[k].at[ds(block_of(k, c1, sender), Tr), :],
            f1_s.at[k, b],
            f1_r.at[k, sender],
            {"tensor": block_of(k, c1, b)},
        )

    def f2_copy(k, a, b, sender, src):
        s2 = size[k][1]
        return rcopy_to(
            src,
            outs[k].at[ds(block_of(k, sender, b), Tr), :],
            f2_s.at[k, a * s2 + b],
            f2_r.at[k, sender * s2 + b],
            {"tensor": block_of(k, a, coord[k][1])},
        )

    home = [
        pltpu.make_async_copy(A.at[k, own, :], outs[k].at[own, :], in_sem.at[k])
        for k in range(2)
    ]
    for k in range(2):
        c1, c2 = coord[k]
        others(k, 1, lambda b, k=k, c2=c2: f1_copy(k, b, c2).start())
    for k in range(2):
        c1, c2 = coord[k]

        def mine_on(a, k=k, c1=c1, c2=c2):
            f2_copy(k, a, c2, c1, A.at[k, own, :]).start()

        others(k, 0, mine_on)
        home[k].start()
    lax.fori_loop(marks[1], marks[2], drain, 0)
    for k in range(2):
        c1, c2 = coord[k]

        def forward(b, k=k, c1=c1):
            f1_copy(k, b, b).wait_recv()
            rows = ds(block_of(k, c1, b), Tr)
            others(k, 0, lambda a: f2_copy(k, a, b, c1, outs[k].at[rows, :]).start())

        others(k, 1, forward)
    lax.fori_loop(marks[2], rest, drain, 0)
    lax.fori_loop(p2_count(rest - 1), steps, p2_one, 0)

    each_tensor(lambda p: st_copy(p, p).wait_recv())
    RT[mt] = ST[...]
    whole = RT[0]
    for p in range(1, tn):
        whole = whole + RT[p]
    row = lax.broadcasted_iota(jnp.int32, (8, Dsl), 0)
    so_ref[0:8, 0:Dsl] = jnp.where(row < 4, whole, ST[...])

    def share(first, stride, size):
        at = me * size
        one = SBT[pl.ds(first + stride * (at // UNIT), 1), :]
        wide = jnp.broadcast_to(one, (8, UNIT))
        return pltpu.roll(wide, (UNIT - at % UNIT) % UNIT, 1)[0:1, :]

    so_ref[8:9, :] = share(F1, 2, d.ub)
    for r in range(3):
        so_ref[9 + r : 10 + r, :] = share(r, 4, d.nb)

    for k in range(2):
        c1, c2 = coord[k]
        s1, s2 = size[k]

        def end0(q, k=k, c1=c1, s2=s2):
            for b in range(s2):
                s1_copy(k, q, b, c1).wait_send()
                f2_copy(k, q, b, c1, A.at[k, own, :]).wait_send()
                f2_copy(k, q, b, q, A.at[k, own, :]).wait_recv()

        def end1(b, k=k, c2=c2):
            s2_copy(k, b, c2).wait_send()
            f1_copy(k, b, c2).wait_send()

        others(k, 0, end0)
        others(k, 1, end1)

    for buf, sem, count in (
        (RP, sp_s.at[0], n_dp - 1),
        (RS1, sm_s.at[0], n_dp - 1),
        (RB2, sm_s.at[1], n_dp - 1),
        (RT, st_s.at[0], tn - 1),
    ):
        if count:
            span = buf.at[0:count]
            rcopy(span, span, sem, sp_r.at[0], sib).wait_send()
    for cp in home:
        cp.wait()

    ag_finish()

    @pl.when(has_r & has_l)
    def _():
        units_sent(p2_s.at[0])
        units_sent(p2_s.at[1])

    for v in range(max(0, U - NS), U):
        rs_finish(v)
    for v in range(max(0, U - 2), U):
        sb_copy(v).wait_send()
        out_wait(v)


def run_layer(d, seq_len, small, rope, x, cot, wqkv, wout, wup, wdown):
    n, tn, T, D, Dsl, U = d.n, d.tn, d.T, d.D, d.Dsl, d.U
    n_dp = 2 * n
    width, hidden = d.heads * UNIT, d.chunks * UNIT
    rp, up = (8 + 3 * d.heads + d.chunks + 7) // 8 * 8, (U + 7) // 8 * 8
    dma = pltpu.SemaphoreType.DMA
    reg = pltpu.SemaphoreType.REGULAR
    vm = pl.BlockSpec(memory_space=pltpu.VMEM)
    hbm = pl.BlockSpec(memory_space=pl.ANY)
    tile = (Dsl, UNIT)
    return pl.pallas_call(
        functools.partial(layer_kernel, d),
        out_shape=(
            pltpu.VMEM((T, D), BF16),
            jax.ShapeDtypeStruct((T, D), BF16),
            jax.ShapeDtypeStruct((3, Dsl, width), F32),
            jax.ShapeDtypeStruct((width, Dsl), F32),
            jax.ShapeDtypeStruct((Dsl, hidden), F32),
            jax.ShapeDtypeStruct((hidden, Dsl), F32),
            jax.ShapeDtypeStruct((2, d.P1 + d.P2, T // tn, D), BF16),
            jax.ShapeDtypeStruct((16, UNIT), F32),
        ),
        in_specs=[pl.BlockSpec(memory_space=pltpu.SMEM)] + [vm] * 7 + [hbm] * 7,
        out_specs=(hbm,) * 7 + (vm,),
        scratch_shapes=[
            pltpu.VMEM((U, n_dp) + tile, BF16),
            pltpu.VMEM((3, T, D), BF16),
            pltpu.VMEM((T, 128), F32),
            pltpu.VMEM((3, T, D), F32),
            pltpu.VMEM((4, T, UNIT), F32),
            pltpu.VMEM((4, T, UNIT), BF16),
            pltpu.VMEM((4, T, UNIT), BF16),
            pltpu.VMEM((T, T), BF16),
            pltpu.VMEM((T, T), BF16),
            pltpu.VMEM((d.NS, n - 2) + tile, BF16),
            pltpu.VMEM((2, n) + tile, BF16),
            pltpu.VMEM((d.NSR, n) + tile, BF16),
            pltpu.VMEM((d.NLR, n) + tile, BF16),
            pltpu.VMEM((2,) + tile, F32),
            pltpu.VMEM((2, UNIT, Dsl), F32),
            pltpu.VMEM((n_dp, rp, UNIT), F32),
            pltpu.VMEM((8, D), F32),
            pltpu.VMEM((U, 8, UNIT), F32),
            pltpu.VMEM((8, D), F32),
            pltpu.VMEM((U, 8, UNIT), F32),
            pltpu.VMEM((up, UNIT), F32),
            pltpu.VMEM((n_dp, 8, Dsl), F32),
            pltpu.VMEM((n_dp, up, UNIT), F32),
            pltpu.VMEM((8, Dsl), F32),
            pltpu.VMEM((tn, 8, Dsl), F32),
            pltpu.VMEM((up, UNIT), F32),
            dma((2,)),
            dma((1,)),
            dma((U, n)),
            dma((U,)),
            dma((n,)),
            dma((n,)),
            dma((n,)),
            reg((2,)),
            reg((2,)),
            dma((2,)),
            dma((d.NSR,)),
            dma((d.NS,)),
            dma((d.NLR, n)),
            dma((2,)),
            dma((1,)),
            dma((n_dp,)),
            dma((2,)),
            dma((2, n_dp)),
            dma((1,)),
            dma((tn,)),
            dma((2, tn)),
            dma((2, tn)),
            dma((2, tn)),
            dma((2, tn)),
            dma((2, tn)),
            dma((2, tn)),
            dma((2, tn)),
            dma((2, tn)),
            dma((2, d.P1 + d.P2)),
            dma((d.heads + d.chunks,)),
            dma((2,)),
            dma((2, U)),
            dma((1,)),
            pltpu.VMEM((rp, UNIT), F32),
            pltpu.VMEM((2, 8, UNIT), F32),
        ],
        compiler_params=pltpu.CompilerParams(
            collective_id=0, has_side_effects=True, vmem_limit_bytes=64_850_000
        ),
        cost_estimate=pl.CostEstimate(
            flops=6 * U * T * D * UNIT,
            bytes_accessed=6 * U * Dsl * UNIT + 8 * T * D,
            transcendentals=T * UNIT * U,
        ),
    )(seq_len, *small, rope, x, cot, wqkv, wout, wup, wdown)


def rope_pair(rows):
    half = ROT // 2
    inv_freq = np.exp(-(2.0 * np.arange(half) / ROT) * math.log(rope_base))
    angles = np.arange(rows)[:, None] * inv_freq[None, :]
    cosine, sine = np.cos(angles), np.sin(angles)
    table = np.concatenate([cosine, cosine, -sine, sine], axis=1).astype(np.float32)
    return jnp.asarray(table)


def per_device(
    n_dp,
    tn,
    block_input,
    cotangent,
    lengths,
    attn_gain,
    attn_shift,
    ffn_gain,
    ffn_shift,
    qkv_weight,
    qkv_bias,
    out_weight,
    out_bias,
    up_weight,
    up_bias,
    down_weight,
):
    T, D = block_input.shape
    n = n_dp // 2
    Dsl = D // n_dp
    width = qkv_weight.shape[2]
    heads = width // HD
    hidden = up_weight.shape[1]
    chunks = hidden // UNIT
    U = 4 * heads + 2 * chunks
    F0, lag, lag2 = 0, 5, 1
    nb, ub = qkv_bias.shape[1], up_bias.shape[0]
    hi = 2 if tn % 2 == 0 else 1
    lo = tn // hi
    d = types.SimpleNamespace(
        n=n,
        tn=tn,
        T=T,
        D=D,
        Dsl=Dsl,
        U=U,
        heads=heads,
        chunks=chunks,
        F0=F0,
        held=3,
        ahead=(1, 3, 2),
        own=5,
        burst=3,
        hop=2,
        lag=lag,
        lag2=lag2,
        nb=nb,
        ub=ub,
        pace=3,
        Q0=U - 8,
        NS=min(U, lag + (n - 3) * lag2 + 4),
        NSR=4,
        NLR=min(U, lag + (n - 3) * lag2 + 1),
        lo=lo,
        P1=max((lo - 1) * hi, (hi - 1) * lo),
        P2=max(lo, hi) - 1,
        marks=(3, 4, 6),
    )
    flat = (attn_gain, attn_shift, ffn_gain, ffn_shift, out_bias, jnp.pad(up_bias, (0, -ub % 128)))
    small = [v.reshape(-1, 128) for v in flat] + [qkv_bias]
    out, dx, dqkv, dout, dup, ddown, _, so = run_layer(
        d,
        lengths,
        small,
        rope_pair(T),
        block_input,
        cotangent,
        qkv_weight,
        out_weight,
        up_weight,
        down_weight,
    )
    return (
        out,
        dx,
        so[0, :Dsl],
        so[1, :Dsl],
        so[2, :Dsl],
        so[3, :Dsl],
        dqkv,
        so[9:12, :nb],
        dout,
        so[4, :Dsl],
        dup,
        so[8, :ub],
        ddown,
    )


def solution(mesh):
    in_specs = (
        P("dp", None),
        P("dp", None),
        P("dp"),
        P("dp"),
        P("dp"),
        P("dp"),
        P("dp"),
        P(None, "dp", "tensor"),
        P(None, ("tensor", "dp")),
        P("tensor", "dp"),
        P("dp"),
        P("dp", "tensor"),
        P(("tensor", "dp")),
        P("tensor", "dp"),
    )
    out_specs = (
        P("dp", None),
        P("dp", None),
        P("dp"),
        P("dp"),
        P("dp"),
        P("dp"),
        P(None, "dp", "tensor"),
        P(None, ("tensor", "dp")),
        P("tensor", "dp"),
        P("dp"),
        P("dp", "tensor"),
        P(("tensor", "dp")),
        P("tensor", "dp"),
    )
    return jax.shard_map(
        functools.partial(per_device, mesh.shape["dp"], mesh.shape["tensor"]),
        mesh=mesh,
        in_specs=in_specs,
        out_specs=out_specs,
        check_vma=False,
    )
```
